16 devices in a mesh: local: 4 (over z, y), data: 4 (over x, core).
Axes of the slice: x: 2, y: 2, z: 2, core: 2. Of those that a mesh axis runs over, the one named last changes fastest.
Arguments:
- tokens: bfloat16 [32768, 1024], P(('data', 'local'))
- cotangent: bfloat16 [32768, 1024], P(('data', 'local'))
- w_up: bfloat16 [4, 1024, 4096], P(None, ('data', 'local'))
- w_down: bfloat16 [4, 4096, 1024], P(None, ('data', 'local'))
- lora_a: float32 [4, 1024, 4], replicated
- lora_b: float32 [4, 4, 4096], replicated
Outputs:
- output 1: bfloat16 [32768, 1024], P(('data', 'local'))
- output 2: bfloat16 [32768, 1024], P(('data', 'local'))
- output 3: float32 [4, 1024, 4], replicated
- output 4: float32 [4, 4, 4096], replicated
All inputs are finite; a program needn't handle non-finite values.
Results may differ from the reference program's by a relative error of at most 0.0186195.
Values are sent between devices in bfloat16 or wider.
A program may use at most 1 GiB of HBM per device.

```python
import jax
import jax.numpy as jnp
from jax import lax

TOKENS = 2048
NUM_DEVICES = 16
HIDDEN = 1024
FF_DIM = 4096
RANK = 4
LAYERS = 4

TOTAL_TOKENS = NUM_DEVICES * TOKENS


def setup_inputs(seed: int = 0) -> dict:
    keys = jax.random.split(jax.random.key(seed), 6)
    tokens = jax.random.normal(keys[0], (TOTAL_TOKENS, HIDDEN), jnp.float32).astype(jnp.bfloat16)
    cotangent = jax.random.normal(keys[1], (TOTAL_TOKENS, HIDDEN), jnp.float32).astype(jnp.bfloat16)
    w_up = (jax.random.normal(keys[2], (LAYERS, HIDDEN, FF_DIM), jnp.float32) * HIDDEN ** -0.5).astype(jnp.bfloat16)
    w_down = (jax.random.normal(keys[3], (LAYERS, FF_DIM, HIDDEN), jnp.float32) * FF_DIM ** -0.5).astype(jnp.bfloat16)
    lora_a = jax.random.normal(keys[4], (LAYERS, HIDDEN, RANK), jnp.float32) * HIDDEN ** -0.5
    lora_b = jax.random.normal(keys[5], (LAYERS, RANK, FF_DIM), jnp.float32) * (0.5 / RANK) ** 0.5
    return {"tokens": tokens, "cotangent": cotangent, "w_up": w_up, "w_down": w_down, "lora_a": lora_a, "lora_b": lora_b}


def layer_forward(resid, w_in, w_out, adapt_a, adapt_b):
    resid_f = resid.astype(jnp.float32)
    inv_rms = lax.rsqrt(jnp.mean(resid_f * resid_f, axis=-1, keepdims=True) + 1e-6)
    normed = (resid_f * inv_rms).astype(jnp.bfloat16)
    low_rank = jnp.dot(normed.astype(jnp.float32), adapt_a)
    pre_act = (jnp.dot(normed, w_in, preferred_element_type=jnp.float32) + jnp.dot(low_rank, adapt_b)).astype(jnp.bfloat16)
    hidden_act = jax.nn.gelu(pre_act.astype(jnp.float32), approximate=True).astype(jnp.bfloat16)
    return (resid_f + jnp.dot(hidden_act, w_out, preferred_element_type=jnp.float32)).astype(jnp.bfloat16)


def stack_forward(resid, w_up, w_down, lora_a, lora_b):
    def body(carry, weights):
        w_in, w_out, adapt_a, adapt_b = weights
        return layer_forward(carry, w_in, w_out, adapt_a, adapt_b), None
    result, _ = lax.scan(body, resid, (w_up, w_down, lora_a, lora_b))
    return result


def reference(tokens, cotangent, w_up, w_down, lora_a, lora_b):
    tok_blocks = tokens.reshape(NUM_DEVICES, TOKENS, HIDDEN)
    cot_blocks = cotangent.reshape(NUM_DEVICES, TOKENS, HIDDEN)

    def block_step(running, pair):
        blk_tokens, blk_cot = pair
        result, pullback = jax.vjp(lambda blk_in, adapt_a, adapt_b: stack_forward(blk_in, w_up, w_down, adapt_a, adapt_b), blk_tokens, lora_a, lora_b)
        grad_x, grad_a, grad_b = pullback(blk_cot)
        return (running[0] + grad_a, running[1] + grad_b), (result, grad_x)

    start_sums = (jnp.zeros(lora_a.shape, jnp.float32), jnp.zeros(lora_b.shape, jnp.float32))
    (sum_a, sum_b), (out_blocks, grad_blocks) = lax.scan(block_step, start_sums, (tok_blocks, cot_blocks))
    return (out_blocks.reshape(TOTAL_TOKENS, HIDDEN), grad_blocks.reshape(TOTAL_TOKENS, HIDDEN), sum_a, sum_b)
```

```python
import jax
import jax.numpy as jnp
from jax import lax
from jax.experimental import pallas as pl
from jax.experimental.pallas import tpu as pltpu
from jax.sharding import PartitionSpec as P

GROUP = ("data", "local")
NORM_EPS = 1e-6
BF = jnp.bfloat16
F32 = jnp.float32
C0 = 0.7978845608028654
K0 = 0.044715

T = 2048
H = 1024
F = 4096
L = 4
NG = 8 * L
MU = 512
MD = 1024
ROWS = ((0, 96), (96, 80), (176, 80))
GW = 640


def nn(a, b):
    return lax.dot_general(a, b, (((1,), (0,)), ((), ())), preferred_element_type=F32)


def nt(a, b):
    return lax.dot_general(a, b, (((1,), (1,)), ((), ())), preferred_element_type=F32)


def tn(a, b):
    return lax.dot_general(a, b, (((0,), (0,)), ((), ())), preferred_element_type=F32)


def split3(v):
    p1 = v.astype(BF).astype(F32)
    rest = v - p1
    p2 = rest.astype(BF).astype(F32)
    return p1, p2, (rest - p2).astype(BF).astype(F32)


def left_parts(v):
    p1, p2, p3 = split3(v)
    return jnp.concatenate([p1, p2, p3, p1, p1, p2], axis=0).astype(BF)


def right_parts(v):
    p1, p2, p3 = split3(v)
    return jnp.concatenate([p3, p2, p1, p1, p2, p1], axis=0).astype(BF)


def sum_parts(v):
    return v[0:8] + v[8:16] + v[16:24]


def gelu_and_slope(pre):
    x = pre.astype(F32)
    sq = x * x
    half = 0.5 * jnp.tanh(x * (sq * (C0 * K0) + C0)) + 0.5
    act = x * half
    slope = (act * (1.0 - half)) * (sq * (6.0 * C0 * K0) + 2.0 * C0) + half
    return act.astype(BF), slope


def rows_of(m, size):
    return pl.ds(pl.multiple_of(m * size, size), size)


def kernel(
    tok, cot, up, down, a8, b8,
    xout, gtok, gout, gp, xs, kept,
    w, sd, xb, ub, db, gst, acat, bcat, vcat, dcat, dlt, gb, ga, gacc, rbuf, gall,
    own_sem, fs_sem, fr_sem, kept_sem, gp_sem, io_sem, bo_sem, bs_sem, br_sem, rs_sem, rr_sem, as_sem, ar_sem,
    cred,
):
    data = lax.axis_index("data")
    local = lax.axis_index("local")
    x, c = lax.div(data, 2), lax.rem(data, 2)
    z, y = lax.div(local, 2), lax.rem(local, 2)
    me = data * 4 + local
    dx, dy, dz, dc = 1 - 2 * x, 1 - 2 * y, 1 - 2 * z, 1 - 2 * c
    par = lax.rem(x + y + z, 2)

    def quarter(i):
        hi, lo = lax.div(i, 2), lax.rem(i, 2)
        return 2 * (par + hi - 2 * par * hi) + (c + lo - 2 * c * lo)

    q_own, q_miss = quarter(0), quarter(2)

    def pick(dim, a0, a1, a2):
        return lax.div((1 - dim) * (2 - dim), 2) * a0 + dim * (2 - dim) * a1 + lax.div(dim * (dim - 1), 2) * a2

    def device(dim):
        return (local + pick(dim, 0, dy, 2 * dz), data + pick(dim, 2 * dx, 0, 0))

    neighbours = ((local, data + 2 * dx), (local + dy, data), (local + 2 * dz, data), (local, data + dc))
    partner = neighbours[3]

    def remote(src, dst, ssem, rsem, dev):
        return pltpu.make_async_remote_copy(
            src_ref=src, dst_ref=dst, send_sem=ssem, recv_sem=rsem, device_id=dev, device_id_type=pl.DeviceIdType.MESH
        )


    def own_load(g):
        s, l = lax.rem(g, 8), lax.div(g, 8)

        @pl.when(s < 4)
        def _():
            for n in range(4):
                pltpu.make_async_copy(
                    up.at[l, :, pl.ds(pl.multiple_of(s * 1024 + n * 256, 256), 256)],
                    w.at[s, me, pl.ds(n * 64, 64), :],
                    own_sem.at[s],
                ).start()

        @pl.when(s >= 4)
        def _():
            pltpu.make_async_copy(
                down.at[l, :, pl.ds(pl.multiple_of((s - 4) * 256, 256), 256)], w.at[s, me], own_sem.at[s]
            ).start()

    def colour(g):
        q = lax.rem(g + c, 3)
        return q, lax.rem(q + 2, 3), lax.rem(q + 1, 3)

    def delta(dim):
        return pick(dim, 8 * dx, dy, 2 * dz)

    def use_credit(g, dim):
        @pl.when(g >= 8)
        def _():
            pl.semaphore_wait(cred.at[dim, lax.rem(g, 8)], 1)

    def send_blocks(g, phase, dim, blocks, dev):
        s = lax.rem(g, 8)
        use_credit(g, dim)
        for b in blocks:
            remote(w.at[s, b], w.at[s, b], fs_sem.at[phase, s], fr_sem.at[phase, s], dev).start()

    def span(g, phase):
        s = lax.rem(g, 8)
        r = w.at[s, pl.ds(0, (1, 2, 4, 8)[phase])]
        return remote(r, r, fs_sem.at[phase, s], fr_sem.at[phase, s], partner)

    def ready(g):
        return jnp.logical_and(g >= 0, g < NG)

    def event0(r):
        g3, g6 = r + 3, r + 6

        @pl.when(ready(g3))
        def _():
            d1, d2, d3 = colour(g3)
            e1, e2 = delta(d1), delta(d2)
            span(g3, 1).wait_recv()
            send_blocks(g3, 2, d3, (me, me + e1, me + e2, me + e1 + e2), device(d3))

        @pl.when(ready(g6))
        def _():
            d1, _, _ = colour(g6)
            s = lax.rem(g6, 8)
            pltpu.make_async_copy(w.at[s, me], w.at[s, me], own_sem.at[s]).wait()
            send_blocks(g6, 0, d1, (me,), device(d1))

    def event1(r):
        g5, g2 = r + 5, r + 2

        @pl.when(ready(g5))
        def _():
            d1, d2, _ = colour(g5)
            span(g5, 0).wait_recv()
            send_blocks(g5, 1, d2, (me, me + delta(d1)), device(d2))

        @pl.when(ready(g2))
        def _():
            s = lax.rem(g2, 8)
            span(g2, 2).wait_recv()
            use_credit(g2, 3)
            for h in range(2):
                r2 = w.at[s, pl.ds(8 * h + 4 * c, 4)]
                remote(r2, r2, fs_sem.at[3, s], fr_sem.at[3, s], partner).start()

    def keep_copy(g):
        s, l = lax.rem(g, 8), lax.div(g, 8)
        return pltpu.make_async_copy(w.at[s, pl.ds(4 * q_own, 4)], kept.at[l, s], kept_sem.at[s])

    def arrive(g):
        span(g, 3).wait_recv()
        keep_copy(g).start()

    def release(g):
        s = lax.rem(g, 8)
        for phase in range(4):
            span(g, phase).wait_send()
        keep_copy(g).wait()
        for i in range(4):
            pl.semaphore_signal(cred.at[i, s], inc=1, device_id=neighbours[i], device_id_type=pl.DeviceIdType.MESH)

        @pl.when(g + 8 < NG)
        def _():
            own_load(g + 8)


    def whole(m, q):
        return w.at[pl.ds(4 * m, 4), pl.ds(4 * q, 4)]

    def part(ref, dim):
        return ref.at[:, :, pl.ds(*ROWS[dim]), :]

    def b_own(m, l):
        return pltpu.make_async_copy(kept.at[l, pl.ds(4 * m, 4)], whole(m, q_own), bo_sem.at[m])

    def b_send(m, l, i, q):
        src, dst = kept.at[l, pl.ds(4 * m, 4)], whole(m, q)
        if i < 3:
            src, dst = part(src, i), part(dst, i)
        return remote(src, dst, bs_sem.at[m, i], br_sem.at[m, i], neighbours[i])

    def b_forward(m):
        return remote(whole(m, q_miss), whole(m, q_miss), bs_sem.at[m, 4], br_sem.at[m, 4], partner)

    def gather(m, l):
        b_own(m, l).start()
        for i in range(4):
            for s in range(4):
                pl.semaphore_wait(cred.at[i, 4 * m + s], 1)
            b_send(m, l, i, q_own).start()

    def b_events(m, l, i):
        @pl.when(i == 0)
        def _():
            b_own(m, l).wait()

        @pl.when(i == 1)
        def _():
            b_send(m, l, 3, quarter(1)).wait_recv()

        @pl.when(i == 2)
        def _():
            for d in range(3):
                b_send(m, l, d, q_miss).wait_recv()
            b_forward(m).start()

        @pl.when(i == 3)
        def _():
            b_forward(m).wait_recv()

    def b_release(m, l):
        b_forward(m).wait_send()
        for i in range(4):
            b_send(m, l, i, q_own).wait_send()

        @pl.when(l > 0)
        def _():
            for i in range(4):
                for s in range(4):
                    pl.semaphore_signal(
                        cred.at[i, 4 * m + s], inc=1, device_id=neighbours[i], device_id_type=pl.DeviceIdType.MESH
                    )


    def grad_send(l, i):
        return remote(
            gacc.at[l, :, pl.ds(i * GW, GW)], rbuf.at[me], rs_sem.at[l], rr_sem, (jnp.int32(i), l)
        )

    def grads_out(l):
        for i in range(4):
            mine = me == 4 * l + i

            @pl.when(jnp.logical_not(mine))
            def _():
                grad_send(l, i).start()

            @pl.when(mine)
            def _():
                rbuf[me] = gacc[l, :, i * GW : (i + 1) * GW]


    tok_in = pltpu.make_async_copy(tok, xb, io_sem.at[0])
    cot_in = pltpu.make_async_copy(cot, db, io_sem.at[1])

    def first_loads(g, _):
        own_load(g)
        return 0

    lax.fori_loop(0, 8, first_loads, 0)
    tok_in.start()
    cot_in.start()

    def fill(r, _):
        event0(r)
        event1(r)
        return 0

    for l in range(L):
        acat[l] = right_parts(a8[l])
        bcat[l] = right_parts(b8[l])
    lax.fori_loop(-6, 0, fill, 0)
    tok_in.wait()
    cot_in.wait()


    def inv_rms(rf):
        return lax.rsqrt(jnp.mean(rf * rf, axis=-1, keepdims=True) + NORM_EPS)

    def x_save(l):
        return pltpu.make_async_copy(xb, xs.at[l - 1], io_sem.at[0])

    def gp_out(l, k, m):
        b = lax.rem(m, 2)
        return pltpu.make_async_copy(gst.at[b], gp.at[l, k, rows_of(m, MU), :], gp_sem.at[b])

    def forward_layer(l, _):
        @pl.when(l > 0)
        def _():
            x_save(l).start()

        def prep(m, _):
            r = rows_of(m, MU)
            rf = xb[r, :].astype(F32)
            u = (rf * inv_rms(rf)).astype(BF)
            ub[r, :] = u
            vcat[l, :, r] = left_parts(sum_parts(nt(acat[l, 0:32], u)))
            return 0

        lax.fori_loop(0, T // MU, prep, 0)

        def up_chunk(k, _):
            g = 8 * l + k

            def tile(m, _):
                @pl.when(m == 0)
                def _():
                    event0(g)
                    arrive(g)

                @pl.when(m == 2)
                def _():
                    event1(g)

                @pl.when(g * 4 + m - 16 * l >= 2)
                def _():
                    gp_out(l, k, m).wait()

                r = rows_of(m, MU)
                for n in range(4):
                    cols = pl.ds(pl.multiple_of(k * 1024 + n * 256, 256), 256)
                    rhs = w[k, :, n * 64 : (n + 1) * 64, :].reshape(H, 256)
                    pre = nn(ub[r, :], rhs) + tn(vcat[l, :, r], bcat[l, :, cols])
                    act, slope = gelu_and_slope(pre.astype(BF))
                    sd[r, cols] = act
                    gst[lax.rem(m, 2), :, n * 256 : (n + 1) * 256] = slope
                gp_out(l, k, m).start()
                return 0

            lax.fori_loop(0, T // MU, tile, 0)
            release(g)
            return 0

        lax.fori_loop(0, 4, up_chunk, 0)

        @pl.when(l > 0)
        def _():
            x_save(l).wait()

        def down_chunk(k, _):
            g = 8 * l + 4 + k

            def tile(m, _):
                @pl.when(m == 0)
                def _():
                    event0(g)
                    arrive(g)

                @pl.when(m == 1)
                def _():
                    event1(g)

                r = rows_of(m, MD)
                cols = pl.ds(pl.multiple_of(k * 256, 256), 256)
                step = nn(sd[r, :], w[4 + k].reshape(F, 256))
                xb[r, cols] = (xb[r, cols].astype(F32) + step).astype(BF)
                return 0

            lax.fori_loop(0, T // MD, tile, 0)
            release(g)
            return 0

        lax.fori_loop(0, 4, down_chunk, 0)
        return 0

    lax.fori_loop(0, L, forward_layer, 0)


    x_final = pltpu.make_async_copy(xb, xout, io_sem.at[0])
    x_final.start()
    gather(1, L - 1)
    gp_out(L - 1, 3, 2).wait()
    gp_out(L - 1, 3, 3).wait()

    def gp_in(t):
        l = L - 1 - lax.div(t, 16)
        q = quarter(lax.div(lax.rem(t, 16), 4))
        m = lax.rem(t, 4)
        b = lax.rem(m, 2)
        return pltpu.make_async_copy(gp.at[l, q, rows_of(m, MU), :], gst.at[b], gp_sem.at[b])

    gp_in(jnp.int32(0)).start()
    x_final.wait()


    def x_load(l, start):
        @pl.when(l > 0)
        def _():
            cp = pltpu.make_async_copy(xs.at[l - 1], xb, io_sem.at[0])
            cp.start() if start else cp.wait()

        @pl.when(l == 0)
        def _():
            cp = pltpu.make_async_copy(tok, xb, io_sem.at[0])
            cp.start() if start else cp.wait()

    def backward_layer(rl, _):
        l = L - 1 - rl
        x_load(l, True)
        dlt[...] = jnp.zeros_like(dlt)
        gb[...] = jnp.zeros_like(gb)
        ga[...] = jnp.zeros_like(ga)

        def down_step(i, _):
            @pl.when(i == 0)
            def _():
                gather(0, l)

            b_events(1, l, i)
            q = quarter(i)
            cols = pl.ds(pl.multiple_of(q * 1024, 1024), 1024)

            def tile(m, _):
                t = rl * 16 + i * 4 + m

                @pl.when(t + 1 < 16 * L)
                def _():
                    gp_in(t + 1).start()

                gp_in(t).wait()
                r = rows_of(m, MU)
                acc = None
                for k in range(4):
                    rhs = w[4 + k, pl.ds(4 * q, 4)].reshape(1024, 256)
                    term = nt(db[r, k * 256 : (k + 1) * 256], rhs)
                    acc = term if acc is None else acc + term
                d = (acc.astype(BF).astype(F32) * gst[lax.rem(m, 2)]).astype(BF)
                sd[r, cols] = d
                dlt[:, r] += nt(bcat[l, 0:32, cols], d)
                gb[:, cols] += nn(vcat[l, 0:32, r], d)
                return 0

            lax.fori_loop(0, T // MU, tile, 0)
            return 0

        lax.fori_loop(0, 4, down_step, 0)
        b_release(1, l)
        dcat[...] = left_parts(sum_parts(dlt[...]))
        gb8 = sum_parts(gb[...])
        gacc[l, :, 0:2048] = gb8[:, 0:2048] + pltpu.roll(gb8[:, 2048:4096], 4, 0)

        def up_step(i, _):
            @pl.when(jnp.logical_and(i == 0, l > 0))
            def _():
                gather(1, l - 1)

            b_events(0, l, i)
            q = quarter(i)
            cols = pl.ds(pl.multiple_of(q * 256, 256), 256)

            def tile(m, _):
                r = rows_of(m, MD)
                acc = None
                for k in range(4):
                    for n in range(4):
                        rhs = w[k, pl.ds(4 * q, 4), n * 64 : (n + 1) * 64, :].reshape(256, 256)
                        j = 4 * k + n
                        term = nt(sd[r, j * 256 : (j + 1) * 256], rhs)
                        acc = term if acc is None else acc + term
                side = tn(dcat[:, r], acat[l, :, cols]).astype(BF)
                ub[r, cols] = acc.astype(BF) + side
                return 0

            lax.fori_loop(0, T // MD, tile, 0)
            return 0

        lax.fori_loop(0, 4, up_step, 0)
        b_release(0, l)
        x_load(l, False)

        def finish(m, _):
            r = rows_of(m, MU)
            rf = xb[r, :].astype(F32)
            inv = inv_rms(rf)
            dn = ub[r, :].astype(F32)
            dot = jnp.mean(rf * dn, axis=-1, keepdims=True)
            db[r, :] = (db[r, :].astype(F32) + inv * dn - rf * (inv * inv * inv) * dot).astype(BF)
            u = (rf * inv).astype(BF)
            ga[...] += nn(dcat[0:32, r], u)
            return 0

        lax.fori_loop(0, T // MU, finish, 0)
        ga8 = sum_parts(ga[...])
        gacc[l, :, 2048:2560] = ga8[:, 0:512] + pltpu.roll(ga8[:, 512:1024], 4, 0)
        grads_out(l)
        return 0

    lax.fori_loop(0, L, backward_layer, 0)


    g_final = pltpu.make_async_copy(db, gtok, io_sem.at[1])
    g_final.start()
    for l in range(L):
        for i in range(4):

            @pl.when(me != 4 * l + i)
            def _():
                grad_send(jnp.int32(l), i).wait_send()

    others = rbuf.at[pl.ds(0, 15)]
    remote(others, others, rr_sem, rr_sem, partner).wait_recv()
    total = rbuf[0]
    for i in range(1, 16):
        total = total + rbuf[i]
    gall[me] = total

    def share(o, _):
        @pl.when(o != me)
        def _():
            remote(gall.at[me], gall.at[me], as_sem, ar_sem, (lax.rem(o, 4), lax.div(o, 4))).start()

        return 0

    lax.fori_loop(0, 16, share, 0)
    others = gall.at[pl.ds(0, 15)]
    remote(others, others, as_sem, ar_sem, partner).wait_send()
    remote(others, others, as_sem, ar_sem, partner).wait_recv()
    gout[...] = gall[...]
    g_final.wait()


def solution(mesh):
    tok_spec = P(GROUP, None)
    weight_spec = P(None, GROUP, None)

    def device_step(tokens, cotangent, up, down, lora_a, lora_b):
        a8 = jnp.pad(lora_a.transpose(0, 2, 1), ((0, 0), (0, 4), (0, 0)))
        b8 = jnp.pad(lora_b, ((0, 0), (0, 4), (0, 0)))
        hbm = pl.BlockSpec(memory_space=pltpu.HBM)
        vmem = pl.BlockSpec(memory_space=pltpu.VMEM)
        shape = jax.ShapeDtypeStruct
        dma, regular = pltpu.SemaphoreType.DMA, pltpu.SemaphoreType.REGULAR
        outs = pl.pallas_call(
            kernel,
            name="stack",
            out_shape=[
                shape((T, H), BF),
                shape((T, H), BF),
                shape((16, 8, GW), F32),
                shape((L, 4, T, 1024), F32),
                shape((L - 1, T, H), BF),
                shape((L, 8, 4, 256, 256), BF),
            ],
            in_specs=[hbm, hbm, hbm, hbm, vmem, vmem],
            out_specs=[hbm, hbm, vmem, hbm, hbm, hbm],
            scratch_shapes=[
                pltpu.VMEM((8, 16, 256, 256), BF),
                pltpu.VMEM((T, F), BF),
                pltpu.VMEM((T, H), BF),
                pltpu.VMEM((T, H), BF),
                pltpu.VMEM((T, H), BF),
                pltpu.VMEM((2, MU, 1024), F32),
                pltpu.VMEM((L, 48, H), BF),
                pltpu.VMEM((L, 48, F), BF),
                pltpu.VMEM((L, 48, T), BF),
                pltpu.VMEM((48, T), BF),
                pltpu.VMEM((32, T), F32),
                pltpu.VMEM((32, F), F32),
                pltpu.VMEM((32, H), F32),
                pltpu.VMEM((L, 8, 4 * GW), F32),
                pltpu.VMEM((16, 8, GW), F32),
                pltpu.VMEM((16, 8, GW), F32),
                dma((8,)),
                dma((4, 8)),
                dma((4, 8)),
                dma((8,)),
                dma((2,)),
                dma((2,)),
                dma((2,)),
                dma((2, 5)),
                dma((2, 5)),
                dma((L,)),
                dma,
                dma,
                dma,
                regular((4, 8)),
            ],
            compiler_params=pltpu.CompilerParams(vmem_limit_bytes=67000000, has_side_effects=True),
        )(tokens, cotangent, up, down, a8, b8)
        x_out, g_tok, shares = outs[:3]
        grads = shares.reshape(L, 4, 2, 4, GW).transpose(0, 2, 3, 1, 4).reshape(L, 2, 4, 4 * GW)
        grad_b = grads[..., 0:2048].transpose(0, 2, 1, 3).reshape(L, 4, F)
        grad_a = grads[..., 2048:2560].transpose(0, 1, 3, 2).reshape(L, H, 4)
        return x_out, g_tok, grad_a, grad_b

    return jax.shard_map(
        device_step,
        mesh=mesh,
        in_specs=(tok_spec, tok_spec, weight_spec, weight_spec, P(), P()),
        out_specs=(tok_spec, tok_spec, P(), P()),
        check_vma=False,
    )
```

```python
import jax
import jax.numpy as jnp
from jax import lax
from jax.experimental import pallas as pl
from jax.experimental.pallas import tpu as pltpu
from jax.sharding import PartitionSpec as P

GROUP = ("data", "local")
NORM_EPS = 1e-6
BF = jnp.bfloat16
F32 = jnp.float32
C0 = 0.7978845608028654
K0 = 0.044715

T = 2048
H = 1024
F = 4096
L = 4
NG = 8 * L
MU = 512
MD = 1024
MX = 256
RB, CB = 32, 256
ROWS = ((0, 96), (96, 80), (176, 80))
GW = 640


def nn(a, b):
    return lax.dot_general(a, b, (((1,), (0,)), ((), ())), preferred_element_type=F32)


def nt(a, b):
    return lax.dot_general(a, b, (((1,), (1,)), ((), ())), preferred_element_type=F32)


def tn(a, b):
    return lax.dot_general(a, b, (((0,), (0,)), ((), ())), preferred_element_type=F32)


def split3(v):
    p1 = v.astype(BF).astype(F32)
    rest = v - p1
    p2 = rest.astype(BF).astype(F32)
    return p1, p2, (rest - p2).astype(BF).astype(F32)


def left_parts(v):
    p1, p2, p3 = split3(v)
    return jnp.concatenate([p1, p2, p3, p1, p1, p2], axis=0).astype(BF)


def right_parts(v):
    p1, p2, p3 = split3(v)
    return jnp.concatenate([p3, p2, p1, p1, p2, p1], axis=0).astype(BF)


def sum_parts(v):
    return v[0:8] + v[8:16] + v[16:24]


def gelu_and_slope(pre):
    x = pre.astype(F32)
    sq = x * x
    half = 0.5 * jnp.tanh(x * (sq * (C0 * K0) + C0)) + 0.5
    act = x * half
    slope = (act * (1.0 - half)) * (sq * (6.0 * C0 * K0) + 2.0 * C0) + half
    return act.astype(BF), slope


def rows_of(m, size):
    return pl.ds(pl.multiple_of(m * size, size), size)


def kernel(
    tok, cot, up, down, a8, b8,
    xout, gtok, gout, gp, xs, kept,
    w, sd, xb, ub, db, gst, pre0, pre1, acat, bcat, vcat, dcat, dlt, gb, ga, gacc, rbuf, gall,
    own_sem, fs_sem, fr_sem, kept_sem, gp_sem, io_sem, bo_sem, bs_sem, br_sem, rs_sem, rr_sem, as_sem, ar_sem,
    cred,
):
    data = lax.axis_index("data")
    local = lax.axis_index("local")
    x, c = lax.div(data, 2), lax.rem(data, 2)
    z, y = lax.div(local, 2), lax.rem(local, 2)
    me = data * 4 + local
    dx, dy, dz, dc = 1 - 2 * x, 1 - 2 * y, 1 - 2 * z, 1 - 2 * c
    par = lax.rem(x + y + z, 2)

    def quarter(i):
        hi, lo = lax.div(i, 2), lax.rem(i, 2)
        return 2 * (par + hi - 2 * par * hi) + (c + lo - 2 * c * lo)

    q_own, q_miss = quarter(0), quarter(2)

    def pick(dim, a0, a1, a2):
        return lax.div((1 - dim) * (2 - dim), 2) * a0 + dim * (2 - dim) * a1 + lax.div(dim * (dim - 1), 2) * a2

    def device(dim):
        return (local + pick(dim, 0, dy, 2 * dz), data + pick(dim, 2 * dx, 0, 0))

    neighbours = ((local, data + 2 * dx), (local + dy, data), (local + 2 * dz, data), (local, data + dc))
    partner = neighbours[3]

    def remote(src, dst, ssem, rsem, dev):
        return pltpu.make_async_remote_copy(
            src_ref=src, dst_ref=dst, send_sem=ssem, recv_sem=rsem, device_id=dev, device_id_type=pl.DeviceIdType.MESH
        )


    def own_load(g):
        s, l = lax.rem(g, 8), lax.div(g, 8)

        @pl.when(s < 4)
        def _():
            for n in range(4):
                pltpu.make_async_copy(
                    up.at[l, :, pl.ds(pl.multiple_of(s * 1024 + n * 256, 256), 256)],
                    w.at[s, me, pl.ds(n * 64, 64), :],
                    own_sem.at[s],
                ).start()

        @pl.when(s >= 4)
        def _():
            pltpu.make_async_copy(
                down.at[l, :, pl.ds(pl.multiple_of((s - 4) * 256, 256), 256)], w.at[s, me], own_sem.at[s]
            ).start()

    def colour(g):
        q = lax.rem(g + c, 3)
        return q, lax.rem(q + 2, 3), lax.rem(q + 1, 3)

    def delta(dim):
        return pick(dim, 8 * dx, dy, 2 * dz)

    def use_credit(g, dim):
        @pl.when(g >= 8)
        def _():
            pl.semaphore_wait(cred.at[dim, lax.rem(g, 8)], 1)

    def send_blocks(g, phase, dim, blocks, dev):
        s = lax.rem(g, 8)
        use_credit(g, dim)
        for b in blocks:
            remote(w.at[s, b], w.at[s, b], fs_sem.at[phase, s], fr_sem.at[phase, s], dev).start()

    def span(g, phase):
        s = lax.rem(g, 8)
        r = w.at[s, pl.ds(0, (1, 2, 4, 8)[phase])]
        return remote(r, r, fs_sem.at[phase, s], fr_sem.at[phase, s], partner)

    def ready(g):
        return jnp.logical_and(g >= 0, g < NG)

    def first_hop(g):
        d1, _, _ = colour(g)
        s = lax.rem(g, 8)
        pltpu.make_async_copy(w.at[s, me], w.at[s, me], own_sem.at[s]).wait()
        send_blocks(g, 0, d1, (me,), device(d1))

    def event0(r):
        g3, g6 = r + 3, r + 6

        @pl.when(ready(g3))
        def _():
            d1, d2, d3 = colour(g3)
            e1, e2 = delta(d1), delta(d2)
            span(g3, 1).wait_recv()
            send_blocks(g3, 2, d3, (me, me + e1, me + e2, me + e1 + e2), device(d3))

        @pl.when(jnp.logical_and(r >= 0, ready(g6)))
        def _():
            first_hop(g6)

    def event1(r):
        g5, g1 = r + 5, r + 1

        @pl.when(ready(g5))
        def _():
            d1, d2, _ = colour(g5)
            span(g5, 0).wait_recv()
            send_blocks(g5, 1, d2, (me, me + delta(d1)), device(d2))

        @pl.when(ready(g1))
        def _():
            s = lax.rem(g1, 8)
            span(g1, 2).wait_recv()
            use_credit(g1, 3)
            for h in range(2):
                r2 = w.at[s, pl.ds(8 * h + 4 * c, 4)]
                remote(r2, r2, fs_sem.at[3, s], fr_sem.at[3, s], partner).start()

    def keep_copy(g):
        s, l = lax.rem(g, 8), lax.div(g, 8)
        return pltpu.make_async_copy(w.at[s, pl.ds(4 * q_own, 4)], kept.at[l, s], kept_sem.at[s])

    def arrive(g):
        span(g, 3).wait_recv()
        keep_copy(g).start()

    def release(g):
        s = lax.rem(g, 8)
        for phase in range(4):
            span(g, phase).wait_send()
        keep_copy(g).wait()
        for i in range(4):
            pl.semaphore_signal(cred.at[i, s], inc=1, device_id=neighbours[i], device_id_type=pl.DeviceIdType.MESH)

        @pl.when(g + 8 < NG)
        def _():
            own_load(g + 8)


    def whole(m, q):
        return w.at[pl.ds(4 * m, 4), pl.ds(4 * q, 4)]

    def part(ref, dim):
        return ref.at[:, :, pl.ds(*ROWS[dim]), :]

    def b_own(m, l):
        return pltpu.make_async_copy(kept.at[l, pl.ds(4 * m, 4)], whole(m, q_own), bo_sem.at[m])

    def b_send(m, l, i, q):
        src, dst = kept.at[l, pl.ds(4 * m, 4)], whole(m, q)
        if i < 3:
            src, dst = part(src, i), part(dst, i)
        return remote(src, dst, bs_sem.at[m, i], br_sem.at[m, i], neighbours[i])

    def b_forward(m):
        return remote(whole(m, q_miss), whole(m, q_miss), bs_sem.at[m, 4], br_sem.at[m, 4], partner)

    def gather(m, l):
        @pl.when(jnp.logical_or(l < L - 1, m == 0))
        def _():
            b_own(m, l).start()

        for i in range(4):
            for s in range(4):
                pl.semaphore_wait(cred.at[i, 4 * m + s], 1)
            b_send(m, l, i, q_own).start()

    def b_events(m, l, i):
        @pl.when(jnp.logical_and(i == 0, jnp.logical_or(l < L - 1, m == 0)))
        def _():
            b_own(m, l).wait()

        @pl.when(i == 1)
        def _():
            b_send(m, l, 3, quarter(1)).wait_recv()

        @pl.when(i == 2)
        def _():
            for d in range(3):
                b_send(m, l, d, q_miss).wait_recv()
            b_forward(m).start()

        @pl.when(i == 3)
        def _():
            b_forward(m).wait_recv()

    def b_release(m, l):
        b_forward(m).wait_send()
        for i in range(4):
            b_send(m, l, i, q_own).wait_send()

        @pl.when(l > 0)
        def _():
            for i in range(4):
                for s in range(4):
                    pl.semaphore_signal(
                        cred.at[i, 4 * m + s], inc=1, device_id=neighbours[i], device_id_type=pl.DeviceIdType.MESH
                    )


    def grad_send(l, i):
        return remote(
            gacc.at[l, :, pl.ds(i * GW, GW)], rbuf.at[me], rs_sem.at[l], rr_sem, (jnp.int32(i), l)
        )

    def grads_out(l):
        for i in range(4):
            mine = me == 4 * l + i

            @pl.when(jnp.logical_not(mine))
            def _():
                grad_send(l, i).start()

            @pl.when(mine)
            def _():
                rbuf[me] = gacc[l, :, i * GW : (i + 1) * GW]


    tok_in = pltpu.make_async_copy(tok, xb, io_sem.at[0])
    cot_in = pltpu.make_async_copy(cot, db, io_sem.at[1])

    def first_loads(g, _):
        own_load(g)
        return 0

    def first_hops(g, _):
        first_hop(g)
        return 0

    lax.fori_loop(0, 8, first_loads, 0)
    lax.fori_loop(0, 6, first_hops, 0)
    tok_in.start()
    cot_in.start()

    def fill(r, _):
        event0(r)
        event1(r)
        return 0

    for l in range(L):
        acat[l] = right_parts(a8[l])
        bcat[l] = right_parts(b8[l])
    lax.fori_loop(-6, 0, fill, 0)
    tok_in.wait()
    cot_in.wait()


    def inv_rms(rf):
        return lax.rsqrt(jnp.mean(rf * rf, axis=-1, keepdims=True) + NORM_EPS)

    def x_save(l):
        return pltpu.make_async_copy(xb, xs.at[l - 1], io_sem.at[0])

    def slope_out(l, k, m):
        b = lax.rem(m, 2)
        return pltpu.make_async_copy(gst.at[b, pl.ds(0, MX)], gp.at[l, k, rows_of(m, MX), :], gp_sem.at[b])

    blocks = [(rb, cb) for cb in range(0, 1024, CB) for rb in range(0, MX, RB)]

    def activate(src, k, m, slot, part):
        r0, s0 = lax.rem(slot, 2), lax.div(slot, 2) * MX
        for rb, cb in blocks[part * len(blocks) // 5 : (part + 1) * len(blocks) // 5]:
            act, slope = gelu_and_slope(src[rb : rb + RB, cb : cb + CB].astype(BF))
            r = pl.ds(pl.multiple_of(m * MX + rb, RB), RB)
            sd[r, pl.ds(pl.multiple_of(k * 1024 + cb, CB), CB)] = act
            gst[r0, pl.ds(pl.multiple_of(s0 + rb, RB), RB), cb : cb + CB] = slope

    def up_tile(l, k, m, dst, kp, mp, src, slot):
        r = rows_of(m, MX)
        cols = pl.ds(pl.multiple_of(k * 1024, 1024), 1024)
        acc = None
        for kt in range(5):
            if kt < 4:
                rhs = w[k, 4 * kt : 4 * kt + 4]
                rhs = jnp.concatenate([rhs[:, n * 64 : (n + 1) * 64, :].reshape(256, 256) for n in range(4)], axis=1)
                term = nn(ub[r, kt * 256 : (kt + 1) * 256], rhs)
            else:
                term = tn(vcat[l, :, r], bcat[l, :, cols])
            acc = term if acc is None else acc + term
            activate(src, kp, mp, slot, kt)
        dst[...] = acc

    def forward_layer(l, _):
        @pl.when(l > 0)
        def _():
            x_save(l).start()

        def prep(m, _):
            r = rows_of(m, MU)
            rf = xb[r, :].astype(F32)
            u = (rf * inv_rms(rf)).astype(BF)
            ub[r, :] = u
            vcat[l, :, r] = left_parts(sum_parts(nt(acat[l, 0:32], u)))
            return 0

        lax.fori_loop(0, T // MU, prep, 0)

        def up_step(t, _):
            k, m = lax.div(t, 8), lax.rem(t, 8)
            g = 8 * l + k

            @pl.when(m == 0)
            def _():
                event0(g)
                arrive(g)

            @pl.when(m == 4)
            def _():
                event1(g)

            tp = jnp.maximum(t - 1, 0)
            kp, mp = lax.div(tp, 8), lax.rem(tp, 8)

            @pl.when(jnp.logical_and(t > 0, 32 * l + tp >= 2))
            def _():
                slope_out(l, kp, mp).wait()

            slot = jnp.where(t == 0, 2, lax.rem(mp, 2))

            @pl.when(lax.rem(t, 2) == 0)
            def _():
                up_tile(l, k, m, pre0, kp, mp, pre1, slot)

            @pl.when(lax.rem(t, 2) == 1)
            def _():
                up_tile(l, k, m, pre1, kp, mp, pre0, slot)

            @pl.when(t > 0)
            def _():
                slope_out(l, kp, mp).start()

            @pl.when(m == 7)
            def _():
                release(g)

            return 0

        lax.fori_loop(0, 32, up_step, 0)
        last = jnp.int32(7)
        slope_out(l, 3, last).wait()
        for part in range(5):
            activate(pre1, 3, last, jnp.int32(1), part)
        slope_out(l, 3, last).start()

        @pl.when(l > 0)
        def _():
            x_save(l).wait()

        def down_chunk(k, _):
            g = 8 * l + 4 + k

            def tile(m, _):
                @pl.when(m == 0)
                def _():
                    event0(g)
                    arrive(g)

                @pl.when(m == 1)
                def _():
                    event1(g)

                r = rows_of(m, MD)
                cols = pl.ds(pl.multiple_of(k * 256, 256), 256)
                step = nn(sd[r, :], w[4 + k].reshape(F, 256))
                xb[r, cols] = (xb[r, cols].astype(F32) + step).astype(BF)
                return 0

            lax.fori_loop(0, T // MD, tile, 0)
            release(g)
            return 0

        lax.fori_loop(0, 4, down_chunk, 0)
        return 0

    lax.fori_loop(0, L, forward_layer, 0)


    x_final = pltpu.make_async_copy(xb, xout, io_sem.at[0])
    x_final.start()
    gather(1, L - 1)
    slope_out(L - 1, 3, jnp.int32(6)).wait()
    slope_out(L - 1, 3, jnp.int32(7)).wait()

    def gp_in(t):
        l = L - 1 - lax.div(t, 16)
        q = quarter(lax.div(lax.rem(t, 16), 4))
        m = lax.rem(t, 4)
        b = lax.rem(m, 2)
        return pltpu.make_async_copy(gp.at[l, q, rows_of(m, MU), :], gst.at[b], gp_sem.at[b])

    gp_in(jnp.int32(0)).start()
    x_final.wait()


    def x_load(l, start):
        @pl.when(l > 0)
        def _():
            cp = pltpu.make_async_copy(xs.at[l - 1], xb, io_sem.at[0])
            cp.start() if start else cp.wait()

        @pl.when(l == 0)
        def _():
            cp = pltpu.make_async_copy(tok, xb, io_sem.at[0])
            cp.start() if start else cp.wait()

    def backward_layer(rl, _):
        l = L - 1 - rl
        x_load(l, True)
        dlt[...] = jnp.zeros_like(dlt)
        gb[...] = jnp.zeros_like(gb)
        ga[...] = jnp.zeros_like(ga)

        def down_step(i, _):
            @pl.when(i == 0)
            def _():
                gather(0, l)

            b_events(1, l, i)
            q = quarter(i)
            cols = pl.ds(pl.multiple_of(q * 1024, 1024), 1024)

            def tile(m, _):
                t = rl * 16 + i * 4 + m

                @pl.when(t + 1 < 16 * L)
                def _():
                    gp_in(t + 1).start()

                gp_in(t).wait()
                r = rows_of(m, MU)
                acc = None
                for k in range(4):
                    rhs = w[4 + k, pl.ds(4 * q, 4)].reshape(1024, 256)
                    term = nt(db[r, k * 256 : (k + 1) * 256], rhs)
                    acc = term if acc is None else acc + term
                d = (acc.astype(BF).astype(F32) * gst[lax.rem(m, 2)]).astype(BF)
                sd[r, cols] = d
                dlt[:, r] += nt(bcat[l, 0:32, cols], d)
                gb[:, cols] += nn(vcat[l, 0:32, r], d)
                return 0

            lax.fori_loop(0, T // MU, tile, 0)
            return 0

        lax.fori_loop(0, 4, down_step, 0)
        b_release(1, l)
        dcat[...] = left_parts(sum_parts(dlt[...]))
        gb8 = sum_parts(gb[...])
        gacc[l, :, 0:2048] = gb8[:, 0:2048] + pltpu.roll(gb8[:, 2048:4096], 4, 0)

        def up_step(i, _):
            @pl.when(jnp.logical_and(i == 0, l > 0))
            def _():
                gather(1, l - 1)

            b_events(0, l, i)
            q = quarter(i)
            cols = pl.ds(pl.multiple_of(q * 256, 256), 256)

            def tile(m, _):
                r = rows_of(m, MD)
                acc = None
                for k in range(4):
                    for n in range(4):
                        rhs = w[k, pl.ds(4 * q, 4), n * 64 : (n + 1) * 64, :].reshape(256, 256)
                        j = 4 * k + n
                        term = nt(sd[r, j * 256 : (j + 1) * 256], rhs)
                        acc = term if acc is None else acc + term
                side = tn(dcat[:, r], acat[l, :, cols]).astype(BF)
                ub[r, cols] = acc.astype(BF) + side
                return 0

            lax.fori_loop(0, T // MD, tile, 0)
            return 0

        lax.fori_loop(0, 4, up_step, 0)
        b_release(0, l)
        x_load(l, False)

        def finish(m, _):
            r = rows_of(m, MU)
            rf = xb[r, :].astype(F32)
            inv = inv_rms(rf)
            dn = ub[r, :].astype(F32)
            dot = jnp.mean(rf * dn, axis=-1, keepdims=True)
            db[r, :] = (db[r, :].astype(F32) + inv * dn - rf * ((inv * inv * inv) * dot)).astype(BF)
            u = (rf * inv).astype(BF)
            ga[...] += nn(dcat[0:32, r], u)
            return 0

        lax.fori_loop(0, T // MU, finish, 0)
        ga8 = sum_parts(ga[...])
        gacc[l, :, 2048:2560] = ga8[:, 0:512] + pltpu.roll(ga8[:, 512:1024], 4, 0)
        grads_out(l)
        return 0

    lax.fori_loop(0, L, backward_layer, 0)


    g_final = pltpu.make_async_copy(db, gtok, io_sem.at[1])
    g_final.start()
    for l in range(L):
        for i in range(4):

            @pl.when(me != 4 * l + i)
            def _():
                grad_send(jnp.int32(l), i).wait_send()

    others = rbuf.at[pl.ds(0, 15)]
    remote(others, others, rr_sem, rr_sem, partner).wait_recv()
    total = rbuf[0]
    for i in range(1, 16):
        total = total + rbuf[i]
    gall[me] = total

    def share(o, _):
        @pl.when(o != me)
        def _():
            remote(gall.at[me], gall.at[me], as_sem, ar_sem, (lax.rem(o, 4), lax.div(o, 4))).start()

        return 0

    lax.fori_loop(0, 16, share, 0)
    others = gall.at[pl.ds(0, 15)]
    remote(others, others, as_sem, ar_sem, partner).wait_send()
    remote(others, others, as_sem, ar_sem, partner).wait_recv()
    gout[...] = gall[...]
    g_final.wait()


def solution(mesh):
    tok_spec = P(GROUP, None)
    weight_spec = P(None, GROUP, None)

    def device_step(tokens, cotangent, up, down, lora_a, lora_b):
        a8 = jnp.pad(lora_a.transpose(0, 2, 1), ((0, 0), (0, 4), (0, 0)))
        b8 = jnp.pad(lora_b, ((0, 0), (0, 4), (0, 0)))
        hbm = pl.BlockSpec(memory_space=pltpu.HBM)
        vmem = pl.BlockSpec(memory_space=pltpu.VMEM)
        shape = jax.ShapeDtypeStruct
        dma, regular = pltpu.SemaphoreType.DMA, pltpu.SemaphoreType.REGULAR
        outs = pl.pallas_call(
            kernel,
            name="stack",
            out_shape=[
                shape((T, H), BF),
                shape((T, H), BF),
                shape((16, 8, GW), F32),
                shape((L, 4, T, 1024), F32),
                shape((L - 1, T, H), BF),
                shape((L, 8, 4, 256, 256), BF),
            ],
            in_specs=[hbm, hbm, hbm, hbm, vmem, vmem],
            out_specs=[hbm, hbm, vmem, hbm, hbm, hbm],
            scratch_shapes=[
                pltpu.VMEM((8, 16, 256, 256), BF),
                pltpu.VMEM((T, F), BF),
                pltpu.VMEM((T, H), BF),
                pltpu.VMEM((T, H), BF),
                pltpu.VMEM((T, H), BF),
                pltpu.VMEM((2, MU, 1024), F32),
                pltpu.VMEM((MX, 1024), F32),
                pltpu.VMEM((MX, 1024), F32),
                pltpu.VMEM((L, 48, H), BF),
                pltpu.VMEM((L, 48, F), BF),
                pltpu.VMEM((L, 48, T), BF),
                pltpu.VMEM((48, T), BF),
                pltpu.VMEM((32, T), F32),
                pltpu.VMEM((32, F), F32),
                pltpu.VMEM((32, H), F32),
                pltpu.VMEM((L, 8, 4 * GW), F32),
                pltpu.VMEM((16, 8, GW), F32),
                pltpu.VMEM((16, 8, GW), F32),
                dma((8,)),
                dma((4, 8)),
                dma((4, 8)),
                dma((8,)),
                dma((2,)),
                dma((2,)),
                dma((2,)),
                dma((2, 5)),
                dma((2, 5)),
                dma((L,)),
                dma,
                dma,
                dma,
                regular((4, 8)),
            ],
            compiler_params=pltpu.CompilerParams(
                vmem_limit_bytes=67000000,
                has_side_effects=True,
            ),
        )(tokens, cotangent, up, down, a8, b8)
        x_out, g_tok, shares = outs[:3]
        grads = shares.reshape(L, 4, 2, 4, GW).transpose(0, 2, 3, 1, 4).reshape(L, 2, 4, 4 * GW)
        grad_b = grads[..., 0:2048].transpose(0, 2, 1, 3).reshape(L, 4, F)
        grad_a = grads[..., 2048:2560].transpose(0, 1, 3, 2).reshape(L, H, 4)
        return x_out, g_tok, grad_a, grad_b

    return jax.shard_map(
        device_step,
        mesh=mesh,
        in_specs=(tok_spec, tok_spec, weight_spec, weight_spec, P(), P()),
        out_specs=(tok_spec, tok_spec, P(), P()),
        check_vma=False,
    )
```

```python
import jax
import jax.numpy as jnp
from jax import lax
from jax.experimental import pallas as pl
from jax.experimental.pallas import tpu as pltpu
from jax.sharding import PartitionSpec as P

GROUP = ("data", "local")
NORM_EPS = 1e-6
BF = jnp.bfloat16
F32 = jnp.float32
C0 = 0.7978845608028654
K0 = 0.044715

T = 2048
H = 1024
F = 4096
L = 4
NG = 8 * L
MU = 512
MD = 1024
MX = 256
RB, CB = 32, 256
ROWS = ((0, 96), (96, 80), (176, 80))
GW = 640


def nn(a, b):
    return lax.dot_general(a, b, (((1,), (0,)), ((), ())), preferred_element_type=F32)


def nt(a, b):
    return lax.dot_general(a, b, (((1,), (1,)), ((), ())), preferred_element_type=F32)


def tn(a, b):
    return lax.dot_general(a, b, (((0,), (0,)), ((), ())), preferred_element_type=F32)


def split3(v):
    p1 = v.astype(BF).astype(F32)
    rest = v - p1
    p2 = rest.astype(BF).astype(F32)
    return p1, p2, (rest - p2).astype(BF).astype(F32)


def left_parts(v):
    p1, p2, p3 = split3(v)
    return jnp.concatenate([p1, p2, p3, p1, p1, p2], axis=0).astype(BF)


def right_parts(v):
    p1, p2, p3 = split3(v)
    return jnp.concatenate([p3, p2, p1, p1, p2, p1], axis=0).astype(BF)


def sum_parts(v):
    return v[0:8] + v[8:16] + v[16:24]


def gelu_and_slope(pre):
    x = pre.astype(F32)
    sq = x * x
    half = 0.5 * jnp.tanh(x * (sq * (C0 * K0) + C0)) + 0.5
    act = x * half
    slope = (act * (1.0 - half)) * (sq * (6.0 * C0 * K0) + 2.0 * C0) + half
    return act.astype(BF), slope


def rows_of(m, size):
    return pl.ds(pl.multiple_of(m * size, size), size)


def kernel(
    tok, cot, up, down, a8, b4,
    xout, gtok, gout, gp, xs, kept,
    w, sd, xb, ub, db, gst, pre0, pre1, acat, bcat, vcat, dcat, dlt, gb, ga, gacc, rbuf, gall,
    own_sem, fs_sem, fr_sem, kept_sem, gp_sem, io_sem, bo_sem, bs_sem, br_sem, rs_sem, rr_sem, as_sem, ar_sem,
    cred,
):
    data = lax.axis_index("data")
    local = lax.axis_index("local")
    x, c = lax.div(data, 2), lax.rem(data, 2)
    z, y = lax.div(local, 2), lax.rem(local, 2)
    me = data * 4 + local
    dx, dy, dz, dc = 1 - 2 * x, 1 - 2 * y, 1 - 2 * z, 1 - 2 * c
    par = lax.rem(x + y + z, 2)

    def quarter(i):
        hi, lo = lax.div(i, 2), lax.rem(i, 2)
        return 2 * (par + hi - 2 * par * hi) + (c + lo - 2 * c * lo)

    q_own, q_miss = quarter(0), quarter(2)

    def pick(dim, a0, a1, a2):
        return lax.div((1 - dim) * (2 - dim), 2) * a0 + dim * (2 - dim) * a1 + lax.div(dim * (dim - 1), 2) * a2

    def device(dim):
        return (local + pick(dim, 0, dy, 2 * dz), data + pick(dim, 2 * dx, 0, 0))

    neighbours = ((local, data + 2 * dx), (local + dy, data), (local + 2 * dz, data), (local, data + dc))
    partner = neighbours[3]

    def remote(src, dst, ssem, rsem, dev):
        return pltpu.make_async_remote_copy(
            src_ref=src, dst_ref=dst, send_sem=ssem, recv_sem=rsem, device_id=dev, device_id_type=pl.DeviceIdType.MESH
        )


    def own_load(g):
        s, l = lax.rem(g, 8), lax.div(g, 8)

        @pl.when(s < 4)
        def _():
            for n in range(4):
                pltpu.make_async_copy(
                    up.at[l, :, pl.ds(pl.multiple_of(s * 1024 + n * 256, 256), 256)],
                    w.at[s, me, pl.ds(n * 64, 64), :],
                    own_sem.at[s],
                ).start()

        @pl.when(s >= 4)
        def _():
            pltpu.make_async_copy(
                down.at[l, :, pl.ds(pl.multiple_of((s - 4) * 256, 256), 256)], w.at[s, me], own_sem.at[s]
            ).start()

    def colour(g):
        q = lax.rem(g + c, 3)
        return q, lax.rem(q + 1, 3), lax.rem(q + 2, 3)

    def delta(dim):
        return pick(dim, 8 * dx, dy, 2 * dz)

    def use_credit(g, dim):
        @pl.when(g >= 8)
        def _():
            pl.semaphore_wait(cred.at[dim, lax.rem(g, 8)], 1)

    def send_blocks(g, phase, dim, blocks, dev):
        s = lax.rem(g, 8)
        use_credit(g, dim)
        for b in blocks:
            remote(w.at[s, b], w.at[s, b], fs_sem.at[phase, s], fr_sem.at[phase, s], dev).start()

    def span(g, phase):
        s = lax.rem(g, 8)
        r = w.at[s, pl.ds(0, (1, 2, 4, 8)[phase])]
        return remote(r, r, fs_sem.at[phase, s], fr_sem.at[phase, s], partner)

    def ready(g):
        return jnp.logical_and(g >= 0, g < NG)

    def hop1(g):
        d1, _, _ = colour(g)
        s = lax.rem(g, 8)
        pltpu.make_async_copy(w.at[s, me], w.at[s, me], own_sem.at[s]).wait()
        send_blocks(g, 0, d1, (me,), device(d1))

    def hop2(g):
        d1, d2, _ = colour(g)
        span(g, 0).wait_recv()
        send_blocks(g, 1, d2, (me, me + delta(d1)), device(d2))

    def hop3(g):
        d1, d2, d3 = colour(g)
        e1, e2 = delta(d1), delta(d2)
        span(g, 1).wait_recv()
        send_blocks(g, 2, d3, (me, me + e1, me + e2, me + e1 + e2), device(d3))

    def hand_over(g):
        s = lax.rem(g, 8)
        span(g, 2).wait_recv()
        use_credit(g, 3)
        for h in range(2):
            r2 = w.at[s, pl.ds(8 * h + 4 * c, 4)]
            remote(r2, r2, fs_sem.at[3, s], fr_sem.at[3, s], partner).start()

    def event(j):
        for step, ahead in ((hand_over, 1), (hop2, 5), (hop3, 3), (hop1, 7)):

            @pl.when(j + ahead < NG)
            def _():
                with jax.named_scope("st"):
                    step(j + ahead)

    def keep_copy(g):
        s, l = lax.rem(g, 8), lax.div(g, 8)
        return pltpu.make_async_copy(w.at[s, pl.ds(4 * q_own, 4)], kept.at[l, s], kept_sem.at[s])

    def arrive(g):
        span(g, 3).wait_recv()
        keep_copy(g).start()

    def release(g):
        s = lax.rem(g, 8)
        for phase in range(4):
            span(g, phase).wait_send()
        keep_copy(g).wait()
        for i in range(4):
            pl.semaphore_signal(cred.at[i, s], inc=1, device_id=neighbours[i], device_id_type=pl.DeviceIdType.MESH)

        @pl.when(g + 8 < NG)
        def _():
            own_load(g + 8)


    def whole(m, q):
        return w.at[pl.ds(4 * m, 4), pl.ds(4 * q, 4)]

    def part(ref, dim):
        return ref.at[:, :, pl.ds(*ROWS[dim]), :]

    def b_own(m, l):
        return pltpu.make_async_copy(kept.at[l, pl.ds(4 * m, 4)], whole(m, q_own), bo_sem.at[m])

    def b_send(m, l, i, q):
        src, dst = kept.at[l, pl.ds(4 * m, 4)], whole(m, q)
        if i < 3:
            src, dst = part(src, i), part(dst, i)
        return remote(src, dst, bs_sem.at[m, i], br_sem.at[m, i], neighbours[i])

    def b_forward(m):
        return remote(whole(m, q_miss), whole(m, q_miss), bs_sem.at[m, 4], br_sem.at[m, 4], partner)

    def gather(m, l):
        @pl.when(jnp.logical_or(l < L - 1, m == 0))
        def _():
            b_own(m, l).start()

        for i in range(4):
            for s in range(4):
                pl.semaphore_wait(cred.at[i, 4 * m + s], 1)
            b_send(m, l, i, q_own).start()

    def b_events(m, l, i):
        @pl.when(jnp.logical_and(i == 0, jnp.logical_or(l < L - 1, m == 0)))
        def _():
            b_own(m, l).wait()

        @pl.when(i == 1)
        def _():
            b_send(m, l, 3, quarter(1)).wait_recv()

        @pl.when(i == 2)
        def _():
            for d in range(3):
                b_send(m, l, d, q_miss).wait_recv()
            b_forward(m).start()

        @pl.when(i == 3)
        def _():
            b_forward(m).wait_recv()

    def b_release(m, l):
        b_forward(m).wait_send()
        for i in range(4):
            b_send(m, l, i, q_own).wait_send()

        @pl.when(l > 0)
        def _():
            for i in range(4):
                for s in range(4):
                    pl.semaphore_signal(
                        cred.at[i, 4 * m + s], inc=1, device_id=neighbours[i], device_id_type=pl.DeviceIdType.MESH
                    )


    def grad_send(l, i):
        return remote(
            gacc.at[l, :, pl.ds(i * GW, GW)], rbuf.at[me], rs_sem.at[l], rr_sem, (jnp.int32(i), l)
        )

    def grads_out(l):
        for i in range(4):
            mine = me == 4 * l + i

            @pl.when(jnp.logical_not(mine))
            def _():
                grad_send(l, i).start()

            @pl.when(mine)
            def _():
                rbuf[me] = gacc[l, :, i * GW : (i + 1) * GW]


    tok_in = pltpu.make_async_copy(tok, xb, io_sem.at[0])
    cot_in = pltpu.make_async_copy(cot, db, io_sem.at[1])

    def first_loads(g, _):
        own_load(g)
        return 0

    lax.fori_loop(0, 8, first_loads, 0)
    tok_in.start()
    cot_in.start()
    at = jnp.int32
    with jax.named_scope("hop1"):
        hop1(at(0))
    for l in range(L):
        acat[l] = right_parts(a8[l])
        bcat[l] = right_parts(jnp.concatenate([b4[l], jnp.zeros((4, F), F32)], axis=0))
    with jax.named_scope("hop2"):
        hop2(at(0))
    with jax.named_scope("hop1"):
        hop1(at(1))
    with jax.named_scope("hop1"):
        hop1(at(2))
    with jax.named_scope("tw"):
        tok_in.wait()
    cot_in.wait()


    def inv_rms(rf):
        return lax.rsqrt(jnp.mean(rf * rf, axis=-1, keepdims=True) + NORM_EPS)

    def x_save(l):
        return pltpu.make_async_copy(xb, xs.at[l - 1], io_sem.at[0])

    def slope_out(l, k, m):
        b = lax.rem(m, 2)
        return pltpu.make_async_copy(gst.at[b, pl.ds(0, MX)], gp.at[l, k, rows_of(m, MX), :], gp_sem.at[b])

    blocks = [(rb, cb) for cb in range(0, 1024, CB) for rb in range(0, MX, RB)]

    def activate(src, k, m, slot, part):
        r0, s0 = lax.rem(slot, 2), lax.div(slot, 2) * MX
        for rb, cb in blocks[part * len(blocks) // 5 : (part + 1) * len(blocks) // 5]:
            act, slope = gelu_and_slope(src[rb : rb + RB, cb : cb + CB].astype(BF))
            r = pl.ds(pl.multiple_of(m * MX + rb, RB), RB)
            sd[r, pl.ds(pl.multiple_of(k * 1024 + cb, CB), CB)] = act
            gst[r0, pl.ds(pl.multiple_of(s0 + rb, RB), RB), cb : cb + CB] = slope

    def up_tile(l, k, m, dst, kp, mp, src, slot):
        r = rows_of(m, MX)
        cols = pl.ds(pl.multiple_of(k * 1024, 1024), 1024)
        acc = None
        for kt in range(5):
            if kt < 4:
                rhs = w[k, 4 * kt : 4 * kt + 4]
                rhs = jnp.concatenate([rhs[:, n * 64 : (n + 1) * 64, :].reshape(256, 256) for n in range(4)], axis=1)
                term = nn(ub[r, kt * 256 : (kt + 1) * 256], rhs)
            else:
                term = tn(vcat[l, :, r], bcat[l, :, cols])
            acc = term if acc is None else acc + term
            activate(src, kp, mp, slot, kt)
        dst[...] = acc

    def forward_layer(l, _):
        @pl.when(l > 0)
        def _():
            x_save(l).start()

        def prep(m, _):
            r = rows_of(m, MU)
            rf = xb[r, :].astype(F32)
            u = (rf * inv_rms(rf)).astype(BF)
            ub[r, :] = u
            vcat[l, :, r] = left_parts(sum_parts(nt(acat[l, 0:32], u)))
            return 0

        @pl.when(l == 0)
        def _():
            with jax.named_scope("hop3"):
                hop3(at(0))

        with jax.named_scope("prep"):
            lax.fori_loop(0, T // MU, prep, 0)

        @pl.when(l == 0)
        def _():
            with jax.named_scope("hop2"):
                hop2(at(1))
            with jax.named_scope("hop1"):
                hop1(at(3))
            with jax.named_scope("hop2"):
                hop2(at(2))
            with jax.named_scope("hand_over"):
                hand_over(at(0))
            with jax.named_scope("hop3"):
                hop3(at(1))
            with jax.named_scope("hop1"):
                hop1(at(4))
            with jax.named_scope("hop2"):
                hop2(at(3))

        def up_step(t, _):
            k, m = lax.div(t, 8), lax.rem(t, 8)
            g = 8 * l + k

            @pl.when(lax.rem(t, 7) == 5)
            def _():
                with jax.named_scope("ev"):
                    event(8 * l + lax.div(t, 7))

            @pl.when(jnp.logical_and(l == 0, t == 2))
            def _():
                with jax.named_scope("hop3"):
                    hop3(at(2))
                with jax.named_scope("hop1"):
                    hop1(at(5))
                with jax.named_scope("hop2"):
                    hop2(at(4))
                with jax.named_scope("hop1"):
                    hop1(at(6))

            @pl.when(m == 0)
            def _():
                with jax.named_scope("arr"):
                    arrive(g)

            tp = jnp.maximum(t - 1, 0)
            kp, mp = lax.div(tp, 8), lax.rem(tp, 8)

            @pl.when(jnp.logical_and(t > 0, 32 * l + tp >= 2))
            def _():
                with jax.named_scope("sw"):
                    slope_out(l, kp, mp).wait()

            slot = jnp.where(t == 0, 2, lax.rem(mp, 2))

            @pl.when(lax.rem(t, 2) == 0)
            def _():
                with jax.named_scope("up"):
                    up_tile(l, k, m, pre0, kp, mp, pre1, slot)

            @pl.when(lax.rem(t, 2) == 1)
            def _():
                with jax.named_scope("up"):
                    up_tile(l, k, m, pre1, kp, mp, pre0, slot)

            @pl.when(t > 0)
            def _():
                slope_out(l, kp, mp).start()

            @pl.when(m == 7)
            def _():
                with jax.named_scope("rel"):
                    release(g)

            return 0

        lax.fori_loop(0, 32, up_step, 0)
        last = jnp.int32(7)
        slope_out(l, 3, last).wait()
        for part in range(5):
            activate(pre1, 3, last, jnp.int32(1), part)
        slope_out(l, 3, last).start()

        @pl.when(l > 0)
        def _():
            x_save(l).wait()

        def down_step(t, _):
            k, m = lax.div(t, 2), lax.rem(t, 2)
            g = 8 * l + 4 + k

            @pl.when(m == 1)
            def _():
                with jax.named_scope("ev"):
                    event(g)

            @pl.when(m == 0)
            def _():
                with jax.named_scope("arr"):
                    arrive(g)

            r = rows_of(m, MD)
            cols = pl.ds(pl.multiple_of(k * 256, 256), 256)
            with jax.named_scope("dn"):
                step = nn(sd[r, :], w[4 + k].reshape(F, 256))
                xb[r, cols] = (xb[r, cols].astype(F32) + step).astype(BF)

            @pl.when(m == 1)
            def _():
                with jax.named_scope("rel"):
                    release(g)

            return 0

        lax.fori_loop(0, 8, down_step, 0)
        return 0

    lax.fori_loop(0, L, forward_layer, 0)


    x_final = pltpu.make_async_copy(xb, xout, io_sem.at[0])
    x_final.start()
    with jax.named_scope("gat"):
        gather(1, L - 1)
    slope_out(L - 1, 3, jnp.int32(6)).wait()
    slope_out(L - 1, 3, jnp.int32(7)).wait()

    def gp_in(t):
        l = L - 1 - lax.div(t, 16)
        q = quarter(lax.div(lax.rem(t, 16), 4))
        m = lax.rem(t, 4)
        b = lax.rem(m, 2)
        return pltpu.make_async_copy(gp.at[l, q, rows_of(m, MU), :], gst.at[b], gp_sem.at[b])

    gp_in(jnp.int32(0)).start()
    x_final.wait()


    def x_load(l, start):
        @pl.when(l > 0)
        def _():
            cp = pltpu.make_async_copy(xs.at[l - 1], xb, io_sem.at[0])
            cp.start() if start else cp.wait()

        @pl.when(l == 0)
        def _():
            cp = pltpu.make_async_copy(tok, xb, io_sem.at[0])
            cp.start() if start else cp.wait()

    def backward_layer(rl, _):
        l = L - 1 - rl
        dlt[...] = jnp.zeros_like(dlt)
        gb[...] = jnp.zeros_like(gb)
        ga[...] = jnp.zeros_like(ga)

        def down_step(i, _):
            @pl.when(i == 1)
            def _():
                with jax.named_scope("gat"):
                    gather(0, l)

            @pl.when(i == 2)
            def _():
                x_load(l, True)

            with jax.named_scope("bev"):
                b_events(1, l, i)
            q = quarter(i)
            cols = pl.ds(pl.multiple_of(q * 1024, 1024), 1024)

            def tile(m, _):
                t = rl * 16 + i * 4 + m

                @pl.when(t + 1 < 16 * L)
                def _():
                    gp_in(t + 1).start()

                gp_in(t).wait()
                r = rows_of(m, MU)
                acc = None
                for k in range(4):
                    rhs = w[4 + k, pl.ds(4 * q, 4)].reshape(1024, 256)
                    term = nt(db[r, k * 256 : (k + 1) * 256], rhs)
                    acc = term if acc is None else acc + term
                d = (acc.astype(BF).astype(F32) * gst[lax.rem(m, 2)]).astype(BF)
                sd[r, cols] = d
                dlt[:, r] += nt(bcat[l, 0:32, cols], d)
                gb[:, cols] += nn(vcat[l, 0:32, r], d)
                return 0

            with jax.named_scope("p1"):
                lax.fori_loop(0, T // MU, tile, 0)
            return 0

        lax.fori_loop(0, 4, down_step, 0)
        with jax.named_scope("brel"):
            b_release(1, l)
        dcat[...] = left_parts(sum_parts(dlt[...]))
        gb8 = sum_parts(gb[...])
        gacc[l, :, 0:2048] = gb8[:, 0:2048] + pltpu.roll(gb8[:, 2048:4096], 4, 0)

        def up_step(i, _):
            @pl.when(jnp.logical_and(i == 1, l > 0))
            def _():
                with jax.named_scope("gat"):
                    gather(1, l - 1)

            with jax.named_scope("bev"):
                b_events(0, l, i)
            q = quarter(i)
            cols = pl.ds(pl.multiple_of(q * 256, 256), 256)

            def tile(m, _):
                r = rows_of(m, MD)
                acc = None
                for k in range(4):
                    for n in range(4):
                        rhs = w[k, pl.ds(4 * q, 4), n * 64 : (n + 1) * 64, :].reshape(256, 256)
                        j = 4 * k + n
                        term = nt(sd[r, j * 256 : (j + 1) * 256], rhs)
                        acc = term if acc is None else acc + term
                side = tn(dcat[:, r], acat[l, :, cols]).astype(BF)
                ub[r, cols] = acc.astype(BF) + side
                return 0

            with jax.named_scope("p2"):
                lax.fori_loop(0, T // MD, tile, 0)
            return 0

        lax.fori_loop(0, 4, up_step, 0)
        with jax.named_scope("brel"):
            b_release(0, l)
        x_load(l, False)

        def finish(m, _):
            r = rows_of(m, MU)
            rf = xb[r, :].astype(F32)
            inv = inv_rms(rf)
            dn = ub[r, :].astype(F32)
            dot = jnp.mean(rf * dn, axis=-1, keepdims=True)
            db[r, :] = (db[r, :].astype(F32) + inv * dn - rf * ((inv * inv * inv) * dot)).astype(BF)
            u = (rf * inv).astype(BF)
            ga[...] += nn(dcat[0:32, r], u)
            return 0

        with jax.named_scope("fin"):
            lax.fori_loop(0, T // MU, finish, 0)
        ga8 = sum_parts(ga[...])
        gacc[l, :, 2048:2560] = ga8[:, 0:512] + pltpu.roll(ga8[:, 512:1024], 4, 0)
        with jax.named_scope("gout"):
            grads_out(l)
        return 0

    lax.fori_loop(0, L, backward_layer, 0)


    g_final = pltpu.make_async_copy(db, gtok, io_sem.at[1])
    g_final.start()
    for l in range(L):
        for i in range(4):

            @pl.when(me != 4 * l + i)
            def _():
                grad_send(jnp.int32(l), i).wait_send()

    others = rbuf.at[pl.ds(0, 15)]
    with jax.named_scope("redw"):
        remote(others, others, rr_sem, rr_sem, partner).wait_recv()
    total = rbuf[0]
    for i in range(1, 16):
        total = total + rbuf[i]
    gall[me] = total

    def share(o, _):
        @pl.when(o != me)
        def _():
            remote(gall.at[me], gall.at[me], as_sem, ar_sem, (lax.rem(o, 4), lax.div(o, 4))).start()

        return 0

    lax.fori_loop(0, 16, share, 0)
    others = gall.at[pl.ds(0, 15)]
    with jax.named_scope("allw"):
        remote(others, others, as_sem, ar_sem, partner).wait_send()
        remote(others, others, as_sem, ar_sem, partner).wait_recv()
    gout[...] = gall[...]
    g_final.wait()


def solution(mesh):
    tok_spec = P(GROUP, None)
    weight_spec = P(None, GROUP, None)

    def device_step(tokens, cotangent, up, down, lora_a, lora_b):
        a8 = jnp.pad(lora_a.transpose(0, 2, 1), ((0, 0), (0, 4), (0, 0)))
        hbm = pl.BlockSpec(memory_space=pltpu.HBM)
        vmem = pl.BlockSpec(memory_space=pltpu.VMEM)
        shape = jax.ShapeDtypeStruct
        dma, regular = pltpu.SemaphoreType.DMA, pltpu.SemaphoreType.REGULAR
        outs = pl.pallas_call(
            kernel,
            name="stack",
            out_shape=[
                shape((T, H), BF),
                shape((T, H), BF),
                shape((16, 8, GW), F32),
                shape((L, 4, T, 1024), F32),
                shape((L - 1, T, H), BF),
                shape((L, 8, 4, 256, 256), BF),
            ],
            in_specs=[hbm, hbm, hbm, hbm, vmem, vmem],
            out_specs=[hbm, hbm, vmem, hbm, hbm, hbm],
            scratch_shapes=[
                pltpu.VMEM((8, 16, 256, 256), BF),
                pltpu.VMEM((T, F), BF),
                pltpu.VMEM((T, H), BF),
                pltpu.VMEM((T, H), BF),
                pltpu.VMEM((T, H), BF),
                pltpu.VMEM((2, MU, 1024), F32),
                pltpu.VMEM((MX, 1024), F32),
                pltpu.VMEM((MX, 1024), F32),
                pltpu.VMEM((L, 48, H), BF),
                pltpu.VMEM((L, 48, F), BF),
                pltpu.VMEM((L, 48, T), BF),
                pltpu.VMEM((48, T), BF),
                pltpu.VMEM((32, T), F32),
                pltpu.VMEM((32, F), F32),
                pltpu.VMEM((32, H), F32),
                pltpu.VMEM((L, 8, 4 * GW), F32),
                pltpu.VMEM((16, 8, GW), F32),
                pltpu.VMEM((16, 8, GW), F32),
                dma((8,)),
                dma((4, 8)),
                dma((4, 8)),
                dma((8,)),
                dma((2,)),
                dma((2,)),
                dma((2,)),
                dma((2, 5)),
                dma((2, 5)),
                dma((L,)),
                dma,
                dma,
                dma,
                regular((4, 8)),
            ],
            compiler_params=pltpu.CompilerParams(
                vmem_limit_bytes=67000000,
                has_side_effects=True,
            ),
        )(tokens, cotangent, up, down, a8, lora_b)
        x_out, g_tok, shares = outs[:3]
        grads = shares.reshape(L, 4, 2, 4, GW).transpose(0, 2, 3, 1, 4).reshape(L, 2, 4, 4 * GW)
        grad_b = grads[..., 0:2048].transpose(0, 2, 1, 3).reshape(L, 4, F)
        grad_a = grads[..., 2048:2560].transpose(0, 1, 3, 2).reshape(L, H, 4)
        return x_out, g_tok, grad_a, grad_b

    return jax.shard_map(
        device_step,
        mesh=mesh,
        in_specs=(tok_spec, tok_spec, weight_spec, weight_spec, P(), P()),
        out_specs=(tok_spec, tok_spec, P(), P()),
        check_vma=False,
    )
```

```python
import jax
import jax.numpy as jnp
from jax import lax
from jax.experimental import pallas as pl
from jax.experimental.pallas import tpu as pltpu
from jax.sharding import PartitionSpec as P

GROUP = ("data", "local")
NORM_EPS = 1e-6
BF = jnp.bfloat16
F32 = jnp.float32
C0 = 0.7978845608028654
K0 = 0.044715

T = 2048
H = 1024
F = 4096
L = 4
NG = 8 * L
MU = 512
MD = 1024
MX = 256
RB, CB = 32, 256
ROWS = ((0, 96), (96, 80), (176, 80))
GW = 640


def nn(a, b):
    return lax.dot_general(a, b, (((1,), (0,)), ((), ())), preferred_element_type=F32)


def nt(a, b):
    return lax.dot_general(a, b, (((1,), (1,)), ((), ())), preferred_element_type=F32)


def tn(a, b):
    return lax.dot_general(a, b, (((0,), (0,)), ((), ())), preferred_element_type=F32)


def split3(v):
    p1 = v.astype(BF).astype(F32)
    rest = v - p1
    p2 = rest.astype(BF).astype(F32)
    return p1, p2, (rest - p2).astype(BF).astype(F32)


def left_parts(v):
    p1, p2, p3 = split3(v)
    return jnp.concatenate([p1, p2, p3, p1, p1, p2], axis=0).astype(BF)


def right_parts(v):
    p1, p2, p3 = split3(v)
    return jnp.concatenate([p3, p2, p1, p1, p2, p1], axis=0).astype(BF)


def sum_parts(v):
    return v[0:8] + v[8:16] + v[16:24]


def gelu_and_slope(pre):
    x = pre.astype(F32)
    sq = x * x
    half = 0.5 * jnp.tanh(x * (sq * (C0 * K0) + C0)) + 0.5
    act = x * half
    slope = (act * (1.0 - half)) * (sq * (6.0 * C0 * K0) + 2.0 * C0) + half
    return act.astype(BF), slope


def rem3(t):
    return t - 3 * lax.div(t * 43, 128)


def rows_of(m, size):
    return pl.ds(pl.multiple_of(m * size, size), size)


def kernel(
    tok, cot, up, down, a4, b4,
    xout, gtok, gout, gp, xs, kept,
    w, sd, xb, ub, db, gst, pre0, pre1, acat, bcat, vcat, dcat, dlt, gb, ga, gacc, rbuf, gall,
    own_sem, fs_sem, fr_sem, kept_sem, gp_sem, io_sem, bo_sem, bs_sem, br_sem, rs_sem, rr_sem, as_sem, ar_sem,
    cred,
):
    data = lax.axis_index("data")
    local = lax.axis_index("local")
    x, c = lax.div(data, 2), lax.rem(data, 2)
    z, y = lax.div(local, 2), lax.rem(local, 2)
    me = data * 4 + local
    dx, dy, dz, dc = 1 - 2 * x, 1 - 2 * y, 1 - 2 * z, 1 - 2 * c
    par = lax.rem(x + y + z, 2)

    def quarter(i):
        hi, lo = lax.div(i, 2), lax.rem(i, 2)
        return 2 * (par + hi - 2 * par * hi) + (c + lo - 2 * c * lo)

    q_own, q_miss = quarter(0), quarter(2)

    def pick(dim, a0, a1, a2):
        return lax.div((1 - dim) * (2 - dim), 2) * a0 + dim * (2 - dim) * a1 + lax.div(dim * (dim - 1), 2) * a2

    def device(dim):
        return (local + pick(dim, 0, dy, 2 * dz), data + pick(dim, 2 * dx, 0, 0))

    neighbours = ((local, data + 2 * dx), (local + dy, data), (local + 2 * dz, data), (local, data + dc))
    partner = neighbours[3]

    def remote(src, dst, ssem, rsem, dev):
        return pltpu.make_async_remote_copy(
            src_ref=src, dst_ref=dst, send_sem=ssem, recv_sem=rsem, device_id=dev, device_id_type=pl.DeviceIdType.MESH
        )


    def own_load(g):
        s, l = lax.rem(g, 8), lax.div(g, 8)

        @pl.when(s < 4)
        def _():
            for n in range(4):
                pltpu.make_async_copy(
                    up.at[l, :, pl.ds(pl.multiple_of(s * 1024 + n * 256, 256), 256)],
                    w.at[s, me, pl.ds(n * 64, 64), :],
                    own_sem.at[s],
                ).start()

        @pl.when(s >= 4)
        def _():
            pltpu.make_async_copy(
                down.at[l, :, pl.ds(pl.multiple_of((s - 4) * 256, 256), 256)], w.at[s, me], own_sem.at[s]
            ).start()

    def colour(g):
        q = rem3(2 * g + c)
        return q, rem3(q + 1), rem3(q + 2)

    def delta(dim):
        return pick(dim, 8 * dx, dy, 2 * dz)

    def use_credit(g, dim):
        @pl.when(g >= 8)
        def _():
            pl.semaphore_wait(cred.at[dim, lax.rem(g, 8)], 1)

    def send_blocks(g, phase, dim, blocks, dev):
        s = lax.rem(g, 8)
        use_credit(g, dim)
        for b in blocks:
            remote(w.at[s, b], w.at[s, b], fs_sem.at[phase, s], fr_sem.at[phase, s], dev).start()

    def span(g, phase):
        s = lax.rem(g, 8)
        r = w.at[s, pl.ds(0, (1, 2, 4, 8)[phase])]
        return remote(r, r, fs_sem.at[phase, s], fr_sem.at[phase, s], partner)

    def ready(g):
        return jnp.logical_and(g >= 0, g < NG)

    def hop1(g):
        d1, _, _ = colour(g)
        s = lax.rem(g, 8)
        pltpu.make_async_copy(w.at[s, me], w.at[s, me], own_sem.at[s]).wait()
        send_blocks(g, 0, d1, (me,), device(d1))

    def hop2(g):
        d1, d2, _ = colour(g)
        span(g, 0).wait_recv()
        send_blocks(g, 1, d2, (me, me + delta(d1)), device(d2))

    def hop3(g):
        d1, d2, d3 = colour(g)
        e1, e2 = delta(d1), delta(d2)
        span(g, 1).wait_recv()
        send_blocks(g, 2, d3, (me, me + e1, me + e2, me + e1 + e2), device(d3))

    def hand_over(g):
        s = lax.rem(g, 8)
        span(g, 2).wait_recv()
        use_credit(g, 3)
        for h in range(2):
            r2 = w.at[s, pl.ds(8 * h + 4 * c, 4)]
            remote(r2, r2, fs_sem.at[3, s], fr_sem.at[3, s], partner).start()

    def event(j):
        for step, ahead in ((hand_over, 1), (hop2, 4), (hop3, 3), (hop1, 5)):

            @pl.when(j + ahead < NG)
            def _():
                with jax.named_scope("st"):
                    step(j + ahead)

    def keep_copy(g):
        s, l = lax.rem(g, 8), lax.div(g, 8)
        return pltpu.make_async_copy(w.at[s, pl.ds(4 * q_own, 4)], kept.at[l, s], kept_sem.at[s])

    def arrive(g):
        span(g, 3).wait_recv()
        keep_copy(g).start()

    def release(g):
        s = lax.rem(g, 8)
        for phase in range(4):
            span(g, phase).wait_send()
        keep_copy(g).wait()
        for i in range(4):
            pl.semaphore_signal(cred.at[i, s], inc=1, device_id=neighbours[i], device_id_type=pl.DeviceIdType.MESH)

        @pl.when(g + 8 < NG)
        def _():
            own_load(g + 8)


    def whole(m, q):
        return w.at[pl.ds(4 * m, 4), pl.ds(4 * q, 4)]

    def part(ref, dim):
        return ref.at[:, :, pl.ds(*ROWS[dim]), :]

    def b_own(m, l):
        return pltpu.make_async_copy(kept.at[l, pl.ds(4 * m, 4)], whole(m, q_own), bo_sem.at[m])

    def b_send(m, l, i, q):
        src, dst = kept.at[l, pl.ds(4 * m, 4)], whole(m, q)
        if i < 3:
            src, dst = part(src, i), part(dst, i)
        return remote(src, dst, bs_sem.at[m, i], br_sem.at[m, i], neighbours[i])

    def b_forward(m):
        return remote(whole(m, q_miss), whole(m, q_miss), bs_sem.at[m, 4], br_sem.at[m, 4], partner)

    def gather(m, l):
        @pl.when(jnp.logical_or(l < L - 1, m == 0))
        def _():
            b_own(m, l).start()

        for i in range(4):
            for s in range(4):
                pl.semaphore_wait(cred.at[i, 4 * m + s], 1)
            b_send(m, l, i, q_own).start()

    def b_events(m, l, i):
        @pl.when(jnp.logical_and(i == 0, jnp.logical_or(l < L - 1, m == 0)))
        def _():
            b_own(m, l).wait()

        @pl.when(i == 1)
        def _():
            b_send(m, l, 3, quarter(1)).wait_recv()

        @pl.when(i == 2)
        def _():
            for d in range(3):
                b_send(m, l, d, q_miss).wait_recv()
            b_forward(m).start()

        @pl.when(i == 3)
        def _():
            b_forward(m).wait_recv()

    def b_release(m, l):
        b_forward(m).wait_send()
        for i in range(4):
            b_send(m, l, i, q_own).wait_send()

        @pl.when(l > 0)
        def _():
            for i in range(4):
                for s in range(4):
                    pl.semaphore_signal(
                        cred.at[i, 4 * m + s], inc=1, device_id=neighbours[i], device_id_type=pl.DeviceIdType.MESH
                    )


    def grad_send(l, i):
        return remote(
            gacc.at[l, :, pl.ds(i * GW, GW)], rbuf.at[me], rs_sem.at[l], rr_sem, (jnp.int32(i), l)
        )

    def grads_out(l):
        for i in range(4):
            mine = me == 4 * l + i

            @pl.when(jnp.logical_not(mine))
            def _():
                grad_send(l, i).start()

            @pl.when(mine)
            def _():
                rbuf[me] = gacc[l, :, i * GW : (i + 1) * GW]


    tok_in = pltpu.make_async_copy(tok, xb, io_sem.at[0])
    cot_in = pltpu.make_async_copy(cot, db, io_sem.at[1])

    def first_loads(g, _):
        own_load(g)
        return 0

    lax.fori_loop(0, 8, first_loads, 0)
    tok_in.start()
    cot_in.start()
    at = jnp.int32
    with jax.named_scope("hop1"):
        hop1(at(0))
    with jax.named_scope("hop1"):
        hop1(at(1))
    for b in range(2):
        pltpu.make_async_copy(gst.at[b, pl.ds(0, MX)], gp.at[4 * L, pl.ds(b * MX, MX), :], gp_sem.at[b]).start()
    for l in range(L):
        acat[l] = right_parts(jnp.concatenate([a4[l], jnp.zeros((4, H), F32)], axis=0))
        bcat[l] = right_parts(jnp.concatenate([b4[l], jnp.zeros((4, F), F32)], axis=0))
    with jax.named_scope("hop2"):
        hop2(at(0))
    with jax.named_scope("hop1"):
        hop1(at(2))
    with jax.named_scope("hop2"):
        hop2(at(1))
    with jax.named_scope("tw"):
        tok_in.wait()
    cot_in.wait()


    def inv_rms(rf):
        return lax.rsqrt(jnp.mean(rf * rf, axis=-1, keepdims=True) + NORM_EPS)

    def x_save(l):
        return pltpu.make_async_copy(xb, xs.at[l - 1], io_sem.at[0])

    def slope_out(b, lk, m):
        return pltpu.make_async_copy(gst.at[b, pl.ds(0, MX)], gp.at[lk, rows_of(m, MX), :], gp_sem.at[b])

    blocks = [(rb, cb) for cb in range(0, 1024, CB) for rb in range(0, MX, RB)]

    def activate(src, k, m, slot, part):
        for rb, cb in blocks[part * len(blocks) // 5 : (part + 1) * len(blocks) // 5]:
            act, slope = gelu_and_slope(src[rb : rb + RB, cb : cb + CB].astype(BF))
            r = pl.ds(pl.multiple_of(m * MX + rb, RB), RB)
            sd[r, pl.ds(pl.multiple_of(k * 1024 + cb, CB), CB)] = act
            gst[slot, rb : rb + RB, cb : cb + CB] = slope

    def up_tile(l, k, m, dst, kp, mp, src, slot):
        r = rows_of(m, MX)
        cols = pl.ds(pl.multiple_of(k * 1024, 1024), 1024)
        acc = None
        for kt in range(5):
            if kt < 4:
                rhs = w[k, 4 * kt : 4 * kt + 4]
                rhs = jnp.concatenate([rhs[:, n * 64 : (n + 1) * 64, :].reshape(256, 256) for n in range(4)], axis=1)
                term = nn(ub[r, kt * 256 : (kt + 1) * 256], rhs)
            else:
                term = tn(vcat[l, :, r], bcat[l, :, cols])
            acc = term if acc is None else acc + term
            activate(src, kp, mp, slot, kt)
        dst[...] = acc

    def forward_layer(l, _):
        @pl.when(l > 0)
        def _():
            x_save(l).start()

        def prep(m, _):
            r = rows_of(m, MU)
            rf = xb[r, :].astype(F32)
            u = (rf * inv_rms(rf)).astype(BF)
            ub[r, :] = u
            vcat[l, :, r] = left_parts(sum_parts(nt(acat[l, 0:32], u)))
            return 0

        @pl.when(l == 0)
        def _():
            with jax.named_scope("hop3"):
                hop3(at(0))

        with jax.named_scope("prep"):
            lax.fori_loop(0, T // MU, prep, 0)

        @pl.when(l == 0)
        def _():
            with jax.named_scope("hop1"):
                hop1(at(3))
            with jax.named_scope("hop2"):
                hop2(at(2))
            with jax.named_scope("hop3"):
                hop3(at(1))
            with jax.named_scope("hand_over"):
                hand_over(at(0))

        def slopes(t):
            slot = rem3(t)
            old = jnp.maximum(t - 2, 0)
            lk = jnp.where(t == 1, 4 * L, 4 * l + lax.div(old, 8))
            lk = jnp.where(t == 0, jnp.where(l == 0, 4 * L, 4 * l - 1), lk)
            m = jnp.where(t == 0, 7, jnp.where(t == 1, 2, lax.rem(old, 8)))
            slope_out(jnp.where(slot == 0, 2, slot - 1), lk, m).start()
            slope_out(slot, 0, 0).wait()
            return slot

        def up_step(t, _):
            k, m = lax.div(t, 8), lax.rem(t, 8)
            g = 8 * l + k

            due = [t == at(i) for i in (5, 12, 19, 26)]
            due = jnp.logical_or(jnp.logical_or(due[0], due[1]), jnp.logical_or(due[2], due[3]))

            @pl.when(jnp.logical_or(m == 0, jnp.logical_or(due, t == 3)))
            def _():
                @pl.when(m == 0)
                def _():
                    @pl.when(k > 0)
                    def _():
                        release(g - 1)

                    with jax.named_scope("arr"):
                        arrive(g)

                @pl.when(due)
                def _():
                    with jax.named_scope("ev"):
                        event(8 * l + lax.div(t, 7))

                @pl.when(jnp.logical_and(l == 0, t == 3))
                def _():
                    with jax.named_scope("hop3"):
                        hop3(at(2))
                    with jax.named_scope("hop2"):
                        hop2(at(3))
                    with jax.named_scope("hop1"):
                        hop1(at(4))

            tp = jnp.maximum(t - 1, 0)
            kp, mp = lax.div(tp, 8), lax.rem(tp, 8)
            slot = slopes(t)

            @pl.when(lax.rem(t, 2) == 0)
            def _():
                with jax.named_scope("up"):
                    up_tile(l, k, m, pre0, kp, mp, pre1, slot)

            @pl.when(lax.rem(t, 2) == 1)
            def _():
                with jax.named_scope("up"):
                    up_tile(l, k, m, pre1, kp, mp, pre0, slot)

            return 0

        lax.fori_loop(0, 32, up_step, 0)
        release(8 * l + 3)
        slot = slopes(at(32))
        for part in range(5):
            activate(pre1, 3, at(7), slot, part)

        @pl.when(l > 0)
        def _():
            x_save(l).wait()

        def down_step(t, _):
            k, m = lax.div(t, 2), lax.rem(t, 2)
            g = 8 * l + 4 + k

            @pl.when(m == 0)
            def _():
                @pl.when(k > 0)
                def _():
                    release(g - 1)

                with jax.named_scope("arr"):
                    arrive(g)

            @pl.when(m == 1)
            def _():
                with jax.named_scope("ev"):
                    event(g)

            r = rows_of(m, MD)
            cols = pl.ds(pl.multiple_of(k * 256, 256), 256)
            with jax.named_scope("dn"):
                step = nn(sd[r, :], w[4 + k].reshape(F, 256))
                xb[r, cols] = (xb[r, cols].astype(F32) + step).astype(BF)
            return 0

        lax.fori_loop(0, 8, down_step, 0)
        release(8 * l + 7)
        return 0

    lax.fori_loop(0, L, forward_layer, 0)


    x_final = pltpu.make_async_copy(xb, xout, io_sem.at[0])
    x_final.start()
    with jax.named_scope("gat"):
        gather(1, L - 1)
    slope_out(2, 4 * L - 1, at(7)).start()
    for b in range(3):
        slope_out(b, 0, at(0)).wait()

    def gp_in(t):
        lk = 4 * (L - 1 - lax.div(t, 16)) + quarter(lax.div(lax.rem(t, 16), 4))
        b = rem3(t)
        return pltpu.make_async_copy(gp.at[lk, rows_of(lax.rem(t, 4), MU), :], gst.at[b], gp_sem.at[b])

    gp_in(at(0)).start()
    gp_in(at(1)).start()
    x_final.wait()


    def x_load(l, start):
        @pl.when(l > 0)
        def _():
            cp = pltpu.make_async_copy(xs.at[l - 1], xb, io_sem.at[0])
            cp.start() if start else cp.wait()

        @pl.when(l == 0)
        def _():
            cp = pltpu.make_async_copy(tok, xb, io_sem.at[0])
            cp.start() if start else cp.wait()

    def backward_layer(rl, _):
        l = L - 1 - rl
        dlt[...] = jnp.zeros_like(dlt)
        gb[...] = jnp.zeros_like(gb)
        ga[...] = jnp.zeros_like(ga)

        def down_step(i, _):
            @pl.when(i == 1)
            def _():
                with jax.named_scope("gat"):
                    gather(0, l)

            @pl.when(i == 2)
            def _():
                x_load(l, True)

            with jax.named_scope("bev"):
                b_events(1, l, i)
            q = quarter(i)
            cols = pl.ds(pl.multiple_of(q * 1024, 1024), 1024)

            def tile(m, _):
                t = rl * 16 + i * 4 + m

                @pl.when(t + 2 < 16 * L)
                def _():
                    gp_in(t + 2).start()

                gp_in(t).wait()
                r = rows_of(m, MU)
                acc = None
                for k in range(4):
                    rhs = w[4 + k, pl.ds(4 * q, 4)].reshape(1024, 256)
                    term = nt(db[r, k * 256 : (k + 1) * 256], rhs)
                    acc = term if acc is None else acc + term
                d = (acc.astype(BF).astype(F32) * gst[rem3(t)]).astype(BF)
                sd[r, cols] = d
                dlt[:, r] += nt(bcat[l, 0:32, cols], d)
                gb[:, cols] += nn(vcat[l, 0:32, r], d)
                return 0

            with jax.named_scope("p1"):
                lax.fori_loop(0, T // MU, tile, 0)
            return 0

        lax.fori_loop(0, 4, down_step, 0)
        with jax.named_scope("brel"):
            b_release(1, l)
        dcat[...] = left_parts(sum_parts(dlt[...]))
        gb8 = sum_parts(gb[...])
        gacc[l, :, 0:2048] = gb8[:, 0:2048] + pltpu.roll(gb8[:, 2048:4096], 4, 0)

        def up_step(i, _):
            @pl.when(jnp.logical_and(i == 1, l > 0))
            def _():
                with jax.named_scope("gat"):
                    gather(1, l - 1)

            with jax.named_scope("bev"):
                b_events(0, l, i)
            q = quarter(i)
            cols = pl.ds(pl.multiple_of(q * 256, 256), 256)

            def tile(m, _):
                r = rows_of(m, MD)
                acc = None
                for k in range(4):
                    for n in range(4):
                        rhs = w[k, pl.ds(4 * q, 4), n * 64 : (n + 1) * 64, :].reshape(256, 256)
                        j = 4 * k + n
                        term = nt(sd[r, j * 256 : (j + 1) * 256], rhs)
                        acc = term if acc is None else acc + term
                side = tn(dcat[:, r], acat[l, :, cols]).astype(BF)
                ub[r, cols] = acc.astype(BF) + side
                return 0

            with jax.named_scope("p2"):
                lax.fori_loop(0, T // MD, tile, 0)
            return 0

        lax.fori_loop(0, 4, up_step, 0)
        with jax.named_scope("brel"):
            b_release(0, l)
        x_load(l, False)

        def finish(m, _):
            r = rows_of(m, MU)
            rf = xb[r, :].astype(F32)
            inv = inv_rms(rf)
            dn = ub[r, :].astype(F32)
            dot = jnp.mean(rf * dn, axis=-1, keepdims=True)
            db[r, :] = (db[r, :].astype(F32) + inv * dn - rf * ((inv * inv * inv) * dot)).astype(BF)
            u = (rf * inv).astype(BF)
            ga[...] += nn(dcat[0:32, r], u)
            return 0

        with jax.named_scope("fin"):
            lax.fori_loop(0, T // MU, finish, 0)
        ga8 = sum_parts(ga[...])
        gacc[l, :, 2048:2560] = ga8[:, 0:512] + pltpu.roll(ga8[:, 512:1024], 4, 0)
        with jax.named_scope("gout"):
            grads_out(l)
        return 0

    lax.fori_loop(0, L, backward_layer, 0)


    g_final = pltpu.make_async_copy(db, gtok, io_sem.at[1])
    g_final.start()
    for l in range(L):
        for i in range(4):

            @pl.when(me != 4 * l + i)
            def _():
                grad_send(jnp.int32(l), i).wait_send()

    others = rbuf.at[pl.ds(0, 15)]
    with jax.named_scope("redw"):
        remote(others, others, rr_sem, rr_sem, partner).wait_recv()
    total = rbuf[0]
    for i in range(1, 16):
        total = total + rbuf[i]
    gall[me] = total

    def share(o, _):
        @pl.when(o != me)
        def _():
            remote(gall.at[me], gall.at[me], as_sem, ar_sem, (lax.rem(o, 4), lax.div(o, 4))).start()

        return 0

    lax.fori_loop(0, 16, share, 0)
    others = gall.at[pl.ds(0, 15)]
    with jax.named_scope("allw"):
        remote(others, others, as_sem, ar_sem, partner).wait_send()
        remote(others, others, as_sem, ar_sem, partner).wait_recv()
    gout[...] = gall[...]
    g_final.wait()


def solution(mesh):
    tok_spec = P(GROUP, None)
    weight_spec = P(None, GROUP, None)

    def device_step(tokens, cotangent, up, down, lora_a, lora_b):
        hbm = pl.BlockSpec(memory_space=pltpu.HBM)
        vmem = pl.BlockSpec(memory_space=pltpu.VMEM)
        shape = jax.ShapeDtypeStruct
        dma, regular = pltpu.SemaphoreType.DMA, pltpu.SemaphoreType.REGULAR
        outs = pl.pallas_call(
            kernel,
            name="stack",
            out_shape=[
                shape((T, H), BF),
                shape((T, H), BF),
                shape((16, 8, GW), F32),
                shape((4 * L + 1, T, 1024), F32),
                shape((L - 1, T, H), BF),
                shape((L, 8, 4, 256, 256), BF),
            ],
            in_specs=[hbm, hbm, hbm, hbm, vmem, vmem],
            out_specs=[hbm, hbm, vmem, hbm, hbm, hbm],
            scratch_shapes=[
                pltpu.VMEM((8, 16, 256, 256), BF),
                pltpu.VMEM((T, F), BF),
                pltpu.VMEM((T, H), BF),
                pltpu.VMEM((T, H), BF),
                pltpu.VMEM((T, H), BF),
                pltpu.VMEM((3, MU, 1024), F32),
                pltpu.VMEM((MX, 1024), F32),
                pltpu.VMEM((MX, 1024), F32),
                pltpu.VMEM((L, 48, H), BF),
                pltpu.VMEM((L, 48, F), BF),
                pltpu.VMEM((L, 48, T), BF),
                pltpu.VMEM((48, T), BF),
                pltpu.VMEM((32, T), F32),
                pltpu.VMEM((32, F), F32),
                pltpu.VMEM((32, H), F32),
                pltpu.VMEM((L, 8, 4 * GW), F32),
                pltpu.VMEM((16, 8, GW), F32),
                pltpu.VMEM((16, 8, GW), F32),
                dma((8,)),
                dma((4, 8)),
                dma((4, 8)),
                dma((8,)),
                dma((3,)),
                dma((2,)),
                dma((2,)),
                dma((2, 5)),
                dma((2, 5)),
                dma((L,)),
                dma,
                dma,
                dma,
                regular((4, 8)),
            ],
            compiler_params=pltpu.CompilerParams(
                vmem_limit_bytes=67000000,
                has_side_effects=True,
            ),
        )(tokens, cotangent, up, down, lora_a.transpose(0, 2, 1), lora_b)
        x_out, g_tok, shares = outs[:3]
        grads = shares.reshape(L, 4, 2, 4, GW).transpose(0, 2, 3, 1, 4).reshape(L, 2, 4, 4 * GW)
        grad_b = grads[..., 0:2048].transpose(0, 2, 1, 3).reshape(L, 4, F)
        grad_a = grads[..., 2048:2560].transpose(0, 1, 3, 2).reshape(L, H, 4)
        return x_out, g_tok, grad_a, grad_b

    return jax.shard_map(
        device_step,
        mesh=mesh,
        in_specs=(tok_spec, tok_spec, weight_spec, weight_spec, P(), P()),
        out_specs=(tok_spec, tok_spec, P(), P()),
        check_vma=False,
    )
```

```python
import jax
import jax.numpy as jnp
from jax import lax
from jax.experimental import pallas as pl
from jax.experimental.pallas import tpu as pltpu
from jax.sharding import PartitionSpec as P

GROUP = ("data", "local")
NORM_EPS = 1e-6
BF = jnp.bfloat16
F32 = jnp.float32
C0 = 0.7978845608028654
K0 = 0.044715

T = 2048
H = 1024
F = 4096
L = 4
NG = 8 * L
MU = 512
MD = 1024
MX = 256
RB, CB = 32, 256
ROWS = ((0, 96), (96, 80), (176, 80))
GW = 640


def nn(a, b):
    return lax.dot_general(a, b, (((1,), (0,)), ((), ())), preferred_element_type=F32)


def nt(a, b):
    return lax.dot_general(a, b, (((1,), (1,)), ((), ())), preferred_element_type=F32)


def tn(a, b):
    return lax.dot_general(a, b, (((0,), (0,)), ((), ())), preferred_element_type=F32)


def split3(v):
    p1 = v.astype(BF).astype(F32)
    rest = v - p1
    p2 = rest.astype(BF).astype(F32)
    return p1, p2, (rest - p2).astype(BF).astype(F32)


def left_parts(v):
    p1, p2, p3 = split3(v)
    return jnp.concatenate([p1, p2, p3, p1, p1, p2], axis=0).astype(BF)


def right_parts(v):
    p1, p2, p3 = split3(v)
    return jnp.concatenate([p3, p2, p1, p1, p2, p1], axis=0).astype(BF)


def sum_parts(v):
    return v[0:8] + v[8:16] + v[16:24]


def gelu_and_slope(pre):
    x = pre.astype(F32)
    sq = x * x
    half = 0.5 * jnp.tanh(x * (sq * (C0 * K0) + C0)) + 0.5
    act = x * half
    slope = (act * (1.0 - half)) * (sq * (6.0 * C0 * K0) + 2.0 * C0) + half
    return act.astype(BF), slope


def rem3(t):
    return t - 3 * lax.div(t * 43, 128)


def rows_of(m, size):
    return pl.ds(pl.multiple_of(m * size, size), size)


def kernel(
    tok, cot, up, down, a4, b4,
    xout, gtok, gout, gp, xs, kept,
    w, sd, xb, ub, db, gst, pre0, pre1, acat, bcat, vcat, dcat, dlt, gb, ga, gacc, rbuf, gall,
    own_sem, fs_sem, fr_sem, kept_sem, gp_sem, io_sem, bo_sem, bs_sem, br_sem, rs_sem, rr_sem, as_sem, ar_sem,
    cred,
):
    data = lax.axis_index("data")
    local = lax.axis_index("local")
    x, c = lax.div(data, 2), lax.rem(data, 2)
    z, y = lax.div(local, 2), lax.rem(local, 2)
    me = data * 4 + local
    dx, dy, dz, dc = 1 - 2 * x, 1 - 2 * y, 1 - 2 * z, 1 - 2 * c
    par = lax.rem(x + y + z, 2)

    def quarter(i):
        hi, lo = lax.div(i, 2), lax.rem(i, 2)
        return 2 * (par + hi - 2 * par * hi) + (c + lo - 2 * c * lo)

    q_own, q_miss = quarter(0), quarter(2)

    def pick(dim, a0, a1, a2):
        return lax.div((1 - dim) * (2 - dim), 2) * a0 + dim * (2 - dim) * a1 + lax.div(dim * (dim - 1), 2) * a2

    def device(dim):
        return (local + pick(dim, 0, dy, 2 * dz), data + pick(dim, 2 * dx, 0, 0))

    neighbours = ((local, data + 2 * dx), (local + dy, data), (local + 2 * dz, data), (local, data + dc))
    partner = neighbours[3]

    def remote(src, dst, ssem, rsem, dev):
        return pltpu.make_async_remote_copy(
            src_ref=src, dst_ref=dst, send_sem=ssem, recv_sem=rsem, device_id=dev, device_id_type=pl.DeviceIdType.MESH
        )


    def own_load(g):
        s, l = lax.rem(g, 8), lax.div(g, 8)

        @pl.when(s < 4)
        def _():
            for n in range(4):
                pltpu.make_async_copy(
                    up.at[l, :, pl.ds(pl.multiple_of(s * 1024 + n * 256, 256), 256)],
                    w.at[s, me, pl.ds(n * 64, 64), :],
                    own_sem.at[s],
                ).start()

        @pl.when(s >= 4)
        def _():
            pltpu.make_async_copy(
                down.at[l, :, pl.ds(pl.multiple_of((s - 4) * 256, 256), 256)], w.at[s, me], own_sem.at[s]
            ).start()

    def colour(g):
        q = rem3(jnp.where(g < 3, 2 * g, g) + c)
        return q, rem3(q + 1), rem3(q + 2)

    def delta(dim):
        return pick(dim, 8 * dx, dy, 2 * dz)

    def use_credit(g, dim):
        @pl.when(g >= 8)
        def _():
            pl.semaphore_wait(cred.at[dim, lax.rem(g, 8)], 1)

    def send_blocks(g, phase, dim, blocks, dev):
        s = lax.rem(g, 8)
        use_credit(g, dim)
        for b in blocks:
            remote(w.at[s, b], w.at[s, b], fs_sem.at[phase, s], fr_sem.at[phase, s], dev).start()

    def span(g, phase):
        s = lax.rem(g, 8)
        r = w.at[s, pl.ds(0, (1, 2, 4, 8)[phase])]
        return remote(r, r, fs_sem.at[phase, s], fr_sem.at[phase, s], partner)

    def ready(g):
        return jnp.logical_and(g >= 0, g < NG)

    def hop1(g):
        d1, _, _ = colour(g)
        s = lax.rem(g, 8)
        pltpu.make_async_copy(w.at[s, me], w.at[s, me], own_sem.at[s]).wait()
        send_blocks(g, 0, d1, (me,), device(d1))

    def hop2(g):
        d1, d2, _ = colour(g)
        span(g, 0).wait_recv()
        send_blocks(g, 1, d2, (me, me + delta(d1)), device(d2))

    def hop3(g):
        d1, d2, d3 = colour(g)
        e1, e2 = delta(d1), delta(d2)
        span(g, 1).wait_recv()
        send_blocks(g, 2, d3, (me, me + e1, me + e2, me + e1 + e2), device(d3))

    def hand_over(g):
        s = lax.rem(g, 8)
        span(g, 2).wait_recv()
        use_credit(g, 3)
        for h in range(2):
            r2 = w.at[s, pl.ds(8 * h + 4 * c, 4)]
            remote(r2, r2, fs_sem.at[3, s], fr_sem.at[3, s], partner).start()

    def event(j):
        for step, ahead in ((hand_over, 1), (hop2, 5), (hop3, 3)):

            @pl.when(j + ahead < NG)
            def _():
                with jax.named_scope("st"):
                    step(j + ahead)

    def refill(j):
        @pl.when(j + 7 < NG)
        def _():
            hop1(j + 7)

    def keep_copy(g):
        s, l = lax.rem(g, 8), lax.div(g, 8)
        return pltpu.make_async_copy(w.at[s, pl.ds(4 * q_own, 4)], kept.at[l, s], kept_sem.at[s])

    def arrive(g):
        span(g, 3).wait_recv()
        keep_copy(g).start()

    def release(g):
        s = lax.rem(g, 8)
        for phase in range(4):
            span(g, phase).wait_send()
        keep_copy(g).wait()
        for i in range(4):
            pl.semaphore_signal(cred.at[i, s], inc=1, device_id=neighbours[i], device_id_type=pl.DeviceIdType.MESH)

        @pl.when(g + 8 < NG)
        def _():
            own_load(g + 8)


    def whole(m, q):
        return w.at[pl.ds(4 * m, 4), pl.ds(4 * q, 4)]

    def part(ref, dim):
        return ref.at[:, :, pl.ds(*ROWS[dim]), :]

    def b_own(m, l):
        return pltpu.make_async_copy(kept.at[l, pl.ds(4 * m, 4)], whole(m, q_own), bo_sem.at[m])

    def b_send(m, l, i, q):
        src, dst = kept.at[l, pl.ds(4 * m, 4)], whole(m, q)
        if i < 3:
            src, dst = part(src, i), part(dst, i)
        return remote(src, dst, bs_sem.at[m, i], br_sem.at[m, i], neighbours[i])

    def b_forward(m):
        return remote(whole(m, q_miss), whole(m, q_miss), bs_sem.at[m, 4], br_sem.at[m, 4], partner)

    def gather(m, l):
        @pl.when(jnp.logical_or(l < L - 1, m == 0))
        def _():
            b_own(m, l).start()

        for i in range(4):
            for s in range(4):
                pl.semaphore_wait(cred.at[i, 4 * m + s], 1)
            b_send(m, l, i, q_own).start()

    def b_events(m, l, i):
        @pl.when(jnp.logical_and(i == 0, jnp.logical_or(l < L - 1, m == 0)))
        def _():
            b_own(m, l).wait()

        @pl.when(i == 1)
        def _():
            b_send(m, l, 3, quarter(1)).wait_recv()

        @pl.when(i == 2)
        def _():
            for d in range(3):
                b_send(m, l, d, q_miss).wait_recv()
            b_forward(m).start()

        @pl.when(i == 3)
        def _():
            b_forward(m).wait_recv()

    def b_release(m, l):
        b_forward(m).wait_send()
        for i in range(4):
            b_send(m, l, i, q_own).wait_send()

        @pl.when(l > 0)
        def _():
            for i in range(4):
                for s in range(4):
                    pl.semaphore_signal(
                        cred.at[i, 4 * m + s], inc=1, device_id=neighbours[i], device_id_type=pl.DeviceIdType.MESH
                    )


    def grad_send(l, i):
        return remote(
            gacc.at[l, :, pl.ds(i * GW, GW)], rbuf.at[me], rs_sem.at[l], rr_sem, (jnp.int32(i), l)
        )

    def grads_out(l):
        for i in range(4):
            mine = me == 4 * l + i

            @pl.when(jnp.logical_not(mine))
            def _():
                grad_send(l, i).start()

            @pl.when(mine)
            def _():
                rbuf[me] = gacc[l, :, i * GW : (i + 1) * GW]


    tok_in = pltpu.make_async_copy(tok, xb, io_sem.at[0])
    cot_in = pltpu.make_async_copy(cot, db, io_sem.at[1])

    def first_loads(g, _):
        own_load(g)
        return 0

    lax.fori_loop(0, 8, first_loads, 0)
    tok_in.start()
    cot_in.start()
    at = jnp.int32
    with jax.named_scope("hop1"):
        hop1(at(0))
    with jax.named_scope("hop1"):
        hop1(at(1))
    for b in range(2):
        pltpu.make_async_copy(gst.at[b, pl.ds(0, MX)], gp.at[4 * L, pl.ds(b * MX, MX), :], gp_sem.at[b]).start()
    for l in range(L):
        acat[l] = right_parts(jnp.concatenate([a4[l], jnp.zeros((4, H), F32)], axis=0))
        bcat[l] = right_parts(jnp.concatenate([b4[l], jnp.zeros((4, F), F32)], axis=0))
    with jax.named_scope("hop2"):
        hop2(at(0))
    with jax.named_scope("hop1"):
        hop1(at(2))
    with jax.named_scope("hop2"):
        hop2(at(1))
    with jax.named_scope("tw"):
        tok_in.wait()
    cot_in.wait()


    def inv_rms(rf):
        return lax.rsqrt(jnp.mean(rf * rf, axis=-1, keepdims=True) + NORM_EPS)

    def x_save(l):
        return pltpu.make_async_copy(xb, xs.at[l - 1], io_sem.at[0])

    def slope_out(b, lk, m):
        return pltpu.make_async_copy(gst.at[b, pl.ds(0, MX)], gp.at[lk, rows_of(m, MX), :], gp_sem.at[b])

    blocks = [(rb, cb) for cb in range(0, 1024, CB) for rb in range(0, MX, RB)]

    def activate(src, k, m, slot, part):
        for rb, cb in blocks[part * len(blocks) // 5 : (part + 1) * len(blocks) // 5]:
            act, slope = gelu_and_slope(src[rb : rb + RB, cb : cb + CB].astype(BF))
            r = pl.ds(pl.multiple_of(m * MX + rb, RB), RB)
            sd[r, pl.ds(pl.multiple_of(k * 1024 + cb, CB), CB)] = act
            gst[slot, rb : rb + RB, cb : cb + CB] = slope

    def up_tile(l, k, m, dst, kp, mp, src, slot):
        r = rows_of(m, MX)
        cols = pl.ds(pl.multiple_of(k * 1024, 1024), 1024)
        acc = None
        for kt in range(5):
            if kt < 4:
                rhs = w[k, 4 * kt : 4 * kt + 4]
                rhs = jnp.concatenate([rhs[:, n * 64 : (n + 1) * 64, :].reshape(256, 256) for n in range(4)], axis=1)
                term = nn(ub[r, kt * 256 : (kt + 1) * 256], rhs)
            else:
                term = tn(vcat[l, :, r], bcat[l, :, cols])
            acc = term if acc is None else acc + term
            activate(src, kp, mp, slot, kt)
        dst[...] = acc

    def forward_layer(l, _):
        @pl.when(l > 0)
        def _():
            x_save(l).start()

        def prep(m, _):
            r = rows_of(m, MU)
            rf = xb[r, :].astype(F32)
            u = (rf * inv_rms(rf)).astype(BF)
            ub[r, :] = u
            vcat[l, :, r] = left_parts(sum_parts(nt(acat[l, 0:32], u)))
            return 0

        @pl.when(l == 0)
        def _():
            with jax.named_scope("hop3"):
                hop3(at(0))

        with jax.named_scope("prep"):
            lax.fori_loop(0, T // MU, prep, 0)

        @pl.when(l == 0)
        def _():
            with jax.named_scope("hop1"):
                hop1(at(3))
            with jax.named_scope("hop2"):
                hop2(at(2))
            with jax.named_scope("hop3"):
                hop3(at(1))
            with jax.named_scope("hand_over"):
                hand_over(at(0))
            with jax.named_scope("hop1"):
                hop1(at(4))
            with jax.named_scope("hop2"):
                hop2(at(3))

        def slopes(t):
            slot = rem3(t)
            old = jnp.maximum(t - 2, 0)
            lk = jnp.where(t == 1, 4 * L, 4 * l + lax.div(old, 8))
            lk = jnp.where(t == 0, jnp.where(l == 0, 4 * L, 4 * l - 1), lk)
            m = jnp.where(t == 0, 7, jnp.where(t == 1, 2, lax.rem(old, 8)))
            slope_out(jnp.where(slot == 0, 2, slot - 1), lk, m).start()
            slope_out(slot, 0, 0).wait()
            return slot

        def up_step(t, _):
            k, m = lax.div(t, 8), lax.rem(t, 8)
            g = 8 * l + k

            due = t == 5
            j = at(0)
            for i in (10, 17, 24, 30):
                due = jnp.logical_or(due, t == i)
                j = j + jnp.where(t >= i, 1, 0)

            @pl.when(jnp.logical_or(jnp.logical_or(m == 0, m == 3), jnp.logical_or(due, t == 2)))
            def _():
                @pl.when(m == 0)
                def _():
                    @pl.when(k > 0)
                    def _():
                        release(g - 1)

                    with jax.named_scope("arr"):
                        arrive(g)

                @pl.when(due)
                def _():
                    with jax.named_scope("ev"):
                        event(8 * l + j)

                @pl.when(m == 3)
                def _():
                    with jax.named_scope("rf"):
                        refill(g)

                @pl.when(jnp.logical_and(l == 0, t == 2))
                def _():
                    with jax.named_scope("hop3"):
                        hop3(at(2))
                    with jax.named_scope("hop1"):
                        hop1(at(5))
                    with jax.named_scope("hop2"):
                        hop2(at(4))
                    with jax.named_scope("hop1"):
                        hop1(at(6))

            tp = jnp.maximum(t - 1, 0)
            kp, mp = lax.div(tp, 8), lax.rem(tp, 8)
            slot = slopes(t)

            @pl.when(lax.rem(t, 2) == 0)
            def _():
                with jax.named_scope("up"):
                    up_tile(l, k, m, pre0, kp, mp, pre1, slot)

            @pl.when(lax.rem(t, 2) == 1)
            def _():
                with jax.named_scope("up"):
                    up_tile(l, k, m, pre1, kp, mp, pre0, slot)

            return 0

        lax.fori_loop(0, 32, up_step, 0)
        release(8 * l + 3)
        slot = slopes(at(32))
        for part in range(5):
            activate(pre1, 3, at(7), slot, part)

        @pl.when(l > 0)
        def _():
            x_save(l).wait()

        def down_step(t, _):
            k, m = lax.div(t, 2), lax.rem(t, 2)
            g = 8 * l + 4 + k

            @pl.when(m == 0)
            def _():
                @pl.when(k > 0)
                def _():
                    release(g - 1)

                with jax.named_scope("arr"):
                    arrive(g)

                @pl.when(jnp.logical_or(k == 1, k == 2))
                def _():
                    with jax.named_scope("ev"):
                        event(g)

            @pl.when(m == 1)
            def _():
                with jax.named_scope("rf"):
                    refill(g)

                @pl.when(k == 3)
                def _():
                    with jax.named_scope("ev"):
                        event(g)

            r = rows_of(m, MD)
            cols = pl.ds(pl.multiple_of(k * 256, 256), 256)
            with jax.named_scope("dn"):
                step = nn(sd[r, :], w[4 + k].reshape(F, 256))
                xb[r, cols] = (xb[r, cols].astype(F32) + step).astype(BF)
            return 0

        lax.fori_loop(0, 8, down_step, 0)
        release(8 * l + 7)
        return 0

    lax.fori_loop(0, L, forward_layer, 0)


    x_final = pltpu.make_async_copy(xb, xout, io_sem.at[0])
    x_final.start()
    with jax.named_scope("gat"):
        gather(1, L - 1)
    slope_out(2, 4 * L - 1, at(7)).start()
    for b in range(3):
        slope_out(b, 0, at(0)).wait()

    def gp_in(t):
        lk = 4 * (L - 1 - lax.div(t, 16)) + quarter(lax.div(lax.rem(t, 16), 4))
        b = rem3(t)
        return pltpu.make_async_copy(gp.at[lk, rows_of(lax.rem(t, 4), MU), :], gst.at[b], gp_sem.at[b])

    gp_in(at(0)).start()
    gp_in(at(1)).start()
    x_final.wait()


    def x_load(l, start):
        @pl.when(l > 0)
        def _():
            cp = pltpu.make_async_copy(xs.at[l - 1], xb, io_sem.at[0])
            cp.start() if start else cp.wait()

        @pl.when(l == 0)
        def _():
            cp = pltpu.make_async_copy(tok, xb, io_sem.at[0])
            cp.start() if start else cp.wait()

    def backward_layer(rl, _):
        l = L - 1 - rl
        dlt[...] = jnp.zeros_like(dlt)
        gb[...] = jnp.zeros_like(gb)
        ga[...] = jnp.zeros_like(ga)

        def down_step(i, _):
            @pl.when(i == 1)
            def _():
                with jax.named_scope("gat"):
                    gather(0, l)

            @pl.when(i == 2)
            def _():
                x_load(l, True)

            with jax.named_scope("bev"):
                b_events(1, l, i)
            q = quarter(i)
            cols = pl.ds(pl.multiple_of(q * 1024, 1024), 1024)

            def tile(m, _):
                t = rl * 16 + i * 4 + m

                @pl.when(t + 2 < 16 * L)
                def _():
                    gp_in(t + 2).start()

                gp_in(t).wait()
                r = rows_of(m, MU)
                acc = None
                for k in range(4):
                    rhs = w[4 + k, pl.ds(4 * q, 4)].reshape(1024, 256)
                    term = nt(db[r, k * 256 : (k + 1) * 256], rhs)
                    acc = term if acc is None else acc + term
                d = (acc.astype(BF).astype(F32) * gst[rem3(t)]).astype(BF)
                sd[r, cols] = d
                dlt[:, r] += nt(bcat[l, 0:32, cols], d)
                gb[:, cols] += nn(vcat[l, 0:32, r], d)
                return 0

            with jax.named_scope("p1"):
                lax.fori_loop(0, T // MU, tile, 0)
            return 0

        lax.fori_loop(0, 4, down_step, 0)
        with jax.named_scope("brel"):
            b_release(1, l)
        dcat[...] = left_parts(sum_parts(dlt[...]))
        gb8 = sum_parts(gb[...])
        gacc[l, :, 0:2048] = gb8[:, 0:2048] + pltpu.roll(gb8[:, 2048:4096], 4, 0)

        def up_step(i, _):
            @pl.when(jnp.logical_and(i == 1, l > 0))
            def _():
                with jax.named_scope("gat"):
                    gather(1, l - 1)

            with jax.named_scope("bev"):
                b_events(0, l, i)
            q = quarter(i)
            cols = pl.ds(pl.multiple_of(q * 256, 256), 256)

            def tile(m, _):
                r = rows_of(m, MD)
                acc = None
                for k in range(4):
                    for n in range(4):
                        rhs = w[k, pl.ds(4 * q, 4), n * 64 : (n + 1) * 64, :].reshape(256, 256)
                        j = 4 * k + n
                        term = nt(sd[r, j * 256 : (j + 1) * 256], rhs)
                        acc = term if acc is None else acc + term
                side = tn(dcat[:, r], acat[l, :, cols]).astype(BF)
                ub[r, cols] = acc.astype(BF) + side
                return 0

            with jax.named_scope("p2"):
                lax.fori_loop(0, T // MD, tile, 0)
            return 0

        lax.fori_loop(0, 4, up_step, 0)
        with jax.named_scope("brel"):
            b_release(0, l)
        x_load(l, False)

        def finish(m, _):
            r = rows_of(m, MU)
            rf = xb[r, :].astype(F32)
            inv = inv_rms(rf)
            dn = ub[r, :].astype(F32)
            dot = jnp.mean(rf * dn, axis=-1, keepdims=True)
            db[r, :] = (db[r, :].astype(F32) + inv * dn - rf * ((inv * inv * inv) * dot)).astype(BF)
            u = (rf * inv).astype(BF)
            ga[...] += nn(dcat[0:32, r], u)
            return 0

        with jax.named_scope("fin"):
            lax.fori_loop(0, T // MU, finish, 0)
        ga8 = sum_parts(ga[...])
        gacc[l, :, 2048:2560] = ga8[:, 0:512] + pltpu.roll(ga8[:, 512:1024], 4, 0)
        with jax.named_scope("gout"):
            grads_out(l)
        return 0

    lax.fori_loop(0, L, backward_layer, 0)


    g_final = pltpu.make_async_copy(db, gtok, io_sem.at[1])
    g_final.start()
    for l in range(L):
        for i in range(4):

            @pl.when(me != 4 * l + i)
            def _():
                grad_send(jnp.int32(l), i).wait_send()

    others = rbuf.at[pl.ds(0, 15)]
    with jax.named_scope("redw"):
        remote(others, others, rr_sem, rr_sem, partner).wait_recv()
    total = rbuf[0]
    for i in range(1, 16):
        total = total + rbuf[i]
    gall[me] = total

    def share(o, _):
        @pl.when(o != me)
        def _():
            remote(gall.at[me], gall.at[me], as_sem, ar_sem, (lax.rem(o, 4), lax.div(o, 4))).start()

        return 0

    lax.fori_loop(0, 16, share, 0)
    others = gall.at[pl.ds(0, 15)]
    with jax.named_scope("allw"):
        remote(others, others, as_sem, ar_sem, partner).wait_send()
        remote(others, others, as_sem, ar_sem, partner).wait_recv()
    gout[...] = gall[...]
    g_final.wait()


def solution(mesh):
    tok_spec = P(GROUP, None)
    weight_spec = P(None, GROUP, None)

    def device_step(tokens, cotangent, up, down, lora_a, lora_b):
        hbm = pl.BlockSpec(memory_space=pltpu.HBM)
        vmem = pl.BlockSpec(memory_space=pltpu.VMEM)
        shape = jax.ShapeDtypeStruct
        dma, regular = pltpu.SemaphoreType.DMA, pltpu.SemaphoreType.REGULAR
        outs = pl.pallas_call(
            kernel,
            name="stack",
            out_shape=[
                shape((T, H), BF),
                shape((T, H), BF),
                shape((16, 8, GW), F32),
                shape((4 * L + 1, T, 1024), F32),
                shape((L - 1, T, H), BF),
                shape((L, 8, 4, 256, 256), BF),
            ],
            in_specs=[hbm, hbm, hbm, hbm, vmem, vmem],
            out_specs=[hbm, hbm, vmem, hbm, hbm, hbm],
            scratch_shapes=[
                pltpu.VMEM((8, 16, 256, 256), BF),
                pltpu.VMEM((T, F), BF),
                pltpu.VMEM((T, H), BF),
                pltpu.VMEM((T, H), BF),
                pltpu.VMEM((T, H), BF),
                pltpu.VMEM((3, MU, 1024), F32),
                pltpu.VMEM((MX, 1024), F32),
                pltpu.VMEM((MX, 1024), F32),
                pltpu.VMEM((L, 48, H), BF),
                pltpu.VMEM((L, 48, F), BF),
                pltpu.VMEM((L, 48, T), BF),
                pltpu.VMEM((48, T), BF),
                pltpu.VMEM((32, T), F32),
                pltpu.VMEM((32, F), F32),
                pltpu.VMEM((32, H), F32),
                pltpu.VMEM((L, 8, 4 * GW), F32),
                pltpu.VMEM((16, 8, GW), F32),
                pltpu.VMEM((16, 8, GW), F32),
                dma((8,)),
                dma((4, 8)),
                dma((4, 8)),
                dma((8,)),
                dma((3,)),
                dma((2,)),
                dma((2,)),
                dma((2, 5)),
                dma((2, 5)),
                dma((L,)),
                dma,
                dma,
                dma,
                regular((4, 8)),
            ],
            compiler_params=pltpu.CompilerParams(
                vmem_limit_bytes=67000000,
                has_side_effects=True,
            ),
        )(tokens, cotangent, up, down, lora_a.transpose(0, 2, 1), lora_b)
        x_out, g_tok, shares = outs[:3]
        grads = shares.reshape(L, 4, 2, 4, GW).transpose(0, 2, 3, 1, 4).reshape(L, 2, 4, 4 * GW)
        grad_b = grads[..., 0:2048].transpose(0, 2, 1, 3).reshape(L, 4, F)
        grad_a = grads[..., 2048:2560].transpose(0, 1, 3, 2).reshape(L, H, 4)
        return x_out, g_tok, grad_a, grad_b

    return jax.shard_map(
        device_step,
        mesh=mesh,
        in_specs=(tok_spec, tok_spec, weight_spec, weight_spec, P(), P()),
        out_specs=(tok_spec, tok_spec, P(), P()),
        check_vma=False,
    )
```

```python
import jax
import jax.numpy as jnp
from jax import lax
from jax.experimental import pallas as pl
from jax.experimental.pallas import tpu as pltpu
from jax.sharding import PartitionSpec as P

GROUP = ("data", "local")
NORM_EPS = 1e-6
BF = jnp.bfloat16
F32 = jnp.float32
C0 = 0.7978845608028654
K0 = 0.044715

T = 2048
H = 1024
F = 4096
L = 4
NG = 8 * L
MU = 512
MD = 1024
MX = 256
RB, CB = 32, 256
ROWS = ((0, 96), (96, 80), (176, 80))
FIRST_LAYER = (
    (2, ((2, 2),)),
    (4, ((3, 1), (1, 5))),
    (5, ((1, 4),)),
    (10, ((2, 3), (3, 2), (0, 7))),
    (12, ((0, 6),)),
    (14, ((2, 4),)),
    (16, ((0, 8),)),
    (20, ((3, 3), (0, 9))),
    (22, ((1, 6),)),
    (25, ((3, 4), (1, 7), (2, 5))),
    (27, ((1, 8), (2, 6), (0, 10))),
    (30, ((3, 5), (1, 9), (2, 7))),
)
GW = 640


def nn(a, b):
    return lax.dot_general(a, b, (((1,), (0,)), ((), ())), preferred_element_type=F32)


def nt(a, b):
    return lax.dot_general(a, b, (((1,), (1,)), ((), ())), preferred_element_type=F32)


def tn(a, b):
    return lax.dot_general(a, b, (((0,), (0,)), ((), ())), preferred_element_type=F32)


def split3(v):
    p1 = v.astype(BF).astype(F32)
    rest = v - p1
    p2 = rest.astype(BF).astype(F32)
    return p1, p2, (rest - p2).astype(BF).astype(F32)


def left_parts(v):
    p1, p2, p3 = split3(v)
    return jnp.concatenate([p1, p2, p3, p1, p1, p2], axis=0).astype(BF)


def right_parts(v):
    p1, p2, p3 = split3(v)
    return jnp.concatenate([p3, p2, p1, p1, p2, p1], axis=0).astype(BF)


def sum_parts(v):
    return v[0:8] + v[8:16] + v[16:24]


def gelu_and_slope(pre):
    x = pre.astype(F32)
    sq = x * x
    half = 0.5 * jnp.tanh(x * (sq * (C0 * K0) + C0)) + 0.5
    act = x * half
    slope = (act * (1.0 - half)) * (sq * (6.0 * C0 * K0) + 2.0 * C0) + half
    return act.astype(BF), slope


def rem3(t):
    return t - 3 * lax.div(t * 43, 128)


def rows_of(m, size):
    return pl.ds(pl.multiple_of(m * size, size), size)


def kernel(
    tok, cot, up, down, a4, b4,
    xout, gtok, gout, gp, xs, kept,
    w, sd, xb, ub, db, gst, pre0, pre1, acat, bcat, vcat, dcat, dlt, gb, ga, gacc, rbuf, gall,
    own_sem, fs_sem, fr_sem, kept_sem, gp_sem, io_sem, bo_sem, bs_sem, br_sem, rs_sem, rr_sem, as_sem, ar_sem,
    cred,
):
    data = lax.axis_index("data")
    local = lax.axis_index("local")
    x, c = lax.div(data, 2), lax.rem(data, 2)
    z, y = lax.div(local, 2), lax.rem(local, 2)
    me = data * 4 + local
    dx, dy, dz, dc = 1 - 2 * x, 1 - 2 * y, 1 - 2 * z, 1 - 2 * c
    par = lax.rem(x + y + z, 2)

    def quarter(i):
        hi, lo = lax.div(i, 2), lax.rem(i, 2)
        return 2 * (par + hi - 2 * par * hi) + (c + lo - 2 * c * lo)

    q_own, q_miss = quarter(0), quarter(2)

    def pick(dim, a0, a1, a2):
        return lax.div((1 - dim) * (2 - dim), 2) * a0 + dim * (2 - dim) * a1 + lax.div(dim * (dim - 1), 2) * a2

    def device(dim):
        return (local + pick(dim, 0, dy, 2 * dz), data + pick(dim, 2 * dx, 0, 0))

    neighbours = ((local, data + 2 * dx), (local + dy, data), (local + 2 * dz, data), (local, data + dc))
    partner = neighbours[3]

    def remote(src, dst, ssem, rsem, dev):
        return pltpu.make_async_remote_copy(
            src_ref=src, dst_ref=dst, send_sem=ssem, recv_sem=rsem, device_id=dev, device_id_type=pl.DeviceIdType.MESH
        )


    def own_load(g):
        s, l = lax.rem(g, 8), lax.div(g, 8)

        @pl.when(s < 4)
        def _():
            for n in range(4):
                pltpu.make_async_copy(
                    up.at[l, :, pl.ds(pl.multiple_of(s * 1024 + n * 256, 256), 256)],
                    w.at[s, me, pl.ds(n * 64, 64), :],
                    own_sem.at[s],
                ).start()

        @pl.when(s >= 4)
        def _():
            pltpu.make_async_copy(
                down.at[l, :, pl.ds(pl.multiple_of((s - 4) * 256, 256), 256)], w.at[s, me], own_sem.at[s]
            ).start()

    def colour(g):
        q = rem3(jnp.where(g == 1, 2 + c, jnp.where(g < 3, 1 + 2 * c, g + c)))
        turn = jnp.where(jnp.logical_or(g == 1, g == 2), 2, 1)
        return q, rem3(q + turn), rem3(q + 2 * turn)

    def delta(dim):
        return pick(dim, 8 * dx, dy, 2 * dz)

    def use_credit(g, dim):
        @pl.when(g >= 8)
        def _():
            pl.semaphore_wait(cred.at[dim, lax.rem(g, 8)], 1)

    def send_blocks(g, phase, dim, blocks, dev):
        s = lax.rem(g, 8)
        use_credit(g, dim)
        for b in blocks:
            remote(w.at[s, b], w.at[s, b], fs_sem.at[phase, s], fr_sem.at[phase, s], dev).start()

    def span(g, phase):
        s = lax.rem(g, 8)
        r = w.at[s, pl.ds(0, (1, 2, 4, 8)[phase])]
        return remote(r, r, fs_sem.at[phase, s], fr_sem.at[phase, s], partner)

    def ready(g):
        return jnp.logical_and(g >= 0, g < NG)

    def hop1(g):
        d1, _, _ = colour(g)
        s = lax.rem(g, 8)
        pltpu.make_async_copy(w.at[s, me], w.at[s, me], own_sem.at[s]).wait()
        send_blocks(g, 0, d1, (me,), device(d1))

    def hop2(g):
        d1, d2, _ = colour(g)
        span(g, 0).wait_recv()
        send_blocks(g, 1, d2, (me, me + delta(d1)), device(d2))

    def hop3(g):
        d1, d2, d3 = colour(g)
        e1, e2 = delta(d1), delta(d2)
        span(g, 1).wait_recv()
        send_blocks(g, 2, d3, (me, me + e1, me + e2, me + e1 + e2), device(d3))

    def hand_over(g):
        s = lax.rem(g, 8)
        span(g, 2).wait_recv()
        use_credit(g, 3)
        for h in range(2):
            r2 = w.at[s, pl.ds(8 * h + 4 * c, 4)]
            remote(r2, r2, fs_sem.at[3, s], fr_sem.at[3, s], partner).start()

    def event(j):
        for step, ahead in ((hand_over, 1), (hop2, 5), (hop3, 3)):

            @pl.when(j + ahead < NG)
            def _():
                with jax.named_scope("st"):
                    step(j + ahead)

    def refill(j):
        @pl.when(j + 7 < NG)
        def _():
            hop1(j + 7)

    def keep_copy(g):
        s, l = lax.rem(g, 8), lax.div(g, 8)
        return pltpu.make_async_copy(w.at[s, pl.ds(4 * q_own, 4)], kept.at[l, s], kept_sem.at[s])

    def arrive(g):
        span(g, 3).wait_recv()
        keep_copy(g).start()

    def release(g):
        s = lax.rem(g, 8)
        for phase in range(4):
            span(g, phase).wait_send()
        keep_copy(g).wait()
        for i in range(4):
            pl.semaphore_signal(cred.at[i, s], inc=1, device_id=neighbours[i], device_id_type=pl.DeviceIdType.MESH)

        @pl.when(g + 8 < NG)
        def _():
            own_load(g + 8)


    def whole(m, q):
        return w.at[pl.ds(4 * m, 4), pl.ds(4 * q, 4)]

    def part(ref, dim):
        return ref.at[:, :, pl.ds(*ROWS[dim]), :]

    def b_own(m, l):
        return pltpu.make_async_copy(kept.at[l, pl.ds(4 * m, 4)], whole(m, q_own), bo_sem.at[m])

    def b_send(m, l, i, q):
        src, dst = kept.at[l, pl.ds(4 * m, 4)], whole(m, q)
        if i < 3:
            src, dst = part(src, i), part(dst, i)
        return remote(src, dst, bs_sem.at[m, i], br_sem.at[m, i], neighbours[i])

    def b_forward(m):
        return remote(whole(m, q_miss), whole(m, q_miss), bs_sem.at[m, 4], br_sem.at[m, 4], partner)

    def gather(m, l):
        @pl.when(jnp.logical_or(l < L - 1, m == 0))
        def _():
            b_own(m, l).start()

        for i in range(4):
            for s in range(4):
                pl.semaphore_wait(cred.at[i, 4 * m + s], 1)
            b_send(m, l, i, q_own).start()

    def b_events(m, l, i):
        @pl.when(jnp.logical_and(i == 0, jnp.logical_or(l < L - 1, m == 0)))
        def _():
            b_own(m, l).wait()

        @pl.when(i == 1)
        def _():
            b_send(m, l, 3, quarter(1)).wait_recv()

        @pl.when(i == 2)
        def _():
            for d in range(3):
                b_send(m, l, d, q_miss).wait_recv()
            b_forward(m).start()

        @pl.when(i == 3)
        def _():
            b_forward(m).wait_recv()

    def b_release(m, l):
        b_forward(m).wait_send()
        for i in range(4):
            b_send(m, l, i, q_own).wait_send()

        @pl.when(l > 0)
        def _():
            for i in range(4):
                for s in range(4):
                    pl.semaphore_signal(
                        cred.at[i, 4 * m + s], inc=1, device_id=neighbours[i], device_id_type=pl.DeviceIdType.MESH
                    )


    def grad_send(l, i):
        return remote(
            gacc.at[l, :, pl.ds(i * GW, GW)], rbuf.at[me], rs_sem.at[l], rr_sem, (jnp.int32(i), l)
        )

    def grads_out(l):
        for i in range(4):
            mine = me == 4 * l + i

            @pl.when(jnp.logical_not(mine))
            def _():
                grad_send(l, i).start()

            @pl.when(mine)
            def _():
                rbuf[me] = gacc[l, :, i * GW : (i + 1) * GW]


    tok_in = pltpu.make_async_copy(tok, xb, io_sem.at[0])
    cot_in = pltpu.make_async_copy(cot, db, io_sem.at[1])

    def first_loads(g, _):
        own_load(g)
        return 0

    lax.fori_loop(0, 8, first_loads, 0)
    tok_in.start()
    cot_in.start()
    at = jnp.int32
    for g in (0, 2, 1, 5):
        with jax.named_scope("hop1"):
            hop1(at(g))
    for b in range(2):
        pltpu.make_async_copy(gst.at[b, pl.ds(0, MX)], gp.at[4 * L, pl.ds(b * MX, MX), :], gp_sem.at[b]).start()
    for l in range(L):
        acat[l] = right_parts(jnp.concatenate([a4[l], jnp.zeros((4, H), F32)], axis=0))
        bcat[l] = right_parts(jnp.concatenate([b4[l], jnp.zeros((4, F), F32)], axis=0))
    with jax.named_scope("tw"):
        tok_in.wait()
    cot_in.wait()
    with jax.named_scope("hop2"):
        hop2(at(0))


    def inv_rms(rf):
        return lax.rsqrt(jnp.mean(rf * rf, axis=-1, keepdims=True) + NORM_EPS)

    def x_save(l):
        return pltpu.make_async_copy(xb, xs.at[l - 1], io_sem.at[0])

    def slope_out(b, lk, m):
        return pltpu.make_async_copy(gst.at[b, pl.ds(0, MX)], gp.at[lk, rows_of(m, MX), :], gp_sem.at[b])

    def gp_in(t):
        lk = 4 * (L - 1 - lax.div(t, 16)) + quarter(lax.div(lax.rem(t, 16), 4))
        b = rem3(t)
        return pltpu.make_async_copy(gp.at[lk, rows_of(lax.rem(t, 4), MU), :], gst.at[b], gp_sem.at[b])

    blocks = [(rb, cb) for cb in range(0, 1024, CB) for rb in range(0, MX, RB)]

    def activate(src, k, m, slot, part):
        for rb, cb in blocks[part * len(blocks) // 5 : (part + 1) * len(blocks) // 5]:
            act, slope = gelu_and_slope(src[rb : rb + RB, cb : cb + CB].astype(BF))
            r = pl.ds(pl.multiple_of(m * MX + rb, RB), RB)
            sd[r, pl.ds(pl.multiple_of(k * 1024 + cb, CB), CB)] = act
            gst[slot, rb : rb + RB, cb : cb + CB] = slope

    def up_tile(l, k, m, dst, kp, mp, src, slot):
        r = rows_of(m, MX)
        cols = pl.ds(pl.multiple_of(k * 1024, 1024), 1024)
        acc = None
        for kt in range(5):
            if kt < 4:
                rhs = w[k, 4 * kt : 4 * kt + 4]
                rhs = jnp.concatenate([rhs[:, n * 64 : (n + 1) * 64, :].reshape(256, 256) for n in range(4)], axis=1)
                term = nn(ub[r, kt * 256 : (kt + 1) * 256], rhs)
            else:
                term = tn(vcat[l, :, r], bcat[l, :, cols])
            acc = term if acc is None else acc + term
            activate(src, kp, mp, slot, kt)
        dst[...] = acc

    def forward_layer(l, _):
        @pl.when(l > 0)
        def _():
            x_save(l).start()

        def prep(m, _):
            r = rows_of(m, MU)
            rf = xb[r, :].astype(F32)
            u = (rf * inv_rms(rf)).astype(BF)
            ub[r, :] = u
            vcat[l, :, r] = left_parts(sum_parts(nt(acat[l, 0:32], u)))
            return 0

        with jax.named_scope("prep"):
            lax.fori_loop(0, T // MU, prep, 0)

        @pl.when(l == 0)
        def _():
            for step, g in ((hop1, 3), (hop2, 1), (hop3, 0), (hop2, 2), (hop1, 4), (hop2, 3), (hop3, 1), (hand_over, 0)):
                with jax.named_scope("st0"):
                    step(at(g))

        def slopes(t):
            slot = rem3(t)
            old = jnp.maximum(t - 2, 0)
            lk = jnp.where(t == 1, 4 * L, 4 * l + lax.div(old, 8))
            lk = jnp.where(t == 0, jnp.where(l == 0, 4 * L, 4 * l - 1), lk)
            m = jnp.where(t == 0, 7, jnp.where(t == 1, 2, lax.rem(old, 8)))
            slope_out(jnp.where(slot == 0, 2, slot - 1), lk, m).start()
            slope_out(slot, 0, 0).wait()
            return slot

        def up_step(t, _):
            k, m = lax.div(t, 8), lax.rem(t, 8)
            g = 8 * l + k

            due = t == 5
            j = at(0)
            for i in (10, 17, 24, 30):
                due = jnp.logical_or(due, t == i)
                j = j + jnp.where(t >= i, 1, 0)

            @pl.when(m == 0)
            def _():
                @pl.when(k > 0)
                def _():
                    release(g - 1)

                with jax.named_scope("arr"):
                    arrive(g)

            @pl.when(l == 0)
            def _():
                for when, steps in FIRST_LAYER:

                    @pl.when(t == when)
                    def _():
                        for kind, chunk in steps:
                            with jax.named_scope("st1"):
                                (hop1, hop2, hop3, hand_over)[kind](at(chunk))

            @pl.when(jnp.logical_and(l > 0, jnp.logical_or(due, m == 3)))
            def _():
                @pl.when(due)
                def _():
                    with jax.named_scope("ev"):
                        event(8 * l + j)

                @pl.when(m == 3)
                def _():
                    with jax.named_scope("rf"):
                        refill(g)

            tp = jnp.maximum(t - 1, 0)
            kp, mp = lax.div(tp, 8), lax.rem(tp, 8)
            slot = slopes(t)

            @pl.when(lax.rem(t, 2) == 0)
            def _():
                with jax.named_scope("up"):
                    up_tile(l, k, m, pre0, kp, mp, pre1, slot)

            @pl.when(lax.rem(t, 2) == 1)
            def _():
                with jax.named_scope("up"):
                    up_tile(l, k, m, pre1, kp, mp, pre0, slot)

            return 0

        lax.fori_loop(0, 32, up_step, 0)
        release(8 * l + 3)
        slot = slopes(at(32))
        for part in range(5):
            activate(pre1, 3, at(7), slot, part)

        @pl.when(l == L - 1)
        def _():
            slope_out(2, 4 * L - 1, at(7)).start()

        @pl.when(l > 0)
        def _():
            x_save(l).wait()

        def down_step(t, _):
            k, m = lax.div(t, 2), lax.rem(t, 2)
            g = 8 * l + 4 + k

            @pl.when(m == 0)
            def _():
                @pl.when(k > 0)
                def _():
                    release(g - 1)

                with jax.named_scope("arr"):
                    arrive(g)

                @pl.when(jnp.logical_or(k == 1, k == 2))
                def _():
                    with jax.named_scope("ev"):
                        event(g)

            @pl.when(jnp.logical_and(l == L - 1, t == 5))
            def _():
                for b in range(3):
                    slope_out(b, 0, at(0)).wait()
                gp_in(at(0)).start()
                gp_in(at(1)).start()

            @pl.when(m == 1)
            def _():
                with jax.named_scope("rf"):
                    refill(g)

                @pl.when(k == 3)
                def _():
                    with jax.named_scope("ev"):
                        event(g)

            r = rows_of(m, MD)
            cols = pl.ds(pl.multiple_of(k * 256, 256), 256)
            with jax.named_scope("dn"):
                step = nn(sd[r, :], w[4 + k].reshape(F, 256))
                xb[r, cols] = (xb[r, cols].astype(F32) + step).astype(BF)
            return 0

        lax.fori_loop(0, 8, down_step, 0)
        release(8 * l + 7)
        return 0

    lax.fori_loop(0, L, forward_layer, 0)


    x_final = pltpu.make_async_copy(xb, xout, io_sem.at[0])
    x_final.start()
    with jax.named_scope("gat"):
        gather(1, L - 1)


    def x_load(l, start):
        @pl.when(l > 0)
        def _():
            cp = pltpu.make_async_copy(xs.at[l - 1], xb, io_sem.at[0])
            cp.start() if start else cp.wait()

        @pl.when(l == 0)
        def _():
            cp = pltpu.make_async_copy(tok, xb, io_sem.at[0])
            cp.start() if start else cp.wait()

    def backward_layer(rl, _):
        l = L - 1 - rl
        dlt[...] = jnp.zeros_like(dlt)
        gb[...] = jnp.zeros_like(gb)
        ga[...] = jnp.zeros_like(ga)

        def down_step(i, _):
            @pl.when(i == 1)
            def _():
                with jax.named_scope("gat"):
                    gather(0, l)

            @pl.when(i == 2)
            def _():
                @pl.when(l == L - 1)
                def _():
                    x_final.wait()

                x_load(l, True)

            with jax.named_scope("bev"):
                b_events(1, l, i)
            q = quarter(i)
            cols = pl.ds(pl.multiple_of(q * 1024, 1024), 1024)

            def tile(m, _):
                t = rl * 16 + i * 4 + m

                @pl.when(t + 2 < 16 * L)
                def _():
                    gp_in(t + 2).start()

                gp_in(t).wait()
                r = rows_of(m, MU)
                acc = None
                for k in range(4):
                    rhs = w[4 + k, pl.ds(4 * q, 4)].reshape(1024, 256)
                    term = nt(db[r, k * 256 : (k + 1) * 256], rhs)
                    acc = term if acc is None else acc + term
                d = (acc.astype(BF).astype(F32) * gst[rem3(t)]).astype(BF)
                sd[r, cols] = d
                dlt[:, r] += nt(bcat[l, 0:32, cols], d)
                gb[:, cols] += nn(vcat[l, 0:32, r], d)
                return 0

            with jax.named_scope("p1"):
                lax.fori_loop(0, T // MU, tile, 0)
            return 0

        lax.fori_loop(0, 4, down_step, 0)
        with jax.named_scope("brel"):
            b_release(1, l)
        dcat[...] = left_parts(sum_parts(dlt[...]))
        gb8 = sum_parts(gb[...])
        gacc[l, :, 0:2048] = gb8[:, 0:2048] + pltpu.roll(gb8[:, 2048:4096], 4, 0)

        def up_step(i, _):
            @pl.when(jnp.logical_and(i == 1, l > 0))
            def _():
                with jax.named_scope("gat"):
                    gather(1, l - 1)

            with jax.named_scope("bev"):
                b_events(0, l, i)
            q = quarter(i)
            cols = pl.ds(pl.multiple_of(q * 256, 256), 256)

            def tile(m, _):
                r = rows_of(m, MD)
                acc = None
                for k in range(4):
                    for n in range(4):
                        rhs = w[k, pl.ds(4 * q, 4), n * 64 : (n + 1) * 64, :].reshape(256, 256)
                        j = 4 * k + n
                        term = nt(sd[r, j * 256 : (j + 1) * 256], rhs)
                        acc = term if acc is None else acc + term
                side = tn(dcat[:, r], acat[l, :, cols]).astype(BF)
                ub[r, cols] = acc.astype(BF) + side
                return 0

            with jax.named_scope("p2"):
                lax.fori_loop(0, T // MD, tile, 0)
            return 0

        lax.fori_loop(0, 4, up_step, 0)
        with jax.named_scope("brel"):
            b_release(0, l)
        x_load(l, False)

        def finish(m, _):
            r = rows_of(m, MU)
            rf = xb[r, :].astype(F32)
            inv = inv_rms(rf)
            dn = ub[r, :].astype(F32)
            dot = jnp.mean(rf * dn, axis=-1, keepdims=True)
            db[r, :] = (db[r, :].astype(F32) + inv * dn - rf * ((inv * inv * inv) * dot)).astype(BF)
            u = (rf * inv).astype(BF)
            ga[...] += nn(dcat[0:32, r], u)
            return 0

        with jax.named_scope("fin"):
            lax.fori_loop(0, T // MU, finish, 0)
        ga8 = sum_parts(ga[...])
        gacc[l, :, 2048:2560] = ga8[:, 0:512] + pltpu.roll(ga8[:, 512:1024], 4, 0)
        with jax.named_scope("gout"):
            grads_out(l)
        return 0

    lax.fori_loop(0, L, backward_layer, 0)


    g_final = pltpu.make_async_copy(db, gtok, io_sem.at[1])
    g_final.start()
    others = rbuf.at[pl.ds(0, 15)]
    with jax.named_scope("redw"):
        remote(others, others, rr_sem, rr_sem, partner).wait_recv()
    total = rbuf[0]
    for i in range(1, 16):
        total = total + rbuf[i]
    gall[me] = total

    def share(o, _):
        @pl.when(o != me)
        def _():
            remote(gall.at[me], gall.at[me], as_sem, ar_sem, (lax.rem(o, 4), lax.div(o, 4))).start()

        return 0

    lax.fori_loop(0, 16, share, 0)
    others = gall.at[pl.ds(0, 15)]
    with jax.named_scope("allw"):
        remote(others, others, as_sem, ar_sem, partner).wait_send()
        remote(others, others, as_sem, ar_sem, partner).wait_recv()
    for l in range(L):
        for i in range(4):

            @pl.when(me != 4 * l + i)
            def _():
                grad_send(jnp.int32(l), i).wait_send()

    gout[...] = gall[...]
    g_final.wait()


def solution(mesh):
    tok_spec = P(GROUP, None)
    weight_spec = P(None, GROUP, None)

    def device_step(tokens, cotangent, up, down, lora_a, lora_b):
        hbm = pl.BlockSpec(memory_space=pltpu.HBM)
        vmem = pl.BlockSpec(memory_space=pltpu.VMEM)
        shape = jax.ShapeDtypeStruct
        dma, regular = pltpu.SemaphoreType.DMA, pltpu.SemaphoreType.REGULAR
        outs = pl.pallas_call(
            kernel,
            name="stack",
            out_shape=[
                shape((T, H), BF),
                shape((T, H), BF),
                shape((16, 8, GW), F32),
                shape((4 * L + 1, T, 1024), F32),
                shape((L - 1, T, H), BF),
                shape((L, 8, 4, 256, 256), BF),
            ],
            in_specs=[hbm, hbm, hbm, hbm, vmem, vmem],
            out_specs=[hbm, hbm, vmem, hbm, hbm, hbm],
            scratch_shapes=[
                pltpu.VMEM((8, 16, 256, 256), BF),
                pltpu.VMEM((T, F), BF),
                pltpu.VMEM((T, H), BF),
                pltpu.VMEM((T, H), BF),
                pltpu.VMEM((T, H), BF),
                pltpu.VMEM((3, MU, 1024), F32),
                pltpu.VMEM((MX, 1024), F32),
                pltpu.VMEM((MX, 1024), F32),
                pltpu.VMEM((L, 48, H), BF),
                pltpu.VMEM((L, 48, F), BF),
                pltpu.VMEM((L, 48, T), BF),
                pltpu.VMEM((48, T), BF),
                pltpu.VMEM((32, T), F32),
                pltpu.VMEM((32, F), F32),
                pltpu.VMEM((32, H), F32),
                pltpu.VMEM((L, 8, 4 * GW), F32),
                pltpu.VMEM((16, 8, GW), F32),
                pltpu.VMEM((16, 8, GW), F32),
                dma((8,)),
                dma((4, 8)),
                dma((4, 8)),
                dma((8,)),
                dma((3,)),
                dma((2,)),
                dma((2,)),
                dma((2, 5)),
                dma((2, 5)),
                dma((L,)),
                dma,
                dma,
                dma,
                regular((4, 8)),
            ],
            compiler_params=pltpu.CompilerParams(
                vmem_limit_bytes=67000000,
                has_side_effects=True,
            ),
        )(tokens, cotangent, up, down, lora_a.transpose(0, 2, 1), lora_b)
        x_out, g_tok, shares = outs[:3]
        grads = shares.reshape(L, 4, 2, 4, GW).transpose(0, 2, 3, 1, 4).reshape(L, 2, 4, 4 * GW)
        grad_b = grads[..., 0:2048].transpose(0, 2, 1, 3).reshape(L, 4, F)
        grad_a = grads[..., 2048:2560].transpose(0, 1, 3, 2).reshape(L, H, 4)
        return x_out, g_tok, grad_a, grad_b

    return jax.shard_map(
        device_step,
        mesh=mesh,
        in_specs=(tok_spec, tok_spec, weight_spec, weight_spec, P(), P()),
        out_specs=(tok_spec, tok_spec, P(), P()),
        check_vma=False,
    )
```

```python
import jax
import jax.numpy as jnp
from jax import lax
from jax.experimental import pallas as pl
from jax.experimental.pallas import tpu as pltpu
from jax.sharding import PartitionSpec as P

GROUP = ("data", "local")
NORM_EPS = 1e-6
BF = jnp.bfloat16
F32 = jnp.float32
C0 = 0.7978845608028654
K0 = 0.044715

T = 2048
H = 1024
F = 4096
L = 4
NG = 8 * L
MU = 512
MD = 1024
MX = 512
RB, CB = 16, 256
ROWS = ((0, 96), (96, 80), (176, 80))
FIRST_LAYER = (
    (1, ((2, 2),)),
    (2, ((3, 1), (1, 5))),
    (3, ((1, 4),)),
    (5, ((2, 3), (3, 2), (0, 7))),
    (6, ((0, 6),)),
    (7, ((2, 4),)),
    (8, ((0, 8),)),
    (10, ((3, 3), (0, 9))),
    (11, ((1, 6),)),
    (13, ((3, 4), (1, 7), (2, 5))),
    (14, ((1, 8), (2, 6), (0, 10))),
)
GW = 640


def nn(a, b):
    return lax.dot_general(a, b, (((1,), (0,)), ((), ())), preferred_element_type=F32)


def nt(a, b):
    return lax.dot_general(a, b, (((1,), (1,)), ((), ())), preferred_element_type=F32)


def tn(a, b):
    return lax.dot_general(a, b, (((0,), (0,)), ((), ())), preferred_element_type=F32)


def split3(v):
    p1 = v.astype(BF).astype(F32)
    rest = v - p1
    p2 = rest.astype(BF).astype(F32)
    return p1, p2, (rest - p2).astype(BF).astype(F32)


def left_parts(v):
    p1, p2, p3 = split3(v)
    return jnp.concatenate([p1, p2, p3, p1, p1, p2], axis=0).astype(BF)


def right_parts(v):
    p1, p2, p3 = split3(v)
    return jnp.concatenate([p3, p2, p1, p1, p2, p1], axis=0).astype(BF)


def sum_parts(v):
    return v[0:8] + v[8:16] + v[16:24]


def gelu_and_slope(pre):
    x = pre.astype(F32)
    sq = x * x
    half = 0.5 * jnp.tanh(x * (sq * (C0 * K0) + C0)) + 0.5
    act = x * half
    slope = (act * (1.0 - half)) * (sq * (6.0 * C0 * K0) + 2.0 * C0) + half
    return act.astype(BF), slope


def rem3(t):
    return t - 3 * lax.div(t * 43, 128)


def rows_of(m, size):
    return pl.ds(pl.multiple_of(m * size, size), size)


def kernel(
    tok, cot, up, down, a4, b4,
    xout, gtok, gout, gp, xs, kept,
    w, sd, xb, ub, db, gst, pre0, pre1, acat, bcat, vcat, dcat, dlt, gb, ga, gacc, rbuf, gall,
    own_sem, fs_sem, fr_sem, kept_sem, gp_sem, io_sem, bo_sem, bs_sem, br_sem, rs_sem, rr_sem, as_sem, ar_sem,
    cred,
):
    data = lax.axis_index("data")
    local = lax.axis_index("local")
    x, c = lax.div(data, 2), lax.rem(data, 2)
    z, y = lax.div(local, 2), lax.rem(local, 2)
    me = data * 4 + local
    dx, dy, dz, dc = 1 - 2 * x, 1 - 2 * y, 1 - 2 * z, 1 - 2 * c
    par = lax.rem(x + y + z, 2)

    def quarter(i):
        hi, lo = lax.div(i, 2), lax.rem(i, 2)
        return 2 * (par + hi - 2 * par * hi) + (c + lo - 2 * c * lo)

    q_own, q_miss = quarter(0), quarter(2)

    def pick(dim, a0, a1, a2):
        return lax.div((1 - dim) * (2 - dim), 2) * a0 + dim * (2 - dim) * a1 + lax.div(dim * (dim - 1), 2) * a2

    def device(dim):
        return (local + pick(dim, 0, dy, 2 * dz), data + pick(dim, 2 * dx, 0, 0))

    neighbours = ((local, data + 2 * dx), (local + dy, data), (local + 2 * dz, data), (local, data + dc))
    partner = neighbours[3]

    def remote(src, dst, ssem, rsem, dev):
        return pltpu.make_async_remote_copy(
            src_ref=src, dst_ref=dst, send_sem=ssem, recv_sem=rsem, device_id=dev, device_id_type=pl.DeviceIdType.MESH
        )


    def own_load(g):
        s, l = lax.rem(g, 8), lax.div(g, 8)

        @pl.when(s < 4)
        def _():
            for n in range(4):
                pltpu.make_async_copy(
                    up.at[l, :, pl.ds(pl.multiple_of(s * 1024 + n * 256, 256), 256)],
                    w.at[s, me, pl.ds(n * 64, 64), :],
                    own_sem.at[s],
                ).start()

        @pl.when(s >= 4)
        def _():
            pltpu.make_async_copy(
                down.at[l, :, pl.ds(pl.multiple_of((s - 4) * 256, 256), 256)], w.at[s, me], own_sem.at[s]
            ).start()

    def colour(g):
        q = rem3(jnp.where(g == 1, 2 + c, jnp.where(g < 3, 1 + 2 * c, g + c)))
        turn = jnp.where(jnp.logical_or(g == 1, g == 2), 2, 1)
        return q, rem3(q + turn), rem3(q + 2 * turn)

    def delta(dim):
        return pick(dim, 8 * dx, dy, 2 * dz)

    def use_credit(g, dim):
        @pl.when(g >= 8)
        def _():
            pl.semaphore_wait(cred.at[dim, lax.rem(g, 8)], 1)

    def send_blocks(g, phase, dim, blocks, dev):
        s = lax.rem(g, 8)
        use_credit(g, dim)
        for b in blocks:
            remote(w.at[s, b], w.at[s, b], fs_sem.at[phase, s], fr_sem.at[phase, s], dev).start()

    def span(g, phase):
        s = lax.rem(g, 8)
        r = w.at[s, pl.ds(0, (1, 2, 4, 8)[phase])]
        return remote(r, r, fs_sem.at[phase, s], fr_sem.at[phase, s], partner)

    def ready(g):
        return jnp.logical_and(g >= 0, g < NG)

    def hop1(g):
        d1, _, _ = colour(g)
        s = lax.rem(g, 8)
        pltpu.make_async_copy(w.at[s, me], w.at[s, me], own_sem.at[s]).wait()
        send_blocks(g, 0, d1, (me,), device(d1))

    def hop2(g):
        d1, d2, _ = colour(g)
        span(g, 0).wait_recv()
        send_blocks(g, 1, d2, (me, me + delta(d1)), device(d2))

    def hop3(g):
        d1, d2, d3 = colour(g)
        e1, e2 = delta(d1), delta(d2)
        span(g, 1).wait_recv()
        send_blocks(g, 2, d3, (me, me + e1, me + e2, me + e1 + e2), device(d3))

    def hand_over(g):
        s = lax.rem(g, 8)
        span(g, 2).wait_recv()
        use_credit(g, 3)
        for h in range(2):
            r2 = w.at[s, pl.ds(8 * h + 4 * c, 4)]
            remote(r2, r2, fs_sem.at[3, s], fr_sem.at[3, s], partner).start()

    def event(j):
        for step, ahead in ((hand_over, 1), (hop2, 5), (hop3, 3)):

            @pl.when(j + ahead < NG)
            def _():
                with jax.named_scope("st"):
                    step(j + ahead)

    def refill(j):
        @pl.when(j + 7 < NG)
        def _():
            hop1(j + 7)

    def keep_copy(g):
        s, l = lax.rem(g, 8), lax.div(g, 8)
        return pltpu.make_async_copy(w.at[s, pl.ds(4 * q_own, 4)], kept.at[l, s], kept_sem.at[s])

    def arrive(g):
        span(g, 3).wait_recv()
        keep_copy(g).start()

    def release(g):
        s = lax.rem(g, 8)
        for phase in range(4):
            span(g, phase).wait_send()
        keep_copy(g).wait()
        for i in range(4):
            pl.semaphore_signal(cred.at[i, s], inc=1, device_id=neighbours[i], device_id_type=pl.DeviceIdType.MESH)

        @pl.when(g + 8 < NG)
        def _():
            own_load(g + 8)


    def whole(m, q):
        return w.at[pl.ds(4 * m, 4), pl.ds(4 * q, 4)]

    def part(ref, dim):
        return ref.at[:, :, pl.ds(*ROWS[dim]), :]

    def b_own(m, l):
        return pltpu.make_async_copy(kept.at[l, pl.ds(4 * m, 4)], whole(m, q_own), bo_sem.at[m])

    def b_send(m, l, i, q):
        src, dst = kept.at[l, pl.ds(4 * m, 4)], whole(m, q)
        if i < 3:
            src, dst = part(src, i), part(dst, i)
        return remote(src, dst, bs_sem.at[m, i], br_sem.at[m, i], neighbours[i])

    def b_forward(m):
        return remote(whole(m, q_miss), whole(m, q_miss), bs_sem.at[m, 4], br_sem.at[m, 4], partner)

    def gather(m, l):
        @pl.when(jnp.logical_or(l < L - 1, m == 0))
        def _():
            b_own(m, l).start()

        for i in range(4):
            for s in range(4):
                pl.semaphore_wait(cred.at[i, 4 * m + s], 1)
            b_send(m, l, i, q_own).start()

    def b_events(m, l, i):
        @pl.when(jnp.logical_and(i == 0, jnp.logical_or(l < L - 1, m == 0)))
        def _():
            b_own(m, l).wait()

        @pl.when(i == 1)
        def _():
            b_send(m, l, 3, quarter(1)).wait_recv()

        @pl.when(i == 2)
        def _():
            for d in range(3):
                b_send(m, l, d, q_miss).wait_recv()
            b_forward(m).start()

        @pl.when(i == 3)
        def _():
            b_forward(m).wait_recv()

    def b_release(m, l):
        b_forward(m).wait_send()
        for i in range(4):
            b_send(m, l, i, q_own).wait_send()

        @pl.when(l > 0)
        def _():
            for i in range(4):
                for s in range(4):
                    pl.semaphore_signal(
                        cred.at[i, 4 * m + s], inc=1, device_id=neighbours[i], device_id_type=pl.DeviceIdType.MESH
                    )


    def grad_send(l, i):
        return remote(
            gacc.at[l, :, pl.ds(i * GW, GW)], rbuf.at[me], rs_sem.at[l], rr_sem, (jnp.int32(i), l)
        )

    def grads_out(l):
        for i in range(4):
            mine = me == 4 * l + i

            @pl.when(jnp.logical_not(mine))
            def _():
                grad_send(l, i).start()

            @pl.when(mine)
            def _():
                rbuf[me] = gacc[l, :, i * GW : (i + 1) * GW]


    tok_in = pltpu.make_async_copy(tok, xb, io_sem.at[0])
    cot_in = pltpu.make_async_copy(cot, db, io_sem.at[1])

    def first_loads(g, _):
        own_load(g)
        return 0

    lax.fori_loop(0, 8, first_loads, 0)
    tok_in.start()
    cot_in.start()
    at = jnp.int32
    for g in (0, 2, 1, 5):
        with jax.named_scope("hop1"):
            hop1(at(g))
    for b in range(2):
        pltpu.make_async_copy(gst.at[b, pl.ds(0, MX)], gp.at[4 * L, pl.ds(b * MX, MX), :], gp_sem.at[b]).start()
    for l in range(L):
        acat[l] = right_parts(jnp.concatenate([a4[l], jnp.zeros((4, H), F32)], axis=0))
        bcat[l] = right_parts(jnp.concatenate([b4[l], jnp.zeros((4, F), F32)], axis=0))
    with jax.named_scope("tw"):
        tok_in.wait()
    cot_in.wait()
    with jax.named_scope("hop2"):
        hop2(at(0))


    def inv_rms(rf):
        return lax.rsqrt(jnp.mean(rf * rf, axis=-1, keepdims=True) + NORM_EPS)

    def x_save(l):
        return pltpu.make_async_copy(xb, xs.at[l - 1], io_sem.at[0])

    def slope_out(b, lk, m):
        return pltpu.make_async_copy(gst.at[b, pl.ds(0, MX)], gp.at[lk, rows_of(m, MX), :], gp_sem.at[b])

    def gp_in(t):
        lk = 4 * (L - 1 - lax.div(t, 16)) + quarter(lax.div(lax.rem(t, 16), 4))
        b = rem3(t)
        return pltpu.make_async_copy(gp.at[lk, rows_of(lax.rem(t, 4), MU), :], gst.at[b], gp_sem.at[b])

    blocks = [(rb, cb) for cb in range(0, 1024, CB) for rb in range(0, MX, RB)]

    def activate(src, k, m, slot, part):
        for rb, cb in blocks[part * len(blocks) // 5 : (part + 1) * len(blocks) // 5]:
            act, slope = gelu_and_slope(src[rb : rb + RB, cb : cb + CB].astype(BF))
            r = pl.ds(pl.multiple_of(m * MX + rb, RB), RB)
            sd[r, pl.ds(pl.multiple_of(k * 1024 + cb, CB), CB)] = act
            gst[slot, rb : rb + RB, cb : cb + CB] = slope

    def up_tile(l, k, m, dst, kp, mp, src, slot):
        r = rows_of(m, MX)
        cols = pl.ds(pl.multiple_of(k * 1024, 1024), 1024)
        acc = None
        for kt in range(5):
            if kt < 4:
                rhs = w[k, 4 * kt : 4 * kt + 4]
                rhs = jnp.concatenate([rhs[:, n * 64 : (n + 1) * 64, :].reshape(256, 256) for n in range(4)], axis=1)
                term = nn(ub[r, kt * 256 : (kt + 1) * 256], rhs)
            else:
                term = tn(vcat[l, :, r], bcat[l, :, cols])
            acc = term if acc is None else acc + term
            activate(src, kp, mp, slot, kt)
        dst[...] = acc

    def forward_layer(l, _):
        @pl.when(l > 0)
        def _():
            x_save(l).start()

        def prep(m, _):
            r = rows_of(m, MU)
            rf = xb[r, :].astype(F32)
            u = (rf * inv_rms(rf)).astype(BF)
            ub[r, :] = u
            vcat[l, :, r] = left_parts(sum_parts(nt(acat[l, 0:32], u)))
            return 0

        with jax.named_scope("prep"):
            lax.fori_loop(0, T // MU, prep, 0)

        @pl.when(l == 0)
        def _():
            for step, g in ((hop1, 3), (hop2, 1), (hop3, 0), (hop2, 2), (hop1, 4), (hop2, 3), (hop3, 1), (hand_over, 0)):
                with jax.named_scope("st0"):
                    step(at(g))

        def slopes(t):
            slot = rem3(2 * l + t)
            old = jnp.maximum(t - 2, 0)
            lk = jnp.where(t == 1, 4 * L, 4 * l + lax.div(old, 4))
            lk = jnp.where(t == 0, jnp.where(l == 0, 4 * L, 4 * l - 1), lk)
            m = jnp.where(t == 0, 3, jnp.where(t == 1, 2, lax.rem(old, 4)))
            slope_out(jnp.where(slot == 0, 2, slot - 1), lk, m).start()
            slope_out(slot, 0, 0).wait()
            return slot

        def up_step(t, _):
            k, m = lax.div(t, 4), lax.rem(t, 4)
            g = 8 * l + k

            due = t == 2
            j = at(0)
            for i in (6, 10, 13):
                due = jnp.logical_or(due, t == i)
                j = j + jnp.where(t >= i, 1, 0)

            @pl.when(m == 0)
            def _():
                @pl.when(k > 0)
                def _():
                    release(g - 1)

                with jax.named_scope("arr"):
                    arrive(g)

            @pl.when(l == 0)
            def _():
                for when, steps in FIRST_LAYER:

                    @pl.when(t == when)
                    def _():
                        for kind, chunk in steps:
                            with jax.named_scope("st1"):
                                (hop1, hop2, hop3, hand_over)[kind](at(chunk))

            @pl.when(jnp.logical_and(l > 0, jnp.logical_or(due, m == 1)))
            def _():
                @pl.when(due)
                def _():
                    with jax.named_scope("ev"):
                        event(8 * l + j)

                @pl.when(m == 1)
                def _():
                    with jax.named_scope("rf"):
                        refill(g)

            tp = jnp.maximum(t - 1, 0)
            kp, mp = lax.div(tp, 4), lax.rem(tp, 4)
            slot = slopes(t)

            @pl.when(lax.rem(t, 2) == 0)
            def _():
                with jax.named_scope("up"):
                    up_tile(l, k, m, pre0, kp, mp, pre1, slot)

            @pl.when(lax.rem(t, 2) == 1)
            def _():
                with jax.named_scope("up"):
                    up_tile(l, k, m, pre1, kp, mp, pre0, slot)

            return 0

        lax.fori_loop(0, 16, up_step, 0)
        release(8 * l + 3)
        slot = slopes(at(16))
        for part in range(5):
            activate(pre1, 3, at(3), slot, part)

        @pl.when(l == L - 1)
        def _():
            slope_out((2 * (L - 1) + 16) % 3, 4 * L - 1, at(3)).start()

        @pl.when(l > 0)
        def _():
            x_save(l).wait()

        def down_step(t, _):
            k, m = lax.div(t, 2), lax.rem(t, 2)
            g = 8 * l + 4 + k

            @pl.when(m == 0)
            def _():
                @pl.when(k > 0)
                def _():
                    release(g - 1)

                with jax.named_scope("arr"):
                    arrive(g)

                with jax.named_scope("ev"):
                    event(g)

            @pl.when(jnp.logical_and(l == L - 1, t == 5))
            def _():
                for b in range(3):
                    slope_out(b, 0, at(0)).wait()
                gp_in(at(0)).start()
                gp_in(at(1)).start()

            @pl.when(m == 1)
            def _():
                with jax.named_scope("rf"):
                    refill(g)

            r = rows_of(m, MD)
            cols = pl.ds(pl.multiple_of(k * 256, 256), 256)
            with jax.named_scope("dn"):
                step = nn(sd[r, :], w[4 + k].reshape(F, 256))
                xb[r, cols] = (xb[r, cols].astype(F32) + step).astype(BF)
            return 0

        lax.fori_loop(0, 8, down_step, 0)
        release(8 * l + 7)
        return 0

    lax.fori_loop(0, L, forward_layer, 0)


    x_final = pltpu.make_async_copy(xb, xout, io_sem.at[0])
    x_final.start()
    with jax.named_scope("gat"):
        gather(1, L - 1)


    def x_load(l, start):
        @pl.when(l > 0)
        def _():
            cp = pltpu.make_async_copy(xs.at[l - 1], xb, io_sem.at[0])
            cp.start() if start else cp.wait()

        @pl.when(l == 0)
        def _():
            cp = pltpu.make_async_copy(tok, xb, io_sem.at[0])
            cp.start() if start else cp.wait()

    def backward_layer(rl, _):
        l = L - 1 - rl
        dlt[...] = jnp.zeros_like(dlt)
        gb[...] = jnp.zeros_like(gb)
        ga[...] = jnp.zeros_like(ga)

        def down_step(i, _):
            @pl.when(i == 1)
            def _():
                with jax.named_scope("gat"):
                    gather(0, l)

            @pl.when(i == 2)
            def _():
                @pl.when(l == L - 1)
                def _():
                    x_final.wait()

                x_load(l, True)

            with jax.named_scope("bev"):
                b_events(1, l, i)
            q = quarter(i)
            cols = pl.ds(pl.multiple_of(q * 1024, 1024), 1024)

            def tile(m, _):
                t = rl * 16 + i * 4 + m

                @pl.when(t + 2 < 16 * L)
                def _():
                    gp_in(t + 2).start()

                gp_in(t).wait()
                r = rows_of(m, MU)
                acc = None
                for k in range(4):
                    rhs = w[4 + k, pl.ds(4 * q, 4)].reshape(1024, 256)
                    term = nt(db[r, k * 256 : (k + 1) * 256], rhs)
                    acc = term if acc is None else acc + term
                d = (acc.astype(BF).astype(F32) * gst[rem3(t)]).astype(BF)
                sd[r, cols] = d
                dlt[:, r] += nt(bcat[l, 0:32, cols], d)
                gb[:, cols] += nn(vcat[l, 0:32, r], d)
                return 0

            with jax.named_scope("p1"):
                lax.fori_loop(0, T // MU, tile, 0)
            return 0

        lax.fori_loop(0, 4, down_step, 0)
        with jax.named_scope("brel"):
            b_release(1, l)
        dcat[...] = left_parts(sum_parts(dlt[...]))
        gb8 = sum_parts(gb[...])
        gacc[l, :, 0:2048] = gb8[:, 0:2048] + pltpu.roll(gb8[:, 2048:4096], 4, 0)

        def up_step(i, _):
            @pl.when(jnp.logical_and(i == 1, l > 0))
            def _():
                with jax.named_scope("gat"):
                    gather(1, l - 1)

            with jax.named_scope("bev"):
                b_events(0, l, i)
            q = quarter(i)
            cols = pl.ds(pl.multiple_of(q * 256, 256), 256)

            def tile(m, _):
                r = rows_of(m, MD)
                acc = None
                for k in range(4):
                    for n in range(4):
                        rhs = w[k, pl.ds(4 * q, 4), n * 64 : (n + 1) * 64, :].reshape(256, 256)
                        j = 4 * k + n
                        term = nt(sd[r, j * 256 : (j + 1) * 256], rhs)
                        acc = term if acc is None else acc + term
                side = tn(dcat[:, r], acat[l, :, cols]).astype(BF)
                ub[r, cols] = acc.astype(BF) + side
                return 0

            with jax.named_scope("p2"):
                lax.fori_loop(0, T // MD, tile, 0)
            return 0

        lax.fori_loop(0, 4, up_step, 0)
        with jax.named_scope("brel"):
            b_release(0, l)
        x_load(l, False)

        def finish(m, _):
            r = rows_of(m, MU)
            rf = xb[r, :].astype(F32)
            inv = inv_rms(rf)
            dn = ub[r, :].astype(F32)
            dot = jnp.mean(rf * dn, axis=-1, keepdims=True)
            db[r, :] = (db[r, :].astype(F32) + inv * dn - rf * ((inv * inv * inv) * dot)).astype(BF)
            u = (rf * inv).astype(BF)
            ga[...] += nn(dcat[0:32, r], u)
            return 0

        with jax.named_scope("fin"):
            lax.fori_loop(0, T // MU, finish, 0)
        ga8 = sum_parts(ga[...])
        gacc[l, :, 2048:2560] = ga8[:, 0:512] + pltpu.roll(ga8[:, 512:1024], 4, 0)
        with jax.named_scope("gout"):
            grads_out(l)
        return 0

    lax.fori_loop(0, L, backward_layer, 0)


    g_final = pltpu.make_async_copy(db, gtok, io_sem.at[1])
    g_final.start()
    others = rbuf.at[pl.ds(0, 15)]
    with jax.named_scope("redw"):
        remote(others, others, rr_sem, rr_sem, partner).wait_recv()
    total = rbuf[0]
    for i in range(1, 16):
        total = total + rbuf[i]
    gall[me] = total

    def share(o, _):
        @pl.when(o != me)
        def _():
            remote(gall.at[me], gall.at[me], as_sem, ar_sem, (lax.rem(o, 4), lax.div(o, 4))).start()

        return 0

    lax.fori_loop(0, 16, share, 0)
    others = gall.at[pl.ds(0, 15)]
    with jax.named_scope("allw"):
        remote(others, others, as_sem, ar_sem, partner).wait_send()
        remote(others, others, as_sem, ar_sem, partner).wait_recv()
    for l in range(L):
        for i in range(4):

            @pl.when(me != 4 * l + i)
            def _():
                grad_send(jnp.int32(l), i).wait_send()

    shares = pltpu.make_async_copy(gall, gout, io_sem.at[0])
    shares.start()
    g_final.wait()
    shares.wait()


def solution(mesh):
    tok_spec = P(GROUP, None)
    weight_spec = P(None, GROUP, None)

    def device_step(tokens, cotangent, up, down, lora_a, lora_b):
        hbm = pl.BlockSpec(memory_space=pltpu.HBM)
        vmem = pl.BlockSpec(memory_space=pltpu.VMEM)
        shape = jax.ShapeDtypeStruct
        dma, regular = pltpu.SemaphoreType.DMA, pltpu.SemaphoreType.REGULAR
        outs = pl.pallas_call(
            kernel,
            name="stack",
            out_shape=[
                shape((T, H), BF),
                shape((T, H), BF),
                shape((16, 8, GW), F32),
                shape((4 * L + 1, T, 1024), F32),
                shape((L - 1, T, H), BF),
                shape((L, 8, 4, 256, 256), BF),
            ],
            in_specs=[hbm, hbm, hbm, hbm, vmem, vmem],
            out_specs=[hbm] * 6,
            scratch_shapes=[
                pltpu.VMEM((8, 16, 256, 256), BF),
                pltpu.VMEM((T, F), BF),
                pltpu.VMEM((T, H), BF),
                pltpu.VMEM((T, H), BF),
                pltpu.VMEM((T, H), BF),
                pltpu.VMEM((3, MU, 1024), F32),
                pltpu.VMEM((MX, 1024), F32),
                pltpu.VMEM((MX, 1024), F32),
                pltpu.VMEM((L, 48, H), BF),
                pltpu.VMEM((L, 48, F), BF),
                pltpu.VMEM((L, 48, T), BF),
                pltpu.VMEM((48, T), BF),
                pltpu.VMEM((32, T), F32),
                pltpu.VMEM((32, F), F32),
                pltpu.VMEM((32, H), F32),
                pltpu.VMEM((L, 8, 4 * GW), F32),
                pltpu.VMEM((16, 8, GW), F32),
                pltpu.VMEM((16, 8, GW), F32),
                dma((8,)),
                dma((4, 8)),
                dma((4, 8)),
                dma((8,)),
                dma((3,)),
                dma((2,)),
                dma((2,)),
                dma((2, 5)),
                dma((2, 5)),
                dma((L,)),
                dma,
                dma,
                dma,
                regular((4, 8)),
            ],
            compiler_params=pltpu.CompilerParams(
                vmem_limit_bytes=67000000,
                has_side_effects=True,
            ),
        )(tokens, cotangent, up, down, lora_a.transpose(0, 2, 1), lora_b)
        x_out, g_tok, shares = outs[:3]
        grads = shares.reshape(L, 4, 2, 4, GW).transpose(0, 2, 3, 1, 4).reshape(L, 2, 4, 4 * GW)
        grad_b = grads[..., 0:2048].transpose(0, 2, 1, 3).reshape(L, 4, F)
        grad_a = grads[..., 2048:2560].transpose(0, 1, 3, 2).reshape(L, H, 4)
        return x_out, g_tok, grad_a, grad_b

    return jax.shard_map(
        device_step,
        mesh=mesh,
        in_specs=(tok_spec, tok_spec, weight_spec, weight_spec, P(), P()),
        out_specs=(tok_spec, tok_spec, P(), P()),
        check_vma=False,
    )
```

```python
import jax
import jax.numpy as jnp
from jax import lax
from jax.experimental import pallas as pl
from jax.experimental.pallas import tpu as pltpu
from jax.sharding import PartitionSpec as P

GROUP = ("data", "local")
NORM_EPS = 1e-6
BF = jnp.bfloat16
F32 = jnp.float32
C0 = 0.7978845608028654
K0 = 0.044715

T = 2048
H = 1024
F = 4096
L = 4
NG = 8 * L
MU = 512
MD = 1024
MX = 512
RB, CB = 16, 256
ROWS = ((0, 96), (96, 80), (176, 80))
FIRST_LAYER = (
    (1, ((2, 2),)),
    (2, ((3, 1), (1, 5))),
    (3, ((1, 4),)),
    (5, ((2, 3), (3, 2), (0, 7))),
    (6, ((0, 6),)),
    (7, ((2, 4),)),
    (8, ((0, 8),)),
    (10, ((3, 3), (0, 9))),
    (11, ((1, 6),)),
    (13, ((3, 4), (1, 7), (2, 5))),
    (14, ((1, 8), (2, 6), (0, 10))),
    (15, ((3, 5), (1, 9), (2, 7))),
)
GW = 640


def nn(a, b):
    return lax.dot_general(a, b, (((1,), (0,)), ((), ())), preferred_element_type=F32)


def nt(a, b):
    return lax.dot_general(a, b, (((1,), (1,)), ((), ())), preferred_element_type=F32)


def tn(a, b):
    return lax.dot_general(a, b, (((0,), (0,)), ((), ())), preferred_element_type=F32)


def split3(v):
    p1 = v.astype(BF).astype(F32)
    rest = v - p1
    p2 = rest.astype(BF).astype(F32)
    return p1, p2, (rest - p2).astype(BF).astype(F32)


def left_parts(v):
    p1, p2, p3 = split3(v)
    return jnp.concatenate([p1, p2, p3, p1, p1, p2], axis=0).astype(BF)


def right_parts(v):
    p1, p2, p3 = split3(v)
    return jnp.concatenate([p3, p2, p1, p1, p2, p1], axis=0).astype(BF)


def sum_parts(v):
    return v[0:8] + v[8:16] + v[16:24]


def gelu_and_slope(pre):
    x = pre.astype(F32)
    sq = x * x
    half = 0.5 * jnp.tanh(x * (sq * (C0 * K0) + C0)) + 0.5
    act = x * half
    slope = (act * (1.0 - half)) * (sq * (6.0 * C0 * K0) + 2.0 * C0) + half
    return act.astype(BF), slope


def rem3(t):
    return t - 3 * lax.div(t * 43, 128)


def rows_of(m, size):
    return pl.ds(pl.multiple_of(m * size, size), size)


def kernel(
    tok, cot, up, down, a4, b4,
    xout, gtok, gout, gp, xs, kept,
    w, sd, xb, ub, db, gst, pre0, pre1, acat, bcat, vcat, dcat, dlt, gb, ga, gacc, rbuf, gall,
    own_sem, fs_sem, fr_sem, kept_sem, gp_sem, io_sem, bo_sem, bs_sem, br_sem, rs_sem, rr_sem, as_sem, ar_sem,
    cred,
):
    data = lax.axis_index("data")
    local = lax.axis_index("local")
    x, c = lax.div(data, 2), lax.rem(data, 2)
    z, y = lax.div(local, 2), lax.rem(local, 2)
    me = data * 4 + local
    dx, dy, dz, dc = 1 - 2 * x, 1 - 2 * y, 1 - 2 * z, 1 - 2 * c
    par = lax.rem(x + y + z, 2)

    def quarter(i):
        hi, lo = lax.div(i, 2), lax.rem(i, 2)
        return 2 * (par + hi - 2 * par * hi) + (c + lo - 2 * c * lo)

    q_own, q_miss = quarter(0), quarter(2)

    def pick(dim, a0, a1, a2):
        return lax.div((1 - dim) * (2 - dim), 2) * a0 + dim * (2 - dim) * a1 + lax.div(dim * (dim - 1), 2) * a2

    def device(dim):
        return (local + pick(dim, 0, dy, 2 * dz), data + pick(dim, 2 * dx, 0, 0))

    neighbours = ((local, data + 2 * dx), (local + dy, data), (local + 2 * dz, data), (local, data + dc))
    partner = neighbours[3]

    def remote(src, dst, ssem, rsem, dev):
        return pltpu.make_async_remote_copy(
            src_ref=src, dst_ref=dst, send_sem=ssem, recv_sem=rsem, device_id=dev, device_id_type=pl.DeviceIdType.MESH
        )


    def own_load(g):
        s, l = lax.rem(g, 8), lax.div(g, 8)

        @pl.when(s < 4)
        def _():
            for n in range(4):
                pltpu.make_async_copy(
                    up.at[l, :, pl.ds(pl.multiple_of(s * 1024 + n * 256, 256), 256)],
                    w.at[s, me, pl.ds(n * 64, 64), :],
                    own_sem.at[s],
                ).start()

        @pl.when(s >= 4)
        def _():
            pltpu.make_async_copy(
                down.at[l, :, pl.ds(pl.multiple_of((s - 4) * 256, 256), 256)], w.at[s, me], own_sem.at[s]
            ).start()

    def colour(g):
        q = rem3(jnp.where(g == 1, 2 + c, jnp.where(g < 3, 1 + 2 * c, g + c)))
        turn = jnp.where(jnp.logical_or(g == 1, g == 2), 2, 1)
        return q, rem3(q + turn), rem3(q + 2 * turn)

    def delta(dim):
        return pick(dim, 8 * dx, dy, 2 * dz)

    def use_credit(g, dim):
        @pl.when(g >= 8)
        def _():
            pl.semaphore_wait(cred.at[dim, lax.rem(g, 8)], 1)

    def send_blocks(g, phase, dim, blocks, dev):
        s = lax.rem(g, 8)
        use_credit(g, dim)
        for b in blocks:
            remote(w.at[s, b], w.at[s, b], fs_sem.at[phase, s], fr_sem.at[phase, s], dev).start()

    def span(g, phase):
        s = lax.rem(g, 8)
        r = w.at[s, pl.ds(0, (1, 2, 4, 8)[phase])]
        return remote(r, r, fs_sem.at[phase, s], fr_sem.at[phase, s], partner)

    def ready(g):
        return jnp.logical_and(g >= 0, g < NG)

    def hop1(g):
        d1, _, _ = colour(g)
        s = lax.rem(g, 8)
        pltpu.make_async_copy(w.at[s, me], w.at[s, me], own_sem.at[s]).wait()
        send_blocks(g, 0, d1, (me,), device(d1))

    def hop2(g):
        d1, d2, _ = colour(g)
        span(g, 0).wait_recv()
        send_blocks(g, 1, d2, (me, me + delta(d1)), device(d2))

    def hop3(g):
        d1, d2, d3 = colour(g)
        e1, e2 = delta(d1), delta(d2)
        span(g, 1).wait_recv()
        send_blocks(g, 2, d3, (me, me + e1, me + e2, me + e1 + e2), device(d3))

    def hand_over(g):
        s = lax.rem(g, 8)
        span(g, 2).wait_recv()
        use_credit(g, 3)
        for h in range(2):
            r2 = w.at[s, pl.ds(8 * h + 4 * c, 4)]
            remote(r2, r2, fs_sem.at[3, s], fr_sem.at[3, s], partner).start()

    def event(j):
        for step, ahead in ((hand_over, 1), (hop2, 5), (hop3, 3)):

            @pl.when(j + ahead < NG)
            def _():
                with jax.named_scope("st"):
                    step(j + ahead)

    def refill(j):
        @pl.when(j + 7 < NG)
        def _():
            hop1(j + 7)

    def keep_copy(g):
        s, l = lax.rem(g, 8), lax.div(g, 8)
        return pltpu.make_async_copy(w.at[s, pl.ds(4 * q_own, 4)], kept.at[l, s], kept_sem.at[s])

    def arrive(g):
        span(g, 3).wait_recv()
        keep_copy(g).start()

    def release(g):
        s = lax.rem(g, 8)
        for phase in range(4):
            span(g, phase).wait_send()
        keep_copy(g).wait()
        for i in range(4):
            pl.semaphore_signal(cred.at[i, s], inc=1, device_id=neighbours[i], device_id_type=pl.DeviceIdType.MESH)

        @pl.when(g + 8 < NG)
        def _():
            own_load(g + 8)


    def whole(m, q):
        return w.at[pl.ds(4 * m, 4), pl.ds(4 * q, 4)]

    def part(ref, dim):
        return ref.at[:, :, pl.ds(*ROWS[dim]), :]

    def b_own(m, l):
        return pltpu.make_async_copy(kept.at[l, pl.ds(4 * m, 4)], whole(m, q_own), bo_sem.at[m])

    def b_send(m, l, i, q):
        src, dst = kept.at[l, pl.ds(4 * m, 4)], whole(m, q)
        if i < 3:
            src, dst = part(src, i), part(dst, i)
        return remote(src, dst, bs_sem.at[m, i], br_sem.at[m, i], neighbours[i])

    def b_forward(m):
        return remote(whole(m, q_miss), whole(m, q_miss), bs_sem.at[m, 4], br_sem.at[m, 4], partner)

    def gather(m, l):
        @pl.when(jnp.logical_or(l < L - 1, m == 0))
        def _():
            b_own(m, l).start()

        for i in range(4):
            for s in range(4):
                pl.semaphore_wait(cred.at[i, 4 * m + s], 1)
            b_send(m, l, i, q_own).start()

    def b_events(m, l, i):
        @pl.when(jnp.logical_and(i == 0, jnp.logical_or(l < L - 1, m == 0)))
        def _():
            b_own(m, l).wait()

        @pl.when(i == 1)
        def _():
            b_send(m, l, 3, quarter(1)).wait_recv()

        @pl.when(i == 2)
        def _():
            for d in range(3):
                b_send(m, l, d, q_miss).wait_recv()
            b_forward(m).start()

        @pl.when(i == 3)
        def _():
            b_forward(m).wait_recv()

    def b_release(m, l):
        b_forward(m).wait_send()
        for i in range(4):
            b_send(m, l, i, q_own).wait_send()

        @pl.when(l > 0)
        def _():
            for i in range(4):
                for s in range(4):
                    pl.semaphore_signal(
                        cred.at[i, 4 * m + s], inc=1, device_id=neighbours[i], device_id_type=pl.DeviceIdType.MESH
                    )


    def grad_send(l, i):
        return remote(
            gacc.at[l, :, pl.ds(i * GW, GW)], rbuf.at[me], rs_sem.at[l], rr_sem, (jnp.int32(i), l)
        )

    def grads_out(l):
        for i in range(4):
            mine = me == 4 * l + i

            @pl.when(jnp.logical_not(mine))
            def _():
                grad_send(l, i).start()

            @pl.when(mine)
            def _():
                rbuf[me] = gacc[l, :, i * GW : (i + 1) * GW]


    tok_in = pltpu.make_async_copy(tok, xb, io_sem.at[0])
    cot_in = pltpu.make_async_copy(cot, db, io_sem.at[1])

    def first_loads(g, _):
        own_load(g)
        return 0

    lax.fori_loop(0, 8, first_loads, 0)
    tok_in.start()
    at = jnp.int32
    for g in (0, 2, 1, 5):
        with jax.named_scope("hop1"):
            hop1(at(g))
    for b in range(2):
        pltpu.make_async_copy(gst.at[b, pl.ds(0, MX)], gp.at[4 * L, pl.ds(b * MX, MX), :], gp_sem.at[b]).start()
    with jax.named_scope("hop2"):
        hop2(at(0))
    for l in range(L):
        acat[l] = right_parts(jnp.concatenate([a4[l], jnp.zeros((4, H), F32)], axis=0))
        bcat[l] = right_parts(jnp.concatenate([b4[l], jnp.zeros((4, F), F32)], axis=0))
    with jax.named_scope("tw"):
        tok_in.wait()


    def inv_rms(rf):
        return lax.rsqrt(jnp.mean(rf * rf, axis=-1, keepdims=True) + NORM_EPS)

    def x_save(l):
        return pltpu.make_async_copy(xb, xs.at[l - 1], io_sem.at[0])

    def slope_out(b, lk, m):
        return pltpu.make_async_copy(gst.at[b, pl.ds(0, MX)], gp.at[lk, rows_of(m, MX), :], gp_sem.at[b])

    def gp_in(t):
        lk = 4 * (L - 1 - lax.div(t, 16)) + quarter(lax.div(lax.rem(t, 16), 4))
        b = rem3(t)
        return pltpu.make_async_copy(gp.at[lk, rows_of(lax.rem(t, 4), MU), :], gst.at[b], gp_sem.at[b])

    blocks = [(rb, cb) for cb in range(0, 1024, CB) for rb in range(0, MX, RB)]

    def activate(src, k, m, slot, part):
        for rb, cb in blocks[part * len(blocks) // 5 : (part + 1) * len(blocks) // 5]:
            act, slope = gelu_and_slope(src[rb : rb + RB, cb : cb + CB].astype(BF))
            r = pl.ds(pl.multiple_of(m * MX + rb, RB), RB)
            sd[r, pl.ds(pl.multiple_of(k * 1024 + cb, CB), CB)] = act
            gst[slot, rb : rb + RB, cb : cb + CB] = slope

    def up_tile(l, k, m, dst, kp, mp, src, slot):
        r = rows_of(m, MX)
        cols = pl.ds(pl.multiple_of(k * 1024, 1024), 1024)
        acc = None
        for kt in range(5):
            if kt < 4:
                rhs = w[k, 4 * kt : 4 * kt + 4]
                rhs = jnp.concatenate([rhs[:, n * 64 : (n + 1) * 64, :].reshape(256, 256) for n in range(4)], axis=1)
                term = nn(ub[r, kt * 256 : (kt + 1) * 256], rhs)
            else:
                term = tn(vcat[l, :, r], bcat[l, :, cols])
            acc = term if acc is None else acc + term
            activate(src, kp, mp, slot, kt)
        dst[...] = acc

    def forward_layer(l, _):
        @pl.when(l > 0)
        def _():
            x_save(l).start()

        def prep(m, _):
            r = rows_of(m, MU)
            rf = xb[r, :].astype(F32)
            u = (rf * inv_rms(rf)).astype(BF)
            ub[r, :] = u
            vcat[l, :, r] = left_parts(sum_parts(nt(acat[l, 0:32], u)))
            return 0

        with jax.named_scope("prep"):
            lax.fori_loop(0, T // MU, prep, 0)

        @pl.when(l == 0)
        def _():
            for step, g in ((hop1, 3), (hop2, 1), (hop3, 0), (hop2, 2), (hop1, 4), (hop2, 3), (hop3, 1), (hand_over, 0)):
                with jax.named_scope("st0"):
                    step(at(g))

        def slopes(t):
            slot = rem3(2 * l + t)
            old = jnp.maximum(t - 2, 0)
            lk = jnp.where(t == 1, 4 * L, 4 * l + lax.div(old, 4))
            lk = jnp.where(t == 0, jnp.where(l == 0, 4 * L, 4 * l - 1), lk)
            m = jnp.where(t == 0, 3, jnp.where(t == 1, 2, lax.rem(old, 4)))
            slope_out(jnp.where(slot == 0, 2, slot - 1), lk, m).start()
            slope_out(slot, 0, 0).wait()
            return slot

        def up_step(t, _):
            k, m = lax.div(t, 4), lax.rem(t, 4)
            g = 8 * l + k

            due = t == 1
            j = at(0)
            for i in (5, 9, 12, 15):
                due = jnp.logical_or(due, t == i)
                j = j + jnp.where(t >= i, 1, 0)

            @pl.when(m == 0)
            def _():
                @pl.when(k > 0)
                def _():
                    release(g - 1)

                with jax.named_scope("arr"):
                    arrive(g)

            @pl.when(l == 0)
            def _():
                for when, steps in FIRST_LAYER:

                    @pl.when(t == when)
                    def _():
                        for kind, chunk in steps:
                            with jax.named_scope("st1"):
                                (hop1, hop2, hop3, hand_over)[kind](at(chunk))

            @pl.when(jnp.logical_and(l > 0, jnp.logical_or(due, m == 1)))
            def _():
                @pl.when(due)
                def _():
                    with jax.named_scope("ev"):
                        event(8 * l + j)

                @pl.when(m == 1)
                def _():
                    with jax.named_scope("rf"):
                        refill(g)

            tp = jnp.maximum(t - 1, 0)
            kp, mp = lax.div(tp, 4), lax.rem(tp, 4)
            slot = slopes(t)

            @pl.when(lax.rem(t, 2) == 0)
            def _():
                with jax.named_scope("up"):
                    up_tile(l, k, m, pre0, kp, mp, pre1, slot)

            @pl.when(lax.rem(t, 2) == 1)
            def _():
                with jax.named_scope("up"):
                    up_tile(l, k, m, pre1, kp, mp, pre0, slot)

            return 0

        lax.fori_loop(0, 16, up_step, 0)
        release(8 * l + 3)
        slot = slopes(at(16))
        for part in range(5):
            activate(pre1, 3, at(3), slot, part)

        @pl.when(l == L - 1)
        def _():
            cot_in.start()
            slope_out((2 * (L - 1) + 16) % 3, 4 * L - 1, at(3)).start()

        @pl.when(l > 0)
        def _():
            x_save(l).wait()

        def down_step(t, _):
            k, m = lax.div(t, 2), lax.rem(t, 2)
            g = 8 * l + 4 + k

            @pl.when(m == 0)
            def _():
                @pl.when(k > 0)
                def _():
                    release(g - 1)

                with jax.named_scope("arr"):
                    arrive(g)

                @pl.when(jnp.logical_or(k == 1, k == 2))
                def _():
                    with jax.named_scope("ev"):
                        event(g)

            @pl.when(jnp.logical_and(l == L - 1, t == 5))
            def _():
                for b in range(3):
                    slope_out(b, 0, at(0)).wait()
                gp_in(at(0)).start()
                gp_in(at(1)).start()

            @pl.when(m == 1)
            def _():
                with jax.named_scope("rf"):
                    refill(g)

                @pl.when(k == 3)
                def _():
                    with jax.named_scope("ev"):
                        event(g)

            r = rows_of(m, MD)
            cols = pl.ds(pl.multiple_of(k * 256, 256), 256)
            with jax.named_scope("dn"):
                step = nn(sd[r, :], w[4 + k].reshape(F, 256))
                xb[r, cols] = (xb[r, cols].astype(F32) + step).astype(BF)
            return 0

        lax.fori_loop(0, 8, down_step, 0)
        release(8 * l + 7)
        return 0

    lax.fori_loop(0, L, forward_layer, 0)


    x_final = pltpu.make_async_copy(xb, xout, io_sem.at[0])
    x_final.start()
    with jax.named_scope("gat"):
        gather(1, L - 1)
    cot_in.wait()


    def x_load(l, start):
        @pl.when(l > 0)
        def _():
            cp = pltpu.make_async_copy(xs.at[l - 1], xb, io_sem.at[0])
            cp.start() if start else cp.wait()

        @pl.when(l == 0)
        def _():
            cp = pltpu.make_async_copy(tok, xb, io_sem.at[0])
            cp.start() if start else cp.wait()

    def backward_layer(rl, _):
        l = L - 1 - rl
        dlt[...] = jnp.zeros_like(dlt)
        gb[...] = jnp.zeros_like(gb)
        ga[...] = jnp.zeros_like(ga)

        def down_step(i, _):
            @pl.when(i == 1)
            def _():
                with jax.named_scope("gat"):
                    gather(0, l)

            @pl.when(i == 2)
            def _():
                @pl.when(l == L - 1)
                def _():
                    x_final.wait()

                x_load(l, True)

            with jax.named_scope("bev"):
                b_events(1, l, i)
            q = quarter(i)
            cols = pl.ds(pl.multiple_of(q * 1024, 1024), 1024)

            def tile(m, _):
                t = rl * 16 + i * 4 + m

                @pl.when(t + 2 < 16 * L)
                def _():
                    gp_in(t + 2).start()

                gp_in(t).wait()
                r = rows_of(m, MU)
                acc = None
                for k in range(4):
                    rhs = w[4 + k, pl.ds(4 * q, 4)].reshape(1024, 256)
                    term = nt(db[r, k * 256 : (k + 1) * 256], rhs)
                    acc = term if acc is None else acc + term
                d = (acc.astype(BF).astype(F32) * gst[rem3(t)]).astype(BF)
                sd[r, cols] = d
                dlt[:, r] += nt(bcat[l, 0:32, cols], d)
                gb[:, cols] += nn(vcat[l, 0:32, r], d)
                return 0

            with jax.named_scope("p1"):
                lax.fori_loop(0, T // MU, tile, 0)
            return 0

        lax.fori_loop(0, 4, down_step, 0)
        with jax.named_scope("brel"):
            b_release(1, l)
        dcat[...] = left_parts(sum_parts(dlt[...]))
        gb8 = sum_parts(gb[...])
        gacc[l, :, 0:2048] = gb8[:, 0:2048] + pltpu.roll(gb8[:, 2048:4096], 4, 0)

        def up_step(i, _):
            @pl.when(jnp.logical_and(i == 1, l > 0))
            def _():
                with jax.named_scope("gat"):
                    gather(1, l - 1)

            with jax.named_scope("bev"):
                b_events(0, l, i)
            q = quarter(i)
            cols = pl.ds(pl.multiple_of(q * 256, 256), 256)

            def tile(m, _):
                r = rows_of(m, MD)
                acc = None
                for k in range(4):
                    for n in range(4):
                        rhs = w[k, pl.ds(4 * q, 4), n * 64 : (n + 1) * 64, :].reshape(256, 256)
                        j = 4 * k + n
                        term = nt(sd[r, j * 256 : (j + 1) * 256], rhs)
                        acc = term if acc is None else acc + term
                side = tn(dcat[:, r], acat[l, :, cols]).astype(BF)
                ub[r, cols] = acc.astype(BF) + side
                return 0

            with jax.named_scope("p2"):
                lax.fori_loop(0, T // MD, tile, 0)
            return 0

        lax.fori_loop(0, 4, up_step, 0)
        with jax.named_scope("brel"):
            b_release(0, l)
        x_load(l, False)

        def finish(m, _):
            r = rows_of(m, MU)
            rf = xb[r, :].astype(F32)
            inv = inv_rms(rf)
            dn = ub[r, :].astype(F32)
            dot = jnp.mean(rf * dn, axis=-1, keepdims=True)
            db[r, :] = (db[r, :].astype(F32) + inv * dn - rf * ((inv * inv * inv) * dot)).astype(BF)
            u = (rf * inv).astype(BF)
            ga[...] += nn(dcat[0:32, r], u)
            return 0

        with jax.named_scope("fin"):
            lax.fori_loop(0, T // MU, finish, 0)
        ga8 = sum_parts(ga[...])
        gacc[l, :, 2048:2560] = ga8[:, 0:512] + pltpu.roll(ga8[:, 512:1024], 4, 0)
        with jax.named_scope("gout"):
            grads_out(l)
        return 0

    lax.fori_loop(0, L, backward_layer, 0)


    g_final = pltpu.make_async_copy(db, gtok, io_sem.at[1])
    g_final.start()
    others = rbuf.at[pl.ds(0, 15)]
    with jax.named_scope("redw"):
        remote(others, others, rr_sem, rr_sem, partner).wait_recv()
    total = rbuf[0]
    for i in range(1, 16):
        total = total + rbuf[i]
    gall[me] = total

    def share(o, _):
        @pl.when(o != me)
        def _():
            remote(gall.at[me], gall.at[me], as_sem, ar_sem, (lax.rem(o, 4), lax.div(o, 4))).start()

        return 0

    lax.fori_loop(0, 16, share, 0)
    others = gall.at[pl.ds(0, 15)]
    with jax.named_scope("allw"):
        remote(others, others, as_sem, ar_sem, partner).wait_send()
        remote(others, others, as_sem, ar_sem, partner).wait_recv()
    for l in range(L):
        for i in range(4):

            @pl.when(me != 4 * l + i)
            def _():
                grad_send(jnp.int32(l), i).wait_send()

    shares = pltpu.make_async_copy(gall, gout, io_sem.at[0])
    shares.start()
    g_final.wait()
    shares.wait()


def solution(mesh):
    tok_spec = P(GROUP, None)
    weight_spec = P(None, GROUP, None)

    def device_step(tokens, cotangent, up, down, lora_a, lora_b):
        hbm = pl.BlockSpec(memory_space=pltpu.HBM)
        vmem = pl.BlockSpec(memory_space=pltpu.VMEM)
        shape = jax.ShapeDtypeStruct
        dma, regular = pltpu.SemaphoreType.DMA, pltpu.SemaphoreType.REGULAR
        outs = pl.pallas_call(
            kernel,
            name="stack",
            out_shape=[
                shape((T, H), BF),
                shape((T, H), BF),
                shape((16, 8, GW), F32),
                shape((4 * L + 1, T, 1024), F32),
                shape((L - 1, T, H), BF),
                shape((L, 8, 4, 256, 256), BF),
            ],
            in_specs=[hbm, hbm, hbm, hbm, vmem, vmem],
            out_specs=[hbm] * 6,
            scratch_shapes=[
                pltpu.VMEM((8, 16, 256, 256), BF),
                pltpu.VMEM((T, F), BF),
                pltpu.VMEM((T, H), BF),
                pltpu.VMEM((T, H), BF),
                pltpu.VMEM((T, H), BF),
                pltpu.VMEM((3, MU, 1024), F32),
                pltpu.VMEM((MX, 1024), F32),
                pltpu.VMEM((MX, 1024), F32),
                pltpu.VMEM((L, 48, H), BF),
                pltpu.VMEM((L, 48, F), BF),
                pltpu.VMEM((L, 48, T), BF),
                pltpu.VMEM((48, T), BF),
                pltpu.VMEM((32, T), F32),
                pltpu.VMEM((32, F), F32),
                pltpu.VMEM((32, H), F32),
                pltpu.VMEM((L, 8, 4 * GW), F32),
                pltpu.VMEM((16, 8, GW), F32),
                pltpu.VMEM((16, 8, GW), F32),
                dma((8,)),
                dma((4, 8)),
                dma((4, 8)),
                dma((8,)),
                dma((3,)),
                dma((2,)),
                dma((2,)),
                dma((2, 5)),
                dma((2, 5)),
                dma((L,)),
                dma,
                dma,
                dma,
                regular((4, 8)),
            ],
            compiler_params=pltpu.CompilerParams(
                vmem_limit_bytes=67000000,
                has_side_effects=True,
            ),
        )(tokens, cotangent, up, down, lora_a.transpose(0, 2, 1), lora_b)
        x_out, g_tok, shares = outs[:3]
        grads = shares.reshape(L, 4, 2, 4, GW).transpose(0, 2, 3, 1, 4).reshape(L, 2, 4, 4 * GW)
        grad_b = grads[..., 0:2048].transpose(0, 2, 1, 3).reshape(L, 4, F)
        grad_a = grads[..., 2048:2560].transpose(0, 1, 3, 2).reshape(L, H, 4)
        return x_out, g_tok, grad_a, grad_b

    return jax.shard_map(
        device_step,
        mesh=mesh,
        in_specs=(tok_spec, tok_spec, weight_spec, weight_spec, P(), P()),
        out_specs=(tok_spec, tok_spec, P(), P()),
        check_vma=False,
    )
```

```python
import jax
import jax.numpy as jnp
from jax import lax
from jax.experimental import pallas as pl
from jax.experimental.pallas import tpu as pltpu
from jax.sharding import PartitionSpec as P

GROUP = ("data", "local")
NORM_EPS = 1e-6
BF = jnp.bfloat16
F32 = jnp.float32
C0 = 0.7978845608028654
K0 = 0.044715

T = 2048
H = 1024
F = 4096
L = 4
NG = 8 * L
MU = 512
MD = 1024
MX = 512
RB, CB = 16, 256
ROWS = ((0, 96), (96, 80), (176, 80))
FIRST_LAYER = (
    (0, ((1, 4), (2, 3))),
    (2, ((3, 1), (1, 6))),
    (5, ((2, 4),)),
    (6, ((0, 8), (3, 2))),
    (8, ((2, 5), (3, 3), (1, 7))),
    (9, ((1, 8),)),
    (12, ((3, 4), (2, 6))),
    (13, ((0, 10), (0, 9))),
    (14, ((2, 7),)),
    (16, ((1, 9), (3, 5))),
    (17, ((0, 11), (2, 8))),
    (18, ((3, 6), (1, 10))),
    (19, ((2, 9),)),
    (20, ((3, 7), (0, 12), (1, 11))),
    (23, ((0, 13), (1, 12), (0, 14), (2, 10), (3, 8))),
)
GW = 640


def nn(a, b):
    return lax.dot_general(a, b, (((1,), (0,)), ((), ())), preferred_element_type=F32)


def nt(a, b):
    return lax.dot_general(a, b, (((1,), (1,)), ((), ())), preferred_element_type=F32)


def tn(a, b):
    return lax.dot_general(a, b, (((0,), (0,)), ((), ())), preferred_element_type=F32)


def split3(v):
    p1 = v.astype(BF).astype(F32)
    rest = v - p1
    p2 = rest.astype(BF).astype(F32)
    return p1, p2, (rest - p2).astype(BF).astype(F32)


def left_parts(v):
    p1, p2, p3 = split3(v)
    return jnp.concatenate([p1, p2, p3, p1, p1, p2], axis=0).astype(BF)


def right_parts(v):
    p1, p2, p3 = split3(v)
    return jnp.concatenate([p3, p2, p1, p1, p2, p1], axis=0).astype(BF)


def sum_parts(v):
    return v[0:8] + v[8:16] + v[16:24]


def gelu_and_slope(pre):
    x = pre.astype(F32)
    sq = x * x
    half = 0.5 * jnp.tanh(x * (sq * (C0 * K0) + C0)) + 0.5
    act = x * half
    slope = (act * (1.0 - half)) * (sq * (6.0 * C0 * K0) + 2.0 * C0) + half
    return act.astype(BF), slope


def rem3(t):
    return t - 3 * lax.div(t * 43, 128)


def rows_of(m, size):
    return pl.ds(pl.multiple_of(m * size, size), size)


def kernel(
    tok, cot, up, down, a4, b4,
    xout, gtok, gout, gp, xs, kept,
    w, sd, xb, ub, db, gst, pre0, pre1, acat, bcat, vcat, dcat, dlt, gb, ga, gacc, rbuf, gall,
    own_sem, fs_sem, fr_sem, kept_sem, gp_sem, io_sem, bo_sem, bs_sem, br_sem, rs_sem, rr_sem, as_sem, ar_sem,
    cred,
):
    data = lax.axis_index("data")
    local = lax.axis_index("local")
    x, c = lax.div(data, 2), lax.rem(data, 2)
    z, y = lax.div(local, 2), lax.rem(local, 2)
    me = data * 4 + local
    dx, dy, dz, dc = 1 - 2 * x, 1 - 2 * y, 1 - 2 * z, 1 - 2 * c
    par = lax.rem(x + y + z, 2)

    def quarter(i):
        hi, lo = lax.div(i, 2), lax.rem(i, 2)
        return 2 * (par + hi - 2 * par * hi) + (c + lo - 2 * c * lo)

    q_own, q_miss = quarter(0), quarter(2)

    def pick(dim, a0, a1, a2):
        return lax.div((1 - dim) * (2 - dim), 2) * a0 + dim * (2 - dim) * a1 + lax.div(dim * (dim - 1), 2) * a2

    def device(dim):
        return (local + pick(dim, 0, dy, 2 * dz), data + pick(dim, 2 * dx, 0, 0))

    neighbours = ((local, data + 2 * dx), (local + dy, data), (local + 2 * dz, data), (local, data + dc))
    partner = neighbours[3]

    def remote(src, dst, ssem, rsem, dev):
        return pltpu.make_async_remote_copy(
            src_ref=src, dst_ref=dst, send_sem=ssem, recv_sem=rsem, device_id=dev, device_id_type=pl.DeviceIdType.MESH
        )


    def own_load(g):
        s, l = lax.rem(g, 8), lax.div(g, 8)

        @pl.when(s < 4)
        def _():
            for n in range(4):
                pltpu.make_async_copy(
                    up.at[l, :, pl.ds(pl.multiple_of(s * 1024 + n * 256, 256), 256)],
                    w.at[s, me, pl.ds(n * 64, 64), :],
                    own_sem.at[s],
                ).start()

        @pl.when(s >= 4)
        def _():
            pltpu.make_async_copy(
                down.at[l, :, pl.ds(pl.multiple_of((s - 4) * 256, 256), 256)], w.at[s, me], own_sem.at[s]
            ).start()

    def colour(g):
        q = rem3(jnp.where(g == 1, 2, g) + c)
        turn = jnp.where(g == 1, 2, 1)
        return q, rem3(q + turn), rem3(q + 2 * turn)

    def delta(dim):
        return pick(dim, 8 * dx, dy, 2 * dz)

    def use_credit(g, dim):
        @pl.when(g >= 8)
        def _():
            pl.semaphore_wait(cred.at[dim, lax.rem(g, 8)], 1)

    def send_blocks(g, phase, dim, blocks, dev):
        s = lax.rem(g, 8)
        use_credit(g, dim)
        for b in blocks:
            remote(w.at[s, b], w.at[s, b], fs_sem.at[phase, s], fr_sem.at[phase, s], dev).start()

    def span(g, phase):
        s = lax.rem(g, 8)
        r = w.at[s, pl.ds(0, (1, 2, 4, 8)[phase])]
        return remote(r, r, fs_sem.at[phase, s], fr_sem.at[phase, s], partner)

    def ready(g):
        return jnp.logical_and(g >= 0, g < NG)

    def hop1(g):
        d1, _, _ = colour(g)
        s = lax.rem(g, 8)
        pltpu.make_async_copy(w.at[s, me], w.at[s, me], own_sem.at[s]).wait()
        send_blocks(g, 0, d1, (me,), device(d1))

    def hop2(g):
        d1, d2, _ = colour(g)
        span(g, 0).wait_recv()
        send_blocks(g, 1, d2, (me, me + delta(d1)), device(d2))

    def hop3(g):
        d1, d2, d3 = colour(g)
        e1, e2 = delta(d1), delta(d2)
        span(g, 1).wait_recv()
        send_blocks(g, 2, d3, (me, me + e1, me + e2, me + e1 + e2), device(d3))

    def hand_over(g):
        s = lax.rem(g, 8)
        span(g, 2).wait_recv()
        use_credit(g, 3)
        for h in range(2):
            r2 = w.at[s, pl.ds(8 * h + 4 * c, 4)]
            remote(r2, r2, fs_sem.at[3, s], fr_sem.at[3, s], partner).start()

    def event(j):
        for step, ahead in ((hand_over, 1), (hop2, 5), (hop3, 3)):

            @pl.when(j + ahead < NG)
            def _():
                with jax.named_scope("st"):
                    step(j + ahead)

    def refill(j):
        @pl.when(j + 7 < NG)
        def _():
            hop1(j + 7)

    def keep_copy(g):
        s, l = lax.rem(g, 8), lax.div(g, 8)
        return pltpu.make_async_copy(w.at[s, pl.ds(4 * q_own, 4)], kept.at[l, s], kept_sem.at[s])

    def arrive(g):
        span(g, 3).wait_recv()
        keep_copy(g).start()

    def release(g):
        s = lax.rem(g, 8)
        for phase in range(4):
            span(g, phase).wait_send()
        keep_copy(g).wait()
        for i in range(4):
            pl.semaphore_signal(cred.at[i, s], inc=1, device_id=neighbours[i], device_id_type=pl.DeviceIdType.MESH)

        @pl.when(g + 8 < NG)
        def _():
            own_load(g + 8)


    def whole(m, q):
        return w.at[pl.ds(4 * m, 4), pl.ds(4 * q, 4)]

    def part(ref, dim):
        return ref.at[:, :, pl.ds(*ROWS[dim]), :]

    def b_own(m, l):
        return pltpu.make_async_copy(kept.at[l, pl.ds(4 * m, 4)], whole(m, q_own), bo_sem.at[m])

    def b_send(m, l, i, q):
        src, dst = kept.at[l, pl.ds(4 * m, 4)], whole(m, q)
        if i < 3:
            src, dst = part(src, i), part(dst, i)
        return remote(src, dst, bs_sem.at[m, i], br_sem.at[m, i], neighbours[i])

    def b_forward(m):
        return remote(whole(m, q_miss), whole(m, q_miss), bs_sem.at[m, 4], br_sem.at[m, 4], partner)

    def gather(m, l):
        @pl.when(jnp.logical_or(l < L - 1, m == 0))
        def _():
            b_own(m, l).start()

        for i in range(4):
            for s in range(4):
                pl.semaphore_wait(cred.at[i, 4 * m + s], 1)
            b_send(m, l, i, q_own).start()

    def b_events(m, l, i):
        @pl.when(jnp.logical_and(i == 0, jnp.logical_or(l < L - 1, m == 0)))
        def _():
            b_own(m, l).wait()

        @pl.when(i == 1)
        def _():
            b_send(m, l, 3, quarter(1)).wait_recv()

        @pl.when(i == 2)
        def _():
            for d in range(3):
                b_send(m, l, d, q_miss).wait_recv()
            b_forward(m).start()

        @pl.when(i == 3)
        def _():
            b_forward(m).wait_recv()

    def b_release(m, l):
        b_forward(m).wait_send()
        for i in range(4):
            b_send(m, l, i, q_own).wait_send()

        @pl.when(l > 0)
        def _():
            for i in range(4):
                for s in range(4):
                    pl.semaphore_signal(
                        cred.at[i, 4 * m + s], inc=1, device_id=neighbours[i], device_id_type=pl.DeviceIdType.MESH
                    )


    def grad_send(l, i):
        return remote(
            gacc.at[l, :, pl.ds(i * GW, GW)], rbuf.at[me], rs_sem.at[l], rr_sem, (jnp.int32(i), l)
        )

    def grads_out(l):
        for i in range(4):
            mine = me == 4 * l + i

            @pl.when(jnp.logical_not(mine))
            def _():
                grad_send(l, i).start()

            @pl.when(mine)
            def _():
                rbuf[me] = gacc[l, :, i * GW : (i + 1) * GW]


    tok_in = pltpu.make_async_copy(tok, xb, io_sem.at[0])
    cot_in = pltpu.make_async_copy(cot, db, io_sem.at[1])

    def first_loads(g, _):
        own_load(g)
        return 0

    lax.fori_loop(0, 8, first_loads, 0)
    tok_in.start()
    at = jnp.int32
    for g in (0, 1, 2, 5, 7, 3, 6):
        with jax.named_scope("hop1"):
            hop1(at(g))
    for b in range(2):
        pltpu.make_async_copy(gst.at[b, pl.ds(0, MX)], gp.at[4 * L, pl.ds(b * MX, MX), :], gp_sem.at[b]).start()
    for l in range(L):
        acat[l] = right_parts(jnp.concatenate([a4[l], jnp.zeros((4, H), F32)], axis=0))
        bcat[l] = right_parts(jnp.concatenate([b4[l], jnp.zeros((4, F), F32)], axis=0))
    with jax.named_scope("tw"):
        tok_in.wait()
    for step, g in ((hop2, 0), (hop2, 1), (hop2, 2), (hop3, 0)):
        with jax.named_scope("st0"):
            step(at(g))

    def first_layer(t, lo, hi):
        for when, steps in FIRST_LAYER:
            if lo <= when < hi:

                @pl.when(t == when - lo)
                def _():
                    for kind, chunk in steps:
                        with jax.named_scope("st1"):
                            (hop1, hop2, hop3, hand_over)[kind](at(chunk))


    def inv_rms(rf):
        return lax.rsqrt(jnp.mean(rf * rf, axis=-1, keepdims=True) + NORM_EPS)

    def x_save(l):
        return pltpu.make_async_copy(xb, xs.at[l - 1], io_sem.at[0])

    def slope_out(b, lk, m):
        return pltpu.make_async_copy(gst.at[b, pl.ds(0, MX)], gp.at[lk, rows_of(m, MX), :], gp_sem.at[b])

    def gp_in(t):
        lk = 4 * (L - 1 - lax.div(t, 16)) + quarter(lax.div(lax.rem(t, 16), 4))
        b = rem3(t)
        return pltpu.make_async_copy(gp.at[lk, rows_of(lax.rem(t, 4), MU), :], gst.at[b], gp_sem.at[b])

    blocks = [(rb, cb) for cb in range(0, 1024, CB) for rb in range(0, MX, RB)]

    def activate(src, k, m, slot, part):
        for rb, cb in blocks[part * len(blocks) // 5 : (part + 1) * len(blocks) // 5]:
            act, slope = gelu_and_slope(src[rb : rb + RB, cb : cb + CB].astype(BF))
            r = pl.ds(pl.multiple_of(m * MX + rb, RB), RB)
            sd[r, pl.ds(pl.multiple_of(k * 1024 + cb, CB), CB)] = act
            gst[slot, rb : rb + RB, cb : cb + CB] = slope

    def up_tile(l, k, m, dst, kp, mp, src, slot):
        r = rows_of(m, MX)
        cols = pl.ds(pl.multiple_of(k * 1024, 1024), 1024)
        acc = None
        for kt in range(5):
            if kt < 4:
                rhs = w[k, 4 * kt : 4 * kt + 4]
                rhs = jnp.concatenate([rhs[:, n * 64 : (n + 1) * 64, :].reshape(256, 256) for n in range(4)], axis=1)
                term = nn(ub[r, kt * 256 : (kt + 1) * 256], rhs)
            else:
                term = tn(vcat[l, :, r], bcat[l, :, cols])
            acc = term if acc is None else acc + term
            activate(src, kp, mp, slot, kt)
        dst[...] = acc

    def forward_layer(l, _):
        @pl.when(l > 0)
        def _():
            x_save(l).start()

        def prep(m, _):
            r = rows_of(m, MU)
            rf = xb[r, :].astype(F32)
            u = (rf * inv_rms(rf)).astype(BF)
            ub[r, :] = u
            vcat[l, :, r] = left_parts(sum_parts(nt(acat[l, 0:32], u)))
            return 0

        with jax.named_scope("prep"):
            lax.fori_loop(0, T // MU, prep, 0)

        @pl.when(l == 0)
        def _():
            for step, g in ((hop2, 3), (hop3, 1), (hop1, 4), (hop2, 5), (hand_over, 0), (hop3, 2)):
                with jax.named_scope("st0"):
                    step(at(g))

        def slopes(t):
            slot = rem3(2 * l + t)
            old = jnp.maximum(t - 2, 0)
            lk = jnp.where(t == 1, 4 * L, 4 * l + lax.div(old, 4))
            lk = jnp.where(t == 0, jnp.where(l == 0, 4 * L, 4 * l - 1), lk)
            m = jnp.where(t == 0, 3, jnp.where(t == 1, 2, lax.rem(old, 4)))
            slope_out(jnp.where(slot == 0, 2, slot - 1), lk, m).start()
            slope_out(slot, 0, 0).wait()
            return slot

        def up_step(t, _):
            k, m = lax.div(t, 4), lax.rem(t, 4)
            g = 8 * l + k

            due = t == 1
            j = at(0)
            for i in (5, 9, 12, 15):
                due = jnp.logical_or(due, t == i)
                j = j + jnp.where(t >= i, 1, 0)

            @pl.when(m == 0)
            def _():
                @pl.when(k > 0)
                def _():
                    release(g - 1)

                with jax.named_scope("arr"):
                    arrive(g)

            @pl.when(l == 0)
            def _():
                with jax.named_scope("fl"):
                    first_layer(t, 0, 16)

            @pl.when(jnp.logical_and(l > 0, jnp.logical_or(due, m == 1)))
            def _():
                @pl.when(due)
                def _():
                    with jax.named_scope("ev"):
                        event(8 * l + j)

                @pl.when(m == 1)
                def _():
                    with jax.named_scope("rf"):
                        refill(g)

            tp = jnp.maximum(t - 1, 0)
            kp, mp = lax.div(tp, 4), lax.rem(tp, 4)
            slot = slopes(t)

            @pl.when(lax.rem(t, 2) == 0)
            def _():
                with jax.named_scope("up"):
                    up_tile(l, k, m, pre0, kp, mp, pre1, slot)

            @pl.when(lax.rem(t, 2) == 1)
            def _():
                with jax.named_scope("up"):
                    up_tile(l, k, m, pre1, kp, mp, pre0, slot)

            return 0

        lax.fori_loop(0, 16, up_step, 0)
        release(8 * l + 3)
        slot = slopes(at(16))
        for part in range(5):
            activate(pre1, 3, at(3), slot, part)

        @pl.when(l == L - 1)
        def _():
            cot_in.start()
            slope_out((2 * (L - 1) + 16) % 3, 4 * L - 1, at(3)).start()

        @pl.when(l > 0)
        def _():
            x_save(l).wait()

        def down_step(t, _):
            k, m = lax.div(t, 2), lax.rem(t, 2)
            g = 8 * l + 4 + k

            @pl.when(m == 0)
            def _():
                @pl.when(k > 0)
                def _():
                    release(g - 1)

                with jax.named_scope("arr"):
                    arrive(g)

                @pl.when(jnp.logical_and(l > 0, jnp.logical_or(k == 1, k == 2)))
                def _():
                    with jax.named_scope("ev"):
                        event(g)

            @pl.when(jnp.logical_and(l == L - 1, t == 5))
            def _():
                for b in range(3):
                    slope_out(b, 0, at(0)).wait()
                gp_in(at(0)).start()
                gp_in(at(1)).start()

            @pl.when(l == 0)
            def _():
                with jax.named_scope("fl"):
                    first_layer(t, 16, 24)

            @pl.when(jnp.logical_and(l > 0, m == 1))
            def _():
                with jax.named_scope("rf"):
                    refill(g)

                @pl.when(k == 3)
                def _():
                    with jax.named_scope("ev"):
                        event(g)

            r = rows_of(m, MD)
            cols = pl.ds(pl.multiple_of(k * 256, 256), 256)
            with jax.named_scope("dn"):
                step = nn(sd[r, :], w[4 + k].reshape(F, 256))
                xb[r, cols] = (xb[r, cols].astype(F32) + step).astype(BF)
            return 0

        lax.fori_loop(0, 8, down_step, 0)
        release(8 * l + 7)
        return 0

    lax.fori_loop(0, L, forward_layer, 0)


    x_final = pltpu.make_async_copy(xb, xout, io_sem.at[0])
    x_final.start()
    with jax.named_scope("gat"):
        gather(1, L - 1)
    cot_in.wait()


    def x_load(l, start):
        @pl.when(l > 0)
        def _():
            cp = pltpu.make_async_copy(xs.at[l - 1], xb, io_sem.at[0])
            cp.start() if start else cp.wait()

        @pl.when(l == 0)
        def _():
            cp = pltpu.make_async_copy(tok, xb, io_sem.at[0])
            cp.start() if start else cp.wait()

    def backward_layer(rl, _):
        l = L - 1 - rl
        dlt[...] = jnp.zeros_like(dlt)
        gb[...] = jnp.zeros_like(gb)
        ga[...] = jnp.zeros_like(ga)

        def down_step(i, _):
            @pl.when(i == 1)
            def _():
                with jax.named_scope("gat"):
                    gather(0, l)

            @pl.when(i == 2)
            def _():
                @pl.when(l == L - 1)
                def _():
                    x_final.wait()

                x_load(l, True)

            with jax.named_scope("bev"):
                b_events(1, l, i)
            q = quarter(i)
            cols = pl.ds(pl.multiple_of(q * 1024, 1024), 1024)

            def tile(m, _):
                t = rl * 16 + i * 4 + m

                @pl.when(t + 2 < 16 * L)
                def _():
                    gp_in(t + 2).start()

                gp_in(t).wait()
                r = rows_of(m, MU)
                acc = None
                for k in range(4):
                    rhs = w[4 + k, pl.ds(4 * q, 4)].reshape(1024, 256)
                    term = nt(db[r, k * 256 : (k + 1) * 256], rhs)
                    acc = term if acc is None else acc + term
                d = (acc.astype(BF).astype(F32) * gst[rem3(t)]).astype(BF)
                sd[r, cols] = d
                dlt[:, r] += nt(bcat[l, 0:32, cols], d)
                gb[:, cols] += nn(vcat[l, 0:32, r], d)
                return 0

            with jax.named_scope("p1"):
                lax.fori_loop(0, T // MU, tile, 0)
            return 0

        lax.fori_loop(0, 4, down_step, 0)
        with jax.named_scope("brel"):
            b_release(1, l)
        dcat[...] = left_parts(sum_parts(dlt[...]))
        gb8 = sum_parts(gb[...])
        gacc[l, :, 0:2048] = gb8[:, 0:2048] + pltpu.roll(gb8[:, 2048:4096], 4, 0)

        def up_step(i, _):
            @pl.when(jnp.logical_and(i == 1, l > 0))
            def _():
                with jax.named_scope("gat"):
                    gather(1, l - 1)

            with jax.named_scope("bev"):
                b_events(0, l, i)
            q = quarter(i)
            cols = pl.ds(pl.multiple_of(q * 256, 256), 256)

            def tile(m, _):
                r = rows_of(m, MD)
                acc = None
                for k in range(4):
                    for n in range(4):
                        rhs = w[k, pl.ds(4 * q, 4), n * 64 : (n + 1) * 64, :].reshape(256, 256)
                        j = 4 * k + n
                        term = nt(sd[r, j * 256 : (j + 1) * 256], rhs)
                        acc = term if acc is None else acc + term
                side = tn(dcat[:, r], acat[l, :, cols]).astype(BF)
                ub[r, cols] = acc.astype(BF) + side
                return 0

            with jax.named_scope("p2"):
                lax.fori_loop(0, T // MD, tile, 0)
            return 0

        lax.fori_loop(0, 4, up_step, 0)
        with jax.named_scope("brel"):
            b_release(0, l)
        x_load(l, False)

        def finish(m, _):
            r = rows_of(m, MU)
            rf = xb[r, :].astype(F32)
            inv = inv_rms(rf)
            dn = ub[r, :].astype(F32)
            dot = jnp.mean(rf * dn, axis=-1, keepdims=True)
            db[r, :] = (db[r, :].astype(F32) + inv * dn - rf * ((inv * inv * inv) * dot)).astype(BF)
            u = (rf * inv).astype(BF)
            ga[...] += nn(dcat[0:32, r], u)
            return 0

        with jax.named_scope("fin"):
            lax.fori_loop(0, T // MU, finish, 0)
        ga8 = sum_parts(ga[...])
        gacc[l, :, 2048:2560] = ga8[:, 0:512] + pltpu.roll(ga8[:, 512:1024], 4, 0)
        with jax.named_scope("gout"):
            grads_out(l)
        return 0

    lax.fori_loop(0, L, backward_layer, 0)


    g_final = pltpu.make_async_copy(db, gtok, io_sem.at[1])
    g_final.start()
    others = rbuf.at[pl.ds(0, 15)]
    with jax.named_scope("redw"):
        remote(others, others, rr_sem, rr_sem, partner).wait_recv()
    total = rbuf[0]
    for i in range(1, 16):
        total = total + rbuf[i]
    gall[me] = total

    def share(o, _):
        @pl.when(o != me)
        def _():
            remote(gall.at[me], gall.at[me], as_sem, ar_sem, (lax.rem(o, 4), lax.div(o, 4))).start()

        return 0

    lax.fori_loop(0, 16, share, 0)
    others = gall.at[pl.ds(0, 15)]
    with jax.named_scope("allw"):
        remote(others, others, as_sem, ar_sem, partner).wait_send()
        remote(others, others, as_sem, ar_sem, partner).wait_recv()
    for l in range(L):
        for i in range(4):

            @pl.when(me != 4 * l + i)
            def _():
                grad_send(jnp.int32(l), i).wait_send()

    shares = pltpu.make_async_copy(gall, gout, io_sem.at[0])
    shares.start()
    g_final.wait()
    shares.wait()


def solution(mesh):
    tok_spec = P(GROUP, None)
    weight_spec = P(None, GROUP, None)

    def device_step(tokens, cotangent, up, down, lora_a, lora_b):
        hbm = pl.BlockSpec(memory_space=pltpu.HBM)
        vmem = pl.BlockSpec(memory_space=pltpu.VMEM)
        shape = jax.ShapeDtypeStruct
        dma, regular = pltpu.SemaphoreType.DMA, pltpu.SemaphoreType.REGULAR
        outs = pl.pallas_call(
            kernel,
            name="stack",
            out_shape=[
                shape((T, H), BF),
                shape((T, H), BF),
                shape((16, 8, GW), F32),
                shape((4 * L + 1, T, 1024), F32),
                shape((L - 1, T, H), BF),
                shape((L, 8, 4, 256, 256), BF),
            ],
            in_specs=[hbm, hbm, hbm, hbm, vmem, vmem],
            out_specs=[hbm] * 6,
            scratch_shapes=[
                pltpu.VMEM((8, 16, 256, 256), BF),
                pltpu.VMEM((T, F), BF),
                pltpu.VMEM((T, H), BF),
                pltpu.VMEM((T, H), BF),
                pltpu.VMEM((T, H), BF),
                pltpu.VMEM((3, MU, 1024), F32),
                pltpu.VMEM((MX, 1024), F32),
                pltpu.VMEM((MX, 1024), F32),
                pltpu.VMEM((L, 48, H), BF),
                pltpu.VMEM((L, 48, F), BF),
                pltpu.VMEM((L, 48, T), BF),
                pltpu.VMEM((48, T), BF),
                pltpu.VMEM((32, T), F32),
                pltpu.VMEM((32, F), F32),
                pltpu.VMEM((32, H), F32),
                pltpu.VMEM((L, 8, 4 * GW), F32),
                pltpu.VMEM((16, 8, GW), F32),
                pltpu.VMEM((16, 8, GW), F32),
                dma((8,)),
                dma((4, 8)),
                dma((4, 8)),
                dma((8,)),
                dma((3,)),
                dma((2,)),
                dma((2,)),
                dma((2, 5)),
                dma((2, 5)),
                dma((L,)),
                dma,
                dma,
                dma,
                regular((4, 8)),
            ],
            compiler_params=pltpu.CompilerParams(
                vmem_limit_bytes=67000000,
                has_side_effects=True,
            ),
        )(tokens, cotangent, up, down, lora_a.transpose(0, 2, 1), lora_b)
        x_out, g_tok, shares = outs[:3]
        grads = shares.reshape(L, 4, 2, 4, GW).transpose(0, 2, 3, 1, 4).reshape(L, 2, 4, 4 * GW)
        grad_b = grads[..., 0:2048].transpose(0, 2, 1, 3).reshape(L, 4, F)
        grad_a = grads[..., 2048:2560].transpose(0, 1, 3, 2).reshape(L, H, 4)
        return x_out, g_tok, grad_a, grad_b

    return jax.shard_map(
        device_step,
        mesh=mesh,
        in_specs=(tok_spec, tok_spec, weight_spec, weight_spec, P(), P()),
        out_specs=(tok_spec, tok_spec, P(), P()),
        check_vma=False,
    )
```

```python
import jax
import jax.numpy as jnp
from jax import lax
from jax.experimental import pallas as pl
from jax.experimental.pallas import tpu as pltpu
from jax.sharding import PartitionSpec as P

GROUP = ("data", "local")
NORM_EPS = 1e-6
BF = jnp.bfloat16
F32 = jnp.float32
C0 = 0.7978845608028654
K0 = 0.044715

T = 2048
H = 1024
F = 4096
L = 4
NG = 8 * L
MU = 512
MD = 1024
MX = 512
RB, CB = 16, 256
ROWS = (((0, 96), (96, 80), (176, 80)), ((0, 80), (80, 96), (176, 80)))
FIRST_LAYER = (
    (0, ((1, 4), (2, 3))),
    (2, ((3, 1), (1, 6))),
    (5, ((2, 4),)),
    (6, ((0, 8), (3, 2))),
    (8, ((2, 5), (3, 3), (1, 7))),
    (9, ((1, 8),)),
    (12, ((3, 4), (2, 6))),
    (13, ((0, 10), (0, 9))),
    (14, ((2, 7),)),
    (16, ((1, 9), (3, 5))),
    (17, ((0, 11), (2, 8))),
    (18, ((3, 6), (1, 10))),
    (19, ((2, 9),)),
    (20, ((3, 7), (0, 12), (1, 11))),
    (23, ((0, 13), (1, 12), (0, 14), (2, 10), (3, 8))),
)
GW = 640


def nn(a, b):
    return lax.dot_general(a, b, (((1,), (0,)), ((), ())), preferred_element_type=F32)


def nt(a, b):
    return lax.dot_general(a, b, (((1,), (1,)), ((), ())), preferred_element_type=F32)


def tn(a, b):
    return lax.dot_general(a, b, (((0,), (0,)), ((), ())), preferred_element_type=F32)


def split3(v):
    p1 = v.astype(BF).astype(F32)
    rest = v - p1
    p2 = rest.astype(BF).astype(F32)
    return p1, p2, (rest - p2).astype(BF).astype(F32)


def left_parts(v):
    p1, p2, p3 = split3(v)
    return jnp.concatenate([p1, p2, p3, p1, p1, p2], axis=0).astype(BF)


def right_parts(v):
    p1, p2, p3 = split3(v)
    return jnp.concatenate([p3, p2, p1, p1, p2, p1], axis=0).astype(BF)


def sum_parts(v):
    return v[0:8] + v[8:16] + v[16:24]


def gelu_and_slope(pre):
    x = pre.astype(F32)
    sq = x * x
    half = 0.5 * jnp.tanh(x * (sq * (C0 * K0) + C0)) + 0.5
    act = x * half
    slope = (act * (1.0 - half)) * (sq * (6.0 * C0 * K0) + 2.0 * C0) + half
    return act.astype(BF), slope


def rem3(t):
    return t - 3 * lax.div(t * 43, 128)


def rows_of(m, size):
    return pl.ds(pl.multiple_of(m * size, size), size)


def kernel(
    tok, cot, up, down, a4, b4,
    xout, gtok, gout, gp, xs, kept,
    w, sd, xb, ub, db, gst, pre0, pre1, acat, bcat, vcat, dcat, dlt, gb, ga, gacc, rbuf, gall,
    own_sem, fs_sem, fr_sem, kept_sem, gp_sem, io_sem, bo_sem, bs_sem, br_sem, rs_sem, rr_sem, as_sem, ar_sem,
    cred,
):
    data = lax.axis_index("data")
    local = lax.axis_index("local")
    x, c = lax.div(data, 2), lax.rem(data, 2)
    z, y = lax.div(local, 2), lax.rem(local, 2)
    me = data * 4 + local
    dx, dy, dz, dc = 1 - 2 * x, 1 - 2 * y, 1 - 2 * z, 1 - 2 * c
    par = lax.rem(x + y + z, 2)

    def quarter(i):
        hi, lo = lax.div(i, 2), lax.rem(i, 2)
        return 2 * (par + hi - 2 * par * hi) + (c + lo - 2 * c * lo)

    q_own, q_miss = quarter(0), quarter(2)

    def pick(dim, a0, a1, a2):
        return lax.div((1 - dim) * (2 - dim), 2) * a0 + dim * (2 - dim) * a1 + lax.div(dim * (dim - 1), 2) * a2

    def device(dim):
        return (local + pick(dim, 0, dy, 2 * dz), data + pick(dim, 2 * dx, 0, 0))

    neighbours = ((local, data + 2 * dx), (local + dy, data), (local + 2 * dz, data), (local, data + dc))
    partner = neighbours[3]

    def remote(src, dst, ssem, rsem, dev):
        return pltpu.make_async_remote_copy(
            src_ref=src, dst_ref=dst, send_sem=ssem, recv_sem=rsem, device_id=dev, device_id_type=pl.DeviceIdType.MESH
        )


    def own_load(g):
        s, l = lax.rem(g, 8), lax.div(g, 8)

        @pl.when(s < 4)
        def _():
            for n in range(4):
                pltpu.make_async_copy(
                    up.at[l, :, pl.ds(pl.multiple_of(s * 1024 + n * 256, 256), 256)],
                    w.at[s, me, pl.ds(n * 64, 64), :],
                    own_sem.at[s],
                ).start()

        @pl.when(s >= 4)
        def _():
            pltpu.make_async_copy(
                down.at[l, :, pl.ds(pl.multiple_of((s - 4) * 256, 256), 256)], w.at[s, me], own_sem.at[s]
            ).start()

    def colour(g):
        q = rem3(jnp.where(g == 1, 2, g) + c)
        turn = jnp.where(g == 1, 2, 1)
        return q, rem3(q + turn), rem3(q + 2 * turn)

    def delta(dim):
        return pick(dim, 8 * dx, dy, 2 * dz)

    def use_credit(g, dim):
        @pl.when(g >= 8)
        def _():
            pl.semaphore_wait(cred.at[dim, lax.rem(g, 8)], 1)

    def send_blocks(g, phase, dim, blocks, dev):
        s = lax.rem(g, 8)
        use_credit(g, dim)
        for b in blocks:
            remote(w.at[s, b], w.at[s, b], fs_sem.at[phase, s], fr_sem.at[phase, s], dev).start()

    def span(g, phase):
        s = lax.rem(g, 8)
        r = w.at[s, pl.ds(0, (1, 2, 4, 8)[phase])]
        return remote(r, r, fs_sem.at[phase, s], fr_sem.at[phase, s], partner)

    def ready(g):
        return jnp.logical_and(g >= 0, g < NG)

    def hop1(g):
        d1, _, _ = colour(g)
        s = lax.rem(g, 8)
        pltpu.make_async_copy(w.at[s, me], w.at[s, me], own_sem.at[s]).wait()
        send_blocks(g, 0, d1, (me,), device(d1))

    def hop2(g):
        d1, d2, _ = colour(g)
        span(g, 0).wait_recv()
        send_blocks(g, 1, d2, (me, me + delta(d1)), device(d2))

    def hop3(g):
        d1, d2, d3 = colour(g)
        e1, e2 = delta(d1), delta(d2)
        span(g, 1).wait_recv()
        send_blocks(g, 2, d3, (me, me + e1, me + e2, me + e1 + e2), device(d3))

    def hand_over(g):
        s = lax.rem(g, 8)
        span(g, 2).wait_recv()
        use_credit(g, 3)
        for h in range(2):
            r2 = w.at[s, pl.ds(8 * h + 4 * c, 4)]
            remote(r2, r2, fs_sem.at[3, s], fr_sem.at[3, s], partner).start()

    def event(j):
        for step, ahead in ((hand_over, 1), (hop2, 5), (hop3, 3)):

            @pl.when(j + ahead < NG)
            def _():
                step(j + ahead)

    def refill(j):
        @pl.when(j + 7 < NG)
        def _():
            hop1(j + 7)

    def keep_copy(g):
        s, l = lax.rem(g, 8), lax.div(g, 8)
        return pltpu.make_async_copy(w.at[s, pl.ds(4 * q_own, 4)], kept.at[l, s], kept_sem.at[s])

    def arrive(g):
        span(g, 3).wait_recv()
        keep_copy(g).start()

    def release(g):
        s = lax.rem(g, 8)
        for phase in range(4):
            span(g, phase).wait_send()
        keep_copy(g).wait()
        for i in range(4):
            pl.semaphore_signal(cred.at[i, s], inc=1, device_id=neighbours[i], device_id_type=pl.DeviceIdType.MESH)

        @pl.when(g + 8 < NG)
        def _():
            own_load(g + 8)


    def whole(m, q):
        return w.at[pl.ds(4 * m, 4), pl.ds(4 * q, 4)]

    def part(ref, rows):
        return ref.at[:, :, pl.ds(*rows), :]

    def b_own(m, l):
        return pltpu.make_async_copy(kept.at[l, pl.ds(4 * m, 4)], whole(m, q_own), bo_sem.at[m])

    def b_send(m, l, i, q, core=None):
        src, dst = kept.at[l, pl.ds(4 * m, 4)], whole(m, q)
        if i < 3:
            src, dst = part(src, ROWS[core][i]), part(dst, ROWS[core][i])
        return remote(src, dst, bs_sem.at[m, i], br_sem.at[m, i], neighbours[i])

    def by_core(fn):
        for core in range(2):

            @pl.when(c == core)
            def _():
                fn(core)

    def b_forward(m):
        return remote(whole(m, q_miss), whole(m, q_miss), bs_sem.at[m, 4], br_sem.at[m, 4], partner)

    def gather(m, l):
        @pl.when(jnp.logical_or(l < L - 1, m == 0))
        def _():
            b_own(m, l).start()

        for i in range(4):
            for s in range(4):
                pl.semaphore_wait(cred.at[i, 4 * m + s], 1)
            if i == 3:
                b_send(m, l, i, q_own).start()
            else:
                by_core(lambda core: b_send(m, l, i, q_own, core).start())

    def b_events(m, l, i):
        @pl.when(jnp.logical_and(i == 0, jnp.logical_or(l < L - 1, m == 0)))
        def _():
            b_own(m, l).wait()

        @pl.when(i == 1)
        def _():
            b_send(m, l, 3, quarter(1)).wait_recv()

        @pl.when(i == 2)
        def _():
            by_core(lambda core: [b_send(m, l, d, q_miss, core).wait_recv() for d in range(3)])
            b_forward(m).start()

        @pl.when(i == 3)
        def _():
            b_forward(m).wait_recv()

    def b_release(m, l):
        b_forward(m).wait_send()
        b_send(m, l, 3, q_own).wait_send()
        by_core(lambda core: [b_send(m, l, d, q_own, core).wait_send() for d in range(3)])

        @pl.when(l > 0)
        def _():
            for i in range(4):
                for s in range(4):
                    pl.semaphore_signal(
                        cred.at[i, 4 * m + s], inc=1, device_id=neighbours[i], device_id_type=pl.DeviceIdType.MESH
                    )


    def grad_send(l, i):
        return remote(
            gacc.at[l, :, pl.ds(i * GW, GW)], rbuf.at[me], rs_sem.at[l], rr_sem, (jnp.int32(i), l)
        )

    def grads_out(l):
        for i in range(4):
            mine = me == 4 * l + i

            @pl.when(jnp.logical_not(mine))
            def _():
                grad_send(l, i).start()

            @pl.when(mine)
            def _():
                rbuf[me] = gacc[l, :, i * GW : (i + 1) * GW]


    tok_in = pltpu.make_async_copy(tok, xb, io_sem.at[0])
    cot_in = pltpu.make_async_copy(cot, db, io_sem.at[1])

    def first_loads(g, _):
        own_load(g)
        return 0

    lax.fori_loop(0, 8, first_loads, 0)
    tok_in.start()
    at = jnp.int32
    for g in (0, 1, 2, 5, 7, 3, 6):
        hop1(at(g))
    for b in range(2):
        pltpu.make_async_copy(gst.at[b, pl.ds(0, MX)], gp.at[4 * L, pl.ds(b * MX, MX), :], gp_sem.at[b]).start()
    for l in range(L):
        acat[l] = right_parts(jnp.concatenate([a4[l], jnp.zeros((4, H), F32)], axis=0))
        bcat[l] = right_parts(jnp.concatenate([b4[l], jnp.zeros((4, F), F32)], axis=0))
    tok_in.wait()
    for step, g in ((hop2, 0), (hop2, 1), (hop2, 2), (hop3, 0)):
        step(at(g))

    def first_layer(t, lo, hi):
        for when, steps in FIRST_LAYER:
            if lo <= when < hi:

                @pl.when(t == when - lo)
                def _():
                    for kind, chunk in steps:
                        (hop1, hop2, hop3, hand_over)[kind](at(chunk))


    def inv_rms(rf):
        return lax.rsqrt(jnp.mean(rf * rf, axis=-1, keepdims=True) + NORM_EPS)

    def x_save(l):
        return pltpu.make_async_copy(xb, xs.at[l - 1], io_sem.at[0])

    def slope_out(b, lk, m):
        return pltpu.make_async_copy(gst.at[b, pl.ds(0, MX)], gp.at[lk, rows_of(m, MX), :], gp_sem.at[b])

    def gp_in(t):
        lk = 4 * (L - 1 - lax.div(t, 16)) + quarter(lax.div(lax.rem(t, 16), 4))
        b = rem3(t)
        return pltpu.make_async_copy(gp.at[lk, rows_of(lax.rem(t, 4), MU), :], gst.at[b], gp_sem.at[b])

    blocks = [(rb, cb) for cb in range(0, 1024, CB) for rb in range(0, MX, RB)]

    def activate(src, k, m, slot, part):
        for rb, cb in blocks[part * len(blocks) // 5 : (part + 1) * len(blocks) // 5]:
            act, slope = gelu_and_slope(src[rb : rb + RB, cb : cb + CB].astype(BF))
            r = pl.ds(pl.multiple_of(m * MX + rb, RB), RB)
            sd[r, pl.ds(pl.multiple_of(k * 1024 + cb, CB), CB)] = act
            gst[slot, rb : rb + RB, cb : cb + CB] = slope

    def up_tile(l, k, m, dst, kp, mp, src, slot):
        r = rows_of(m, MX)
        cols = pl.ds(pl.multiple_of(k * 1024, 1024), 1024)
        acc = None
        for kt in range(5):
            if kt < 4:
                rhs = w[k, 4 * kt : 4 * kt + 4]
                rhs = jnp.concatenate([rhs[:, n * 64 : (n + 1) * 64, :].reshape(256, 256) for n in range(4)], axis=1)
                term = nn(ub[r, kt * 256 : (kt + 1) * 256], rhs)
            else:
                term = tn(vcat[l, :, r], bcat[l, :, cols])
            acc = term if acc is None else acc + term
            activate(src, kp, mp, slot, kt)
        dst[...] = acc

    def forward_layer(l, _):
        @pl.when(l > 0)
        def _():
            x_save(l).start()

        def prep(m, _):
            r = rows_of(m, MU)
            rf = xb[r, :].astype(F32)
            u = (rf * inv_rms(rf)).astype(BF)
            ub[r, :] = u
            vcat[l, :, r] = left_parts(sum_parts(nt(acat[l, 0:32], u)))
            return 0

        lax.fori_loop(0, T // MU, prep, 0)

        @pl.when(l == 0)
        def _():
            for step, g in ((hop2, 3), (hop3, 1), (hop1, 4), (hop2, 5), (hand_over, 0), (hop3, 2)):
                step(at(g))

        def slopes(t):
            slot = rem3(2 * l + t)
            old = jnp.maximum(t - 2, 0)
            lk = jnp.where(t == 1, 4 * L, 4 * l + lax.div(old, 4))
            lk = jnp.where(t == 0, jnp.where(l == 0, 4 * L, 4 * l - 1), lk)
            m = jnp.where(t == 0, 3, jnp.where(t == 1, 2, lax.rem(old, 4)))
            slope_out(jnp.where(slot == 0, 2, slot - 1), lk, m).start()
            slope_out(slot, 0, 0).wait()
            return slot

        def up_step(t, _):
            k, m = lax.div(t, 4), lax.rem(t, 4)
            g = 8 * l + k

            due = t == 1
            j = at(0)
            for i in (5, 9, 12, 15):
                due = jnp.logical_or(due, t == i)
                j = j + jnp.where(t >= i, 1, 0)

            @pl.when(m == 0)
            def _():
                @pl.when(k > 0)
                def _():
                    release(g - 1)

                arrive(g)

            @pl.when(l == 0)
            def _():
                first_layer(t, 0, 16)

            @pl.when(jnp.logical_and(l > 0, jnp.logical_or(due, m == 1)))
            def _():
                @pl.when(due)
                def _():
                    event(8 * l + j)

                @pl.when(m == 1)
                def _():
                    refill(g)

            tp = jnp.maximum(t - 1, 0)
            kp, mp = lax.div(tp, 4), lax.rem(tp, 4)
            slot = slopes(t)

            @pl.when(lax.rem(t, 2) == 0)
            def _():
                up_tile(l, k, m, pre0, kp, mp, pre1, slot)

            @pl.when(lax.rem(t, 2) == 1)
            def _():
                up_tile(l, k, m, pre1, kp, mp, pre0, slot)

            return 0

        lax.fori_loop(0, 16, up_step, 0)
        release(8 * l + 3)
        slot = slopes(at(16))
        for part in range(5):
            activate(pre1, 3, at(3), slot, part)

        @pl.when(l == L - 1)
        def _():
            cot_in.start()
            slope_out((2 * (L - 1) + 16) % 3, 4 * L - 1, at(3)).start()

        @pl.when(l > 0)
        def _():
            x_save(l).wait()

        def down_step(t, _):
            k, m = lax.div(t, 2), lax.rem(t, 2)
            g = 8 * l + 4 + k

            @pl.when(m == 0)
            def _():
                @pl.when(k > 0)
                def _():
                    release(g - 1)

                arrive(g)

                @pl.when(jnp.logical_and(l > 0, jnp.logical_or(k == 1, k == 2)))
                def _():
                    event(g)

            @pl.when(jnp.logical_and(l == L - 1, t == 5))
            def _():
                for b in range(3):
                    slope_out(b, 0, at(0)).wait()
                gp_in(at(0)).start()
                gp_in(at(1)).start()

            @pl.when(l == 0)
            def _():
                first_layer(t, 16, 24)

            @pl.when(jnp.logical_and(l > 0, m == 1))
            def _():
                refill(g)

                @pl.when(k == 3)
                def _():
                    event(g)

            r = rows_of(m, MD)
            cols = pl.ds(pl.multiple_of(k * 256, 256), 256)
            step = nn(sd[r, :], w[4 + k].reshape(F, 256))
            xb[r, cols] = (xb[r, cols].astype(F32) + step).astype(BF)
            return 0

        lax.fori_loop(0, 8, down_step, 0)
        release(8 * l + 7)
        return 0

    lax.fori_loop(0, L, forward_layer, 0)


    x_final = pltpu.make_async_copy(xb, xout, io_sem.at[0])
    x_final.start()
    gather(1, L - 1)
    cot_in.wait()


    def x_load(l, start):
        @pl.when(l > 0)
        def _():
            cp = pltpu.make_async_copy(xs.at[l - 1], xb, io_sem.at[0])
            cp.start() if start else cp.wait()

        @pl.when(l == 0)
        def _():
            cp = pltpu.make_async_copy(tok, xb, io_sem.at[0])
            cp.start() if start else cp.wait()

    def backward_layer(rl, _):
        l = L - 1 - rl
        dlt[...] = jnp.zeros_like(dlt)
        gb[...] = jnp.zeros_like(gb)
        ga[...] = jnp.zeros_like(ga)

        def down_step(i, _):
            @pl.when(i == 1)
            def _():
                gather(0, l)

            @pl.when(i == 2)
            def _():
                @pl.when(l == L - 1)
                def _():
                    x_final.wait()

                x_load(l, True)

            b_events(1, l, i)
            q = quarter(i)
            cols = pl.ds(pl.multiple_of(q * 1024, 1024), 1024)

            def tile(m, _):
                t = rl * 16 + i * 4 + m

                @pl.when(t + 2 < 16 * L)
                def _():
                    gp_in(t + 2).start()

                gp_in(t).wait()
                r = rows_of(m, MU)
                acc = None
                for k in range(4):
                    rhs = w[4 + k, pl.ds(4 * q, 4)].reshape(1024, 256)
                    term = nt(db[r, k * 256 : (k + 1) * 256], rhs)
                    acc = term if acc is None else acc + term
                d = (acc.astype(BF).astype(F32) * gst[rem3(t)]).astype(BF)
                sd[r, cols] = d
                dlt[:, r] += nt(bcat[l, 0:32, cols], d)
                gb[:, cols] += nn(vcat[l, 0:32, r], d)
                return 0

            lax.fori_loop(0, T // MU, tile, 0)
            return 0

        lax.fori_loop(0, 4, down_step, 0)
        b_release(1, l)
        dcat[...] = left_parts(sum_parts(dlt[...]))
        gb8 = sum_parts(gb[...])
        gacc[l, :, 0:2048] = gb8[:, 0:2048] + pltpu.roll(gb8[:, 2048:4096], 4, 0)

        def up_step(i, _):
            @pl.when(jnp.logical_and(i == 1, l > 0))
            def _():
                gather(1, l - 1)

            b_events(0, l, i)
            q = quarter(i)
            cols = pl.ds(pl.multiple_of(q * 256, 256), 256)

            def tile(m, _):
                r = rows_of(m, MD)
                acc = None
                for k in range(4):
                    for n in range(4):
                        rhs = w[k, pl.ds(4 * q, 4), n * 64 : (n + 1) * 64, :].reshape(256, 256)
                        j = 4 * k + n
                        term = nt(sd[r, j * 256 : (j + 1) * 256], rhs)
                        acc = term if acc is None else acc + term
                side = tn(dcat[:, r], acat[l, :, cols]).astype(BF)
                ub[r, cols] = acc.astype(BF) + side
                return 0

            lax.fori_loop(0, T // MD, tile, 0)
            return 0

        lax.fori_loop(0, 4, up_step, 0)
        b_release(0, l)
        x_load(l, False)

        def finish(m, _):
            r = rows_of(m, MU)
            rf = xb[r, :].astype(F32)
            inv = inv_rms(rf)
            dn = ub[r, :].astype(F32)
            dot = jnp.mean(rf * dn, axis=-1, keepdims=True)
            db[r, :] = (db[r, :].astype(F32) + inv * dn - rf * ((inv * inv * inv) * dot)).astype(BF)
            u = (rf * inv).astype(BF)
            ga[...] += nn(dcat[0:32, r], u)
            return 0

        lax.fori_loop(0, T // MU, finish, 0)
        ga8 = sum_parts(ga[...])
        gacc[l, :, 2048:2560] = ga8[:, 0:512] + pltpu.roll(ga8[:, 512:1024], 4, 0)
        grads_out(l)
        return 0

    lax.fori_loop(0, L, backward_layer, 0)


    g_final = pltpu.make_async_copy(db, gtok, io_sem.at[1])
    g_final.start()
    others = rbuf.at[pl.ds(0, 15)]
    remote(others, others, rr_sem, rr_sem, partner).wait_recv()
    total = rbuf[0]
    for i in range(1, 16):
        total = total + rbuf[i]
    gall[me] = total

    def share(o, _):
        @pl.when(o != me)
        def _():
            remote(gall.at[me], gall.at[me], as_sem, ar_sem, (lax.rem(o, 4), lax.div(o, 4))).start()

        return 0

    lax.fori_loop(0, 16, share, 0)
    others = gall.at[pl.ds(0, 15)]
    remote(others, others, as_sem, ar_sem, partner).wait_send()
    remote(others, others, as_sem, ar_sem, partner).wait_recv()
    for l in range(L):
        for i in range(4):

            @pl.when(me != 4 * l + i)
            def _():
                grad_send(jnp.int32(l), i).wait_send()

    shares = pltpu.make_async_copy(gall, gout, io_sem.at[0])
    shares.start()
    g_final.wait()
    shares.wait()


def solution(mesh):
    tok_spec = P(GROUP, None)
    weight_spec = P(None, GROUP, None)

    def device_step(tokens, cotangent, up, down, lora_a, lora_b):
        hbm = pl.BlockSpec(memory_space=pltpu.HBM)
        vmem = pl.BlockSpec(memory_space=pltpu.VMEM)
        shape = jax.ShapeDtypeStruct
        dma, regular = pltpu.SemaphoreType.DMA, pltpu.SemaphoreType.REGULAR
        outs = pl.pallas_call(
            kernel,
            name="stack",
            out_shape=[
                shape((T, H), BF),
                shape((T, H), BF),
                shape((16, 8, GW), F32),
                shape((4 * L + 1, T, 1024), F32),
                shape((L - 1, T, H), BF),
                shape((L, 8, 4, 256, 256), BF),
            ],
            in_specs=[hbm, hbm, hbm, hbm, vmem, vmem],
            out_specs=[hbm] * 6,
            scratch_shapes=[
                pltpu.VMEM((8, 16, 256, 256), BF),
                pltpu.VMEM((T, F), BF),
                pltpu.VMEM((T, H), BF),
                pltpu.VMEM((T, H), BF),
                pltpu.VMEM((T, H), BF),
                pltpu.VMEM((3, MU, 1024), F32),
                pltpu.VMEM((MX, 1024), F32),
                pltpu.VMEM((MX, 1024), F32),
                pltpu.VMEM((L, 48, H), BF),
                pltpu.VMEM((L, 48, F), BF),
                pltpu.VMEM((L, 48, T), BF),
                pltpu.VMEM((48, T), BF),
                pltpu.VMEM((32, T), F32),
                pltpu.VMEM((32, F), F32),
                pltpu.VMEM((32, H), F32),
                pltpu.VMEM((L, 8, 4 * GW), F32),
                pltpu.VMEM((16, 8, GW), F32),
                pltpu.VMEM((16, 8, GW), F32),
                dma((8,)),
                dma((4, 8)),
                dma((4, 8)),
                dma((8,)),
                dma((3,)),
                dma((2,)),
                dma((2,)),
                dma((2, 5)),
                dma((2, 5)),
                dma((L,)),
                dma,
                dma,
                dma,
                regular((4, 8)),
            ],
            compiler_params=pltpu.CompilerParams(
                vmem_limit_bytes=67000000,
                has_side_effects=True,
            ),
        )(tokens, cotangent, up, down, lora_a.transpose(0, 2, 1), lora_b)
        x_out, g_tok, shares = outs[:3]
        grads = shares.reshape(L, 4, 2, 4, GW).transpose(0, 2, 3, 1, 4).reshape(L, 2, 4, 4 * GW)
        grad_b = grads[..., 0:2048].transpose(0, 2, 1, 3).reshape(L, 4, F)
        grad_a = grads[..., 2048:2560].transpose(0, 1, 3, 2).reshape(L, H, 4)
        return x_out, g_tok, grad_a, grad_b

    return jax.shard_map(
        device_step,
        mesh=mesh,
        in_specs=(tok_spec, tok_spec, weight_spec, weight_spec, P(), P()),
        out_specs=(tok_spec, tok_spec, P(), P()),
        check_vma=False,
    )
```

```python
import jax
import jax.numpy as jnp
from jax import lax
from jax.experimental import pallas as pl
from jax.experimental.pallas import tpu as pltpu
from jax.sharding import PartitionSpec as P

GROUP = ("data", "local")
NORM_EPS = 1e-6
BF = jnp.bfloat16
F32 = jnp.float32
C0 = 0.7978845608028654
K0 = 0.044715

T = 2048
H = 1024
F = 4096
L = 4
NG = 8 * L
MU = 512
MD = 1024
MX = 512
RB, CB = 16, 256
ROWS = (((0, 96), (96, 80), (176, 80)), ((0, 80), (80, 96), (176, 80)))
FIRST_LAYER = (
    (0, ((1, 4), (2, 3))),
    (2, ((3, 1), (1, 6))),
    (5, ((2, 4),)),
    (6, ((0, 8), (3, 2))),
    (8, ((2, 5), (3, 3), (1, 7))),
    (9, ((1, 8),)),
    (12, ((3, 4), (2, 6))),
    (13, ((0, 10), (0, 9))),
    (14, ((2, 7),)),
    (16, ((1, 9), (3, 5))),
    (17, ((0, 11), (2, 8))),
    (18, ((3, 6), (1, 10))),
    (19, ((2, 9),)),
    (20, ((3, 7), (0, 12), (1, 11))),
    (23, ((0, 13), (1, 12), (0, 14), (2, 10), (3, 8))),
)
GW = 640


def nn(a, b):
    return lax.dot_general(a, b, (((1,), (0,)), ((), ())), preferred_element_type=F32)


def nt(a, b):
    return lax.dot_general(a, b, (((1,), (1,)), ((), ())), preferred_element_type=F32)


def tn(a, b):
    return lax.dot_general(a, b, (((0,), (0,)), ((), ())), preferred_element_type=F32)


def split3(v):
    p1 = v.astype(BF).astype(F32)
    rest = v - p1
    p2 = rest.astype(BF).astype(F32)
    return p1, p2, (rest - p2).astype(BF).astype(F32)


def left_parts(v):
    p1, p2, p3 = split3(v)
    return jnp.concatenate([p1, p2, p3, p1, p1, p2], axis=0).astype(BF)


def right_parts(v):
    p1, p2, p3 = split3(v)
    return jnp.concatenate([p3, p2, p1, p1, p2, p1], axis=0).astype(BF)


def sum_parts(v):
    return v[0:8] + v[8:16] + v[16:24]


def gelu_and_slope(pre):
    x = pre.astype(F32)
    sq = x * x
    half = 0.5 * jnp.tanh(x * (sq * (C0 * K0) + C0)) + 0.5
    act = x * half
    slope = (act * (1.0 - half)) * (sq * (6.0 * C0 * K0) + 2.0 * C0) + half
    return act.astype(BF), slope


def rem3(t):
    return t - 3 * lax.div(t * 43, 128)


def rows_of(m, size):
    return pl.ds(pl.multiple_of(m * size, size), size)


def kernel(
    tok, cot, up, down, a4, b4,
    xout, gtok, gout, gp, xs, kept,
    w, sd, xb, ub, db, gst, pre0, pre1, acat, bcat, vcat, dcat, dlt, gb, ga, gacc, rbuf, gall,
    own_sem, fs_sem, fr_sem, kept_sem, gp_sem, io_sem, bo_sem, bs_sem, br_sem, rs_sem, rr_sem, as_sem, ar_sem,
    cred,
):
    data = lax.axis_index("data")
    local = lax.axis_index("local")
    x, c = lax.div(data, 2), lax.rem(data, 2)
    z, y = lax.div(local, 2), lax.rem(local, 2)
    me = data * 4 + local
    dx, dy, dz, dc = 1 - 2 * x, 1 - 2 * y, 1 - 2 * z, 1 - 2 * c
    par = lax.rem(x + y + z, 2)

    def quarter(i):
        hi, lo = lax.div(i, 2), lax.rem(i, 2)
        return 2 * (par + hi - 2 * par * hi) + (c + lo - 2 * c * lo)

    q_own, q_miss = quarter(0), quarter(2)

    def pick(dim, a0, a1, a2):
        return lax.div((1 - dim) * (2 - dim), 2) * a0 + dim * (2 - dim) * a1 + lax.div(dim * (dim - 1), 2) * a2

    def device(dim):
        return (local + pick(dim, 0, dy, 2 * dz), data + pick(dim, 2 * dx, 0, 0))

    neighbours = ((local, data + 2 * dx), (local + dy, data), (local + 2 * dz, data), (local, data + dc))
    partner = neighbours[3]

    def remote(src, dst, ssem, rsem, dev):
        return pltpu.make_async_remote_copy(
            src_ref=src, dst_ref=dst, send_sem=ssem, recv_sem=rsem, device_id=dev, device_id_type=pl.DeviceIdType.MESH
        )


    def own_load(g):
        s, l = lax.rem(g, 8), lax.div(g, 8)

        @pl.when(s < 4)
        def _():
            for n in range(4):
                pltpu.make_async_copy(
                    up.at[l, :, pl.ds(pl.multiple_of(s * 1024 + n * 256, 256), 256)],
                    w.at[s, me, pl.ds(n * 64, 64), :],
                    own_sem.at[s],
                ).start()

        @pl.when(s >= 4)
        def _():
            pltpu.make_async_copy(
                down.at[l, :, pl.ds(pl.multiple_of((s - 4) * 256, 256), 256)], w.at[s, me], own_sem.at[s]
            ).start()

    def colour(g):
        q = rem3(jnp.where(g == 1, 2, g) + c)
        turn = jnp.where(g == 1, 2, 1)
        return q, rem3(q + turn), rem3(q + 2 * turn)

    def delta(dim):
        return pick(dim, 8 * dx, dy, 2 * dz)

    def use_credit(g, dim):
        @pl.when(g >= 8)
        def _():
            pl.semaphore_wait(cred.at[dim, lax.rem(g, 8)], 1)

    def send_blocks(g, phase, dim, blocks, dev):
        s = lax.rem(g, 8)
        use_credit(g, dim)
        for b in blocks:
            remote(w.at[s, b], w.at[s, b], fs_sem.at[phase, s], fr_sem.at[phase, s], dev).start()

    def span(g, phase):
        s = lax.rem(g, 8)
        r = w.at[s, pl.ds(0, (1, 2, 4, 8)[phase])]
        return remote(r, r, fs_sem.at[phase, s], fr_sem.at[phase, s], partner)

    def ready(g):
        return jnp.logical_and(g >= 0, g < NG)

    def hop1(g):
        d1, _, _ = colour(g)
        s = lax.rem(g, 8)
        pltpu.make_async_copy(w.at[s, me], w.at[s, me], own_sem.at[s]).wait()
        send_blocks(g, 0, d1, (me,), device(d1))

    def hop2(g):
        d1, d2, _ = colour(g)
        span(g, 0).wait_recv()
        send_blocks(g, 1, d2, (me, me + delta(d1)), device(d2))

    def hop3(g):
        d1, d2, d3 = colour(g)
        e1, e2 = delta(d1), delta(d2)
        span(g, 1).wait_recv()
        send_blocks(g, 2, d3, (me, me + e1, me + e2, me + e1 + e2), device(d3))

    def hand_over(g):
        s = lax.rem(g, 8)
        span(g, 2).wait_recv()
        use_credit(g, 3)
        for h in range(2):
            r2 = w.at[s, pl.ds(8 * h + 4 * c, 4)]
            remote(r2, r2, fs_sem.at[3, s], fr_sem.at[3, s], partner).start()

    def event(j):
        for step, ahead in ((hand_over, 1), (hop2, 5), (hop3, 3)):

            @pl.when(j + ahead < NG)
            def _():
                step(j + ahead)

    def refill(j):
        @pl.when(j + 7 < NG)
        def _():
            hop1(j + 7)

    def keep_copy(g):
        s, l = lax.rem(g, 8), lax.div(g, 8)
        return pltpu.make_async_copy(w.at[s, pl.ds(4 * q_own, 4)], kept.at[l, s], kept_sem.at[s])

    def arrive(g):
        span(g, 3).wait_recv()
        keep_copy(g).start()

    def release(g):
        s = lax.rem(g, 8)
        for phase in range(4):
            span(g, phase).wait_send()
        keep_copy(g).wait()
        for i in range(4):
            pl.semaphore_signal(cred.at[i, s], inc=1, device_id=neighbours[i], device_id_type=pl.DeviceIdType.MESH)

        @pl.when(g + 8 < NG)
        def _():
            own_load(g + 8)


    def whole(m, q):
        return w.at[pl.ds(4 * m, 4), pl.ds(4 * q, 4)]

    def part(ref, rows):
        return ref.at[:, :, pl.ds(*rows), :]

    def b_own(m, l):
        return pltpu.make_async_copy(kept.at[l, pl.ds(4 * m, 4)], whole(m, q_own), bo_sem.at[m])

    def b_send(m, l, i, q, core=None):
        src, dst = kept.at[l, pl.ds(4 * m, 4)], whole(m, q)
        if i < 3:
            src, dst = part(src, ROWS[core][i]), part(dst, ROWS[core][i])
        return remote(src, dst, bs_sem.at[m, i], br_sem.at[m, i], neighbours[i])

    def by_core(fn):
        for core in range(2):

            @pl.when(c == core)
            def _():
                fn(core)

    def b_forward(m):
        return remote(whole(m, q_miss), whole(m, q_miss), bs_sem.at[m, 4], br_sem.at[m, 4], partner)

    def gather(m, l):
        @pl.when(jnp.logical_or(l < L - 1, m == 0))
        def _():
            b_own(m, l).start()

        for i in range(4):
            for s in range(4):
                pl.semaphore_wait(cred.at[i, 4 * m + s], 1)
            if i == 3:
                b_send(m, l, i, q_own).start()
            else:
                by_core(lambda core: b_send(m, l, i, q_own, core).start())

    def b_events(m, l, i):
        @pl.when(jnp.logical_and(i == 0, jnp.logical_or(l < L - 1, m == 0)))
        def _():
            b_own(m, l).wait()

        @pl.when(i == 1)
        def _():
            b_send(m, l, 3, quarter(1)).wait_recv()

        @pl.when(i == 2)
        def _():
            by_core(lambda core: [b_send(m, l, d, q_miss, core).wait_recv() for d in range(3)])
            b_forward(m).start()

        @pl.when(i == 3)
        def _():
            b_forward(m).wait_recv()

    def b_release(m, l):
        b_forward(m).wait_send()
        b_send(m, l, 3, q_own).wait_send()
        by_core(lambda core: [b_send(m, l, d, q_own, core).wait_send() for d in range(3)])

        @pl.when(l > 0)
        def _():
            for i in range(4):
                for s in range(4):
                    pl.semaphore_signal(
                        cred.at[i, 4 * m + s], inc=1, device_id=neighbours[i], device_id_type=pl.DeviceIdType.MESH
                    )


    def grad_send(l, i):
        return remote(
            gacc.at[l, :, pl.ds(i * GW, GW)], rbuf.at[me], rs_sem.at[l], rr_sem, (jnp.int32(i), l)
        )

    def grads_out(l):
        for i in range(4):
            mine = me == 4 * l + i

            @pl.when(jnp.logical_not(mine))
            def _():
                grad_send(l, i).start()

            @pl.when(mine)
            def _():
                rbuf[me] = gacc[l, :, i * GW : (i + 1) * GW]


    tok_in = pltpu.make_async_copy(tok, xb, io_sem.at[0])
    cot_in = pltpu.make_async_copy(cot, db, io_sem.at[1])

    def first_loads(g, _):
        own_load(g)
        return 0

    lax.fori_loop(0, 8, first_loads, 0)
    tok_in.start()
    at = jnp.int32
    for g in (0, 1, 2, 5, 7, 3, 6):
        hop1(at(g))
    for b in range(2):
        pltpu.make_async_copy(gst.at[b, pl.ds(0, MX)], gp.at[4 * L, pl.ds(b * MX, MX), :], gp_sem.at[b]).start()
    for l in range(L):
        acat[l] = right_parts(jnp.concatenate([a4[l], jnp.zeros((4, H), F32)], axis=0))
        bcat[l] = right_parts(jnp.concatenate([b4[l], jnp.zeros((4, F), F32)], axis=0))
    tok_in.wait()
    for step, g in ((hop2, 0), (hop2, 1), (hop2, 2), (hop3, 0)):
        step(at(g))

    def first_layer(t, lo, hi):
        for when, steps in FIRST_LAYER:
            if lo <= when < hi:

                @pl.when(t == when - lo)
                def _():
                    for kind, chunk in steps:
                        (hop1, hop2, hop3, hand_over)[kind](at(chunk))


    def inv_rms(rf):
        return lax.rsqrt(jnp.mean(rf * rf, axis=-1, keepdims=True) + NORM_EPS)

    def x_save(l):
        return pltpu.make_async_copy(xb, xs.at[l - 1], io_sem.at[0])

    def slope_out(b, lk, m):
        return pltpu.make_async_copy(gst.at[b, pl.ds(0, MX)], gp.at[lk, rows_of(m, MX), :], gp_sem.at[b])

    def gp_in(t):
        lk = 4 * (L - 1 - lax.div(t, 16)) + quarter(lax.div(lax.rem(t, 16), 4))
        b = rem3(t)
        return pltpu.make_async_copy(gp.at[lk, rows_of(lax.rem(t, 4), MU), :], gst.at[b], gp_sem.at[b])

    blocks = [(rb, cb) for cb in range(0, 1024, CB) for rb in range(0, MX, RB)]

    def activate(src, k, m, slot, part):
        for rb, cb in blocks[part * len(blocks) // 5 : (part + 1) * len(blocks) // 5]:
            act, slope = gelu_and_slope(src[rb : rb + RB, cb : cb + CB].astype(BF))
            r = pl.ds(pl.multiple_of(m * MX + rb, RB), RB)
            sd[r, pl.ds(pl.multiple_of(k * 1024 + cb, CB), CB)] = act
            gst[slot, rb : rb + RB, cb : cb + CB] = slope

    def up_tile(l, k, m, dst, kp, mp, src, slot):
        r = rows_of(m, MX)
        cols = pl.ds(pl.multiple_of(k * 1024, 1024), 1024)
        acc = None
        for kt in range(5):
            if kt < 4:
                rhs = w[k, 4 * kt : 4 * kt + 4]
                rhs = jnp.concatenate([rhs[:, n * 64 : (n + 1) * 64, :].reshape(256, 256) for n in range(4)], axis=1)
                term = nn(ub[r, kt * 256 : (kt + 1) * 256], rhs)
            else:
                term = tn(vcat[l, :, r], bcat[l, :, cols])
            acc = term if acc is None else acc + term
            activate(src, kp, mp, slot, kt)
        dst[...] = acc

    def forward_layer(l, _):
        @pl.when(l > 0)
        def _():
            x_save(l).start()

        def prep(m, _):
            r = rows_of(m, MU)
            rf = xb[r, :].astype(F32)
            u = (rf * inv_rms(rf)).astype(BF)
            ub[r, :] = u
            vcat[l, :, r] = left_parts(sum_parts(nt(acat[l, 0:32], u)))
            return 0

        lax.fori_loop(0, T // MU, prep, 0)

        @pl.when(l == 0)
        def _():
            for step, g in ((hop2, 3), (hop3, 1), (hop1, 4), (hop2, 5), (hand_over, 0), (hop3, 2)):
                step(at(g))

        def slopes(t):
            slot = rem3(2 * l + t)
            old = jnp.maximum(t - 2, 0)
            lk = jnp.where(t == 1, 4 * L, 4 * l + lax.div(old, 4))
            lk = jnp.where(t == 0, jnp.where(l == 0, 4 * L, 4 * l - 1), lk)
            m = jnp.where(t == 0, 3, jnp.where(t == 1, 2, lax.rem(old, 4)))
            slope_out(jnp.where(slot == 0, 2, slot - 1), lk, m).start()
            slope_out(slot, 0, 0).wait()
            return slot

        def up_step(t, _):
            k, m = lax.div(t, 4), lax.rem(t, 4)
            g = 8 * l + k

            due = t == 1
            j = at(0)
            for i in (5, 9, 12, 15):
                due = jnp.logical_or(due, t == i)
                j = j + jnp.where(t >= i, 1, 0)

            @pl.when(m == 0)
            def _():
                @pl.when(k > 0)
                def _():
                    release(g - 1)

                arrive(g)

            @pl.when(l == 0)
            def _():
                first_layer(t, 0, 16)

            @pl.when(jnp.logical_and(l > 0, jnp.logical_or(due, m == 1)))
            def _():
                @pl.when(due)
                def _():
                    event(8 * l + j)

                @pl.when(m == 1)
                def _():
                    refill(g)

            tp = jnp.maximum(t - 1, 0)
            kp, mp = lax.div(tp, 4), lax.rem(tp, 4)
            slot = slopes(t)

            @pl.when(lax.rem(t, 2) == 0)
            def _():
                up_tile(l, k, m, pre0, kp, mp, pre1, slot)

            @pl.when(lax.rem(t, 2) == 1)
            def _():
                up_tile(l, k, m, pre1, kp, mp, pre0, slot)

            return 0

        lax.fori_loop(0, 16, up_step, 0)
        release(8 * l + 3)
        slot = slopes(at(16))
        for part in range(5):
            activate(pre1, 3, at(3), slot, part)

        @pl.when(l == L - 1)
        def _():
            cot_in.start()
            slope_out((2 * (L - 1) + 16) % 3, 4 * L - 1, at(3)).start()

        @pl.when(l > 0)
        def _():
            x_save(l).wait()

        def down_step(t, _):
            k, m = lax.div(t, 2), lax.rem(t, 2)
            g = 8 * l + 4 + k

            @pl.when(m == 0)
            def _():
                @pl.when(k > 0)
                def _():
                    release(g - 1)

                arrive(g)

                @pl.when(jnp.logical_and(l > 0, jnp.logical_or(k == 1, k == 2)))
                def _():
                    event(g)

            @pl.when(jnp.logical_and(l == L - 1, t == 5))
            def _():
                for b in range(3):
                    slope_out(b, 0, at(0)).wait()
                gp_in(at(0)).start()
                gp_in(at(1)).start()

            @pl.when(l == 0)
            def _():
                first_layer(t, 16, 24)

            @pl.when(jnp.logical_and(l > 0, m == 1))
            def _():
                refill(g)

                @pl.when(k == 3)
                def _():
                    event(g)

            r = rows_of(m, MD)
            cols = pl.ds(pl.multiple_of(k * 256, 256), 256)
            step = nn(sd[r, :], w[4 + k].reshape(F, 256))
            xb[r, cols] = (xb[r, cols].astype(F32) + step).astype(BF)
            return 0

        lax.fori_loop(0, 8, down_step, 0)
        release(8 * l + 7)
        return 0

    lax.fori_loop(0, L, forward_layer, 0)


    x_final = pltpu.make_async_copy(xb, xout, io_sem.at[0])
    x_final.start()
    gather(1, L - 1)
    cot_in.wait()


    def x_load(l, start):
        @pl.when(l > 0)
        def _():
            cp = pltpu.make_async_copy(xs.at[l - 1], xb, io_sem.at[0])
            cp.start() if start else cp.wait()

        @pl.when(l == 0)
        def _():
            cp = pltpu.make_async_copy(tok, xb, io_sem.at[0])
            cp.start() if start else cp.wait()

    def finish_rows(r):
        rf = xb[r, :].astype(F32)
        inv = inv_rms(rf)
        dn = ub[r, :].astype(F32)
        dot = jnp.mean(rf * dn, axis=-1, keepdims=True)
        db[r, :] = (db[r, :].astype(F32) + inv * dn - rf * ((inv * inv * inv) * dot)).astype(BF)
        return rf, inv

    def backward_layer(rl, _):
        l = L - 1 - rl
        dlt[...] = jnp.zeros_like(dlt)
        gb[...] = jnp.zeros_like(gb)
        ga[...] = jnp.zeros_like(ga)

        def down_step(i, _):
            @pl.when(i == 1)
            def _():
                gather(0, l)

            @pl.when(i == 2)
            def _():
                @pl.when(l == L - 1)
                def _():
                    x_final.wait()

                x_load(l, True)

            b_events(1, l, i)
            q = quarter(i)
            cols = pl.ds(pl.multiple_of(q * 1024, 1024), 1024)

            def tile(m, _):
                t = rl * 16 + i * 4 + m

                @pl.when(t + 2 < 16 * L)
                def _():
                    gp_in(t + 2).start()

                gp_in(t).wait()
                r = rows_of(m, MU)
                acc = None
                for k in range(4):
                    rhs = w[4 + k, pl.ds(4 * q, 4)].reshape(1024, 256)
                    term = nt(db[r, k * 256 : (k + 1) * 256], rhs)
                    acc = term if acc is None else acc + term
                d = (acc.astype(BF).astype(F32) * gst[rem3(t)]).astype(BF)
                sd[r, cols] = d
                dlt[:, r] += nt(bcat[l, 0:32, cols], d)
                gb[:, cols] += nn(vcat[l, 0:32, r], d)
                return 0

            lax.fori_loop(0, T // MU, tile, 0)
            return 0

        lax.fori_loop(0, 4, down_step, 0)
        b_release(1, l)
        dcat[...] = left_parts(sum_parts(dlt[...]))
        gb8 = sum_parts(gb[...])
        gacc[l, :, 0:2048] = gb8[:, 0:2048] + pltpu.roll(gb8[:, 2048:4096], 4, 0)

        def up_step(i, _):
            @pl.when(jnp.logical_and(i == 1, l > 0))
            def _():
                gather(1, l - 1)

            b_events(0, l, i)
            q = quarter(i)
            cols = pl.ds(pl.multiple_of(q * 256, 256), 256)

            def tile(m, _):
                r = rows_of(m, MD)
                acc = None
                for k in range(4):
                    for n in range(4):
                        rhs = w[k, pl.ds(4 * q, 4), n * 64 : (n + 1) * 64, :].reshape(256, 256)
                        j = 4 * k + n
                        term = nt(sd[r, j * 256 : (j + 1) * 256], rhs)
                        acc = term if acc is None else acc + term
                side = tn(dcat[:, r], acat[l, :, cols]).astype(BF)
                ub[r, cols] = acc.astype(BF) + side
                return 0

            lax.fori_loop(0, T // MD, tile, 0)
            return 0

        def grads_done():
            ga8 = sum_parts(ga[...])
            gacc[l, :, 2048:2560] = ga8[:, 0:512] + pltpu.roll(ga8[:, 512:1024], 4, 0)
            grads_out(l)

        x_load(l, False)

        @pl.when(l == 0)
        def _():
            def grad_a(m, _):
                r = rows_of(m, MU)
                rf = xb[r, :].astype(F32)
                ga[...] += nn(dcat[0:32, r], (rf * inv_rms(rf)).astype(BF))
                return 0

            lax.fori_loop(0, T // MU, grad_a, 0)
            grads_done()

        lax.fori_loop(0, 4, up_step, 0)
        b_release(0, l)

        @pl.when(l > 0)
        def _():
            def finish(m, _):
                r = rows_of(m, MU)
                rf, inv = finish_rows(r)
                ga[...] += nn(dcat[0:32, r], (rf * inv).astype(BF))
                return 0

            lax.fori_loop(0, T // MU, finish, 0)
            grads_done()

        return 0

    lax.fori_loop(0, L, backward_layer, 0)


    others = rbuf.at[pl.ds(0, 15)]
    remote(others, others, rr_sem, rr_sem, partner).wait_recv()
    total = rbuf[0]
    for i in range(1, 16):
        total = total + rbuf[i]
    gall[me] = total

    def share(o, _):
        @pl.when(o != me)
        def _():
            remote(gall.at[me], gall.at[me], as_sem, ar_sem, (lax.rem(o, 4), lax.div(o, 4))).start()

        return 0

    lax.fori_loop(0, 16, share, 0)

    def last_finish(m, _):
        finish_rows(rows_of(m, MU))
        return 0

    lax.fori_loop(0, T // MU, last_finish, 0)
    g_final = pltpu.make_async_copy(db, gtok, io_sem.at[1])
    g_final.start()
    others = gall.at[pl.ds(0, 15)]
    remote(others, others, as_sem, ar_sem, partner).wait_send()
    remote(others, others, as_sem, ar_sem, partner).wait_recv()
    for l in range(L):
        for i in range(4):

            @pl.when(me != 4 * l + i)
            def _():
                grad_send(jnp.int32(l), i).wait_send()

    shares = pltpu.make_async_copy(gall, gout, io_sem.at[0])
    shares.start()
    g_final.wait()
    shares.wait()


def solution(mesh):
    tok_spec = P(GROUP, None)
    weight_spec = P(None, GROUP, None)

    def device_step(tokens, cotangent, up, down, lora_a, lora_b):
        hbm = pl.BlockSpec(memory_space=pltpu.HBM)
        vmem = pl.BlockSpec(memory_space=pltpu.VMEM)
        shape = jax.ShapeDtypeStruct
        dma, regular = pltpu.SemaphoreType.DMA, pltpu.SemaphoreType.REGULAR
        outs = pl.pallas_call(
            kernel,
            name="stack",
            out_shape=[
                shape((T, H), BF),
                shape((T, H), BF),
                shape((16, 8, GW), F32),
                shape((4 * L + 1, T, 1024), F32),
                shape((L - 1, T, H), BF),
                shape((L, 8, 4, 256, 256), BF),
            ],
            in_specs=[hbm, hbm, hbm, hbm, vmem, vmem],
            out_specs=[hbm] * 6,
            scratch_shapes=[
                pltpu.VMEM((8, 16, 256, 256), BF),
                pltpu.VMEM((T, F), BF),
                pltpu.VMEM((T, H), BF),
                pltpu.VMEM((T, H), BF),
                pltpu.VMEM((T, H), BF),
                pltpu.VMEM((3, MU, 1024), F32),
                pltpu.VMEM((MX, 1024), F32),
                pltpu.VMEM((MX, 1024), F32),
                pltpu.VMEM((L, 48, H), BF),
                pltpu.VMEM((L, 48, F), BF),
                pltpu.VMEM((L, 48, T), BF),
                pltpu.VMEM((48, T), BF),
                pltpu.VMEM((32, T), F32),
                pltpu.VMEM((32, F), F32),
                pltpu.VMEM((32, H), F32),
                pltpu.VMEM((L, 8, 4 * GW), F32),
                pltpu.VMEM((16, 8, GW), F32),
                pltpu.VMEM((16, 8, GW), F32),
                dma((8,)),
                dma((4, 8)),
                dma((4, 8)),
                dma((8,)),
                dma((3,)),
                dma((2,)),
                dma((2,)),
                dma((2, 5)),
                dma((2, 5)),
                dma((L,)),
                dma,
                dma,
                dma,
                regular((4, 8)),
            ],
            compiler_params=pltpu.CompilerParams(
                vmem_limit_bytes=67000000,
                has_side_effects=True,
            ),
        )(tokens, cotangent, up, down, lora_a.transpose(0, 2, 1), lora_b)
        x_out, g_tok, shares = outs[:3]
        grads = shares.reshape(L, 4, 2, 4, GW).transpose(0, 2, 3, 1, 4).reshape(L, 2, 4, 4 * GW)
        grad_b = grads[..., 0:2048].transpose(0, 2, 1, 3).reshape(L, 4, F)
        grad_a = grads[..., 2048:2560].transpose(0, 1, 3, 2).reshape(L, H, 4)
        return x_out, g_tok, grad_a, grad_b

    return jax.shard_map(
        device_step,
        mesh=mesh,
        in_specs=(tok_spec, tok_spec, weight_spec, weight_spec, P(), P()),
        out_specs=(tok_spec, tok_spec, P(), P()),
        check_vma=False,
    )
```
